32 devices in a mesh: dp: 16 (over z, x, core), tensor: 2 (over y).
Axes of the slice: x: 2, y: 2, z: 4, core: 2. Of those that a mesh axis runs over, the one named last changes fastest.
Arguments:
- tokens: bfloat16 [32768, 768], P(('dp', 'tensor')), may hold values from -6 to 6
- grad_tokens: bfloat16 [32768, 768], P(('dp', 'tensor')), may hold values from -6 to 6
- dealing: int32 [32, 1024], P(('dp', 'tensor')), may hold values from 0 to 1023, each once within a row
- segment_ids: int32 [32768], P('dp'), may hold values from 0 to 1, as said below
- ln1_gain: float32 [768], P('dp'), may hold values from 0.5 to 1.5
- ln1_bias: float32 [768], P('dp'), may hold values from -1.5 to 1.5
- w_qkv: bfloat16 [768, 3, 768], P('dp', None, 'tensor'), may hold values from -0.21875 to 0.21875
- b_qv: float32 [2, 768], P(None, 'tensor'), may hold values from -2.5 to 2.5
- w_out: bfloat16 [768, 768], P('tensor', 'dp'), may hold values from -0.875 to 0.875
- b_out: float32 [768], P('dp'), may hold values from -2.5 to 2.5
- ln2_gain: float32 [768], P('dp'), may hold values from 0.5 to 1.5
- ln2_bias: float32 [768], P('dp'), may hold values from -1.5 to 1.5
- w_up: bfloat16 [768, 3072], P('dp', 'tensor'), may hold values from -0.21875 to 0.21875
- b_up: float32 [3072], P('tensor'), may hold values from -2.5 to 2.5
- w_down: bfloat16 [3072, 768], P('tensor', 'dp'), may hold values from -0.109375 to 0.109375
- b_down: float32 [768], P('dp'), may hold values from -2.5 to 2.5
Outputs:
- output: bfloat16 [32768, 768], P(('dp', 'tensor'))
- input_grad: bfloat16 [32768, 768], P(('dp', 'tensor'))
- ln1_gain_grad: float32 [768], P('dp')
- ln1_bias_grad: float32 [768], P('dp')
- w_qkv_grad: float32 [768, 3, 768], P('dp', None, 'tensor')
- b_qv_grad: float32 [2, 768], P(None, 'tensor')
- w_out_grad: float32 [768, 768], P('tensor', 'dp')
- b_out_grad: float32 [768], P('dp')
- ln2_gain_grad: float32 [768], P('dp')
- ln2_bias_grad: float32 [768], P('dp')
- w_up_grad: float32 [768, 3072], P('dp', 'tensor')
- b_up_grad: float32 [3072], P('tensor')
- w_down_grad: float32 [3072, 768], P('tensor', 'dp')
- b_down_grad: float32 [768], P('dp')
The draws below stay inside these ranges and needn't reach their ends.
Inputs may be any that keep to these rules, and one draw needn't show every extreme that they name: Each row of dealing orders 0 to 1023, each number once. `segment_ids`: in dealt order, the 2048 rows of each group are one sequence (all 0) or two sequences of 1024 rows (0s, then 1s); both kinds of group occur.
All inputs are finite; a program needn't handle non-finite values.
Results may differ from the reference program's by a relative error of at most 0.03.
Values may be sent and summed in bfloat16 or wider, within the bound.
A program may use at most 256 MiB of HBM per device.

```python
import jax
import jax.numpy as jnp
from jax import lax

D = 768
HEADS = 12
HD = 64
FF = 3072
TOK_DEV = 1024
GROUP = 2048
TOKENS = 32768
BLK = 64
QBLK = 512
N_DP = 16
N_TENSOR = 2


def draw_segment_ids(key, part):
    groups = TOKENS // GROUP
    coins = jax.random.randint(key, (groups,), 0, 2).astype(jnp.int32)
    coins = coins.at[0].set(1).at[1].set(0)
    later = (jnp.arange(GROUP) >= GROUP // 2).astype(jnp.int32)
    return (coins[:, None] * later[None, :]).reshape(TOKENS).astype(jnp.int32)


def raised(values, key, source, target, shards_of, factor):
    owner, partner = [(jnp.arange(values.shape[position]) // (values.shape[position] // shards_of)).reshape([-1 if axis == position else 1 for axis in range(values.ndim)]) for position in (source, target)]
    chosen = jax.random.permutation(key, shards_of)[partner]
    strong = (owner == chosen) | (owner == (partner + shards_of // 2) % shards_of)
    return jnp.where(strong, factor * values, values)


def levels(rng, extent, split, least, largest):
    level, own = 1.0, jax.random.fold_in(rng, 6)
    for axis_at, parts in split:
        draws = jnp.exp(jax.random.uniform(jax.random.fold_in(own, axis_at), (parts,), jnp.float32, least / len(split), largest / len(split)))
        level = level * jnp.repeat(draws, extent[axis_at] // parts).reshape([-1 if axis == axis_at else 1 for axis in range(len(extent))])
    return level


def noise(key, extent, scale, limit, cuts=(), held_as=jnp.bfloat16):
    gain = levels(key, extent, cuts, -0.22, 0.18) if cuts else 1.0
    values = jax.random.normal(key, extent, jnp.float32) * scale * gain
    return jnp.minimum(jnp.maximum(values, -limit), limit).astype(held_as)


def noise_with(key, dims, spread, bound, shards, heavy, kind=jnp.bfloat16):
    entries = spread * jax.random.normal(key, dims, jnp.float32)
    if shards:
        entries = entries * levels(key, dims, shards, -0.22, 0.18)
    return jnp.clip(raised(entries, jax.random.fold_in(key, 3), *heavy), -bound, bound).astype(kind)


def setup_inputs(seed: int = 0) -> dict:
    keys = jax.random.split(jax.random.key(seed), 17)
    return {
        "tokens": noise(keys[0], (TOKENS, D), 1.0, 6.0, ((0, 32),)),
        "grad_tokens": noise_with(keys[1], (TOKENS, D), 1.0, 6.0, ((0, 32),), (0, 1, 32, 2.75)),
        "dealing": jax.vmap(lambda own: jax.random.permutation(own, TOK_DEV))(jax.random.split(keys[2], (N_DP * N_TENSOR))).reshape((N_DP * N_TENSOR, TOK_DEV)).astype(jnp.int32),
        "segment_ids": draw_segment_ids(jax.random.fold_in(keys[16], 71), 0),
        "ln1_gain": jnp.clip(1.0 + 0.1 * jax.random.normal(keys[4], (D,), jnp.float32), 0.5, 1.5),
        "ln1_bias": noise(keys[5], (D,), 0.3, 1.5, ((0, 16),), jnp.float32),
        "w_qkv": noise(keys[6], (D, 3, D), D ** -0.5, 0.21875, ((0, 16), (2, 2))),
        "b_qv": noise(keys[7], (2, D), 0.5, 2.5, ((1, 2),), jnp.float32),
        "w_out": noise(keys[8], (D, D), (D // 16) ** -0.5, 0.875, ((0, 2), (1, 16))),
        "b_out": noise(keys[9], (D,), 0.5, 2.5, ((0, 16),), jnp.float32),
        "ln2_gain": jnp.clip(1.0 + 0.1 * jax.random.normal(keys[10], (D,), jnp.float32), 0.5, 1.5),
        "ln2_bias": noise(keys[11], (D,), 0.3, 1.5, ((0, 16),), jnp.float32),
        "w_up": noise(keys[12], (D, FF), D ** -0.5, 0.21875, ((0, 16), (1, 2))),
        "b_up": noise(keys[13], (FF,), 0.5, 2.5, ((0, 2),), jnp.float32),
        "w_down": noise(keys[14], (FF, D), FF ** -0.5, 0.109375, ((0, 2), (1, 16))),
        "b_down": noise(keys[15], (D,), 0.5, 2.5, ((0, 16),), jnp.float32),
    }


EPS = 1e-06
MASKED = -1e+30

@jax.custom_vjp
def low(v):
    return lax.optimization_barrier(v.astype(jnp.bfloat16)).astype(jnp.float32)

@jax.custom_vjp
def low_back(v):
    return v

def low_keep(v):
    return (low(v), None)

def low_pass(kept, grad):
    return (grad,)

def back_keep(v):
    return (v, None)

def back_low(kept, grad):
    return (low(grad),)
low.defvjp(low_keep, low_pass)
low_back.defvjp(back_keep, back_low)

def matmul(left, right):
    return jnp.dot(left, right, precision=lax.Precision.HIGHEST, preferred_element_type=jnp.float32)

def layer_norm(values, gain_row, bias_row):
    centred = values - lax.optimization_barrier(jnp.mean(values, axis=-1, keepdims=True))
    factor = lax.rsqrt(lax.optimization_barrier(jnp.mean(centred * centred, axis=-1, keepdims=True)) + EPS)
    return centred * factor * gain_row + bias_row

def attend_block(pieces, key_rows, value_rows, seg_cols):
    queries, seg_rows = pieces
    scores = jnp.einsum('qhd,khd->hqk', queries, key_rows, precision=lax.Precision.HIGHEST) * HD ** (-0.5)
    scores = low_back(scores)
    allowed = seg_rows[:, None] == seg_cols[None, :]
    scores = jnp.where(allowed[None], scores, MASKED)
    row_max = lax.optimization_barrier(jnp.max(scores, axis=-1, keepdims=True))
    weights = jnp.exp(scores - row_max)
    totals = lax.optimization_barrier(jnp.sum(weights, axis=-1, keepdims=True))
    weights_low = low(weights / totals)
    return jnp.einsum('hqk,khd->qhd', weights_low, value_rows, precision=lax.Precision.HIGHEST)

def group_forward(resid, seg_ids, params):
    gain_one, bias_one, w_qkv, b_qv, w_out, b_out, gain_two, bias_two, w_up, b_up, w_down, b_down = params
    group_rows = resid.shape[0]
    ln_one = low(layer_norm(resid, gain_one, bias_one))
    qkv = jnp.einsum('nd,dce->nce', ln_one, w_qkv, precision=lax.Precision.HIGHEST)
    queries = low_back(low(qkv[:, 0] + b_qv[0]))
    key_rows = low_back(low(qkv[:, 1]))
    value_rows = low_back(low(qkv[:, 2] + b_qv[1]))
    queries = queries.reshape(group_rows // QBLK, QBLK, HEADS, HD)
    key_rows = key_rows.reshape(group_rows, HEADS, HD)
    value_rows = value_rows.reshape(group_rows, HEADS, HD)
    block_fn = jax.checkpoint(lambda pieces: attend_block(pieces, key_rows, value_rows, seg_ids))
    mixed_heads = lax.map(block_fn, (queries, seg_ids.reshape(group_rows // QBLK, QBLK)))
    attended = low_back(low(mixed_heads.reshape(group_rows, D)))
    hidden = resid + low_back(matmul(attended, w_out)) + b_out
    ln_two = low(layer_norm(hidden, gain_two, bias_two))
    pre_act = low_back(matmul(ln_two, w_up) + b_up)
    activated = low(jax.nn.gelu(pre_act, approximate=True))
    return hidden + low_back(matmul(activated, w_down)) + b_down

def to_dealt(source_rows, dealing):
    width = source_rows.shape[-1]
    local_rows = source_rows.reshape(N_DP * N_TENSOR, TOK_DEV, width)
    reordered = jax.vmap(lambda piece, row_order: jnp.take(piece, row_order, axis=0))(local_rows, dealing)
    reordered = reordered.reshape(N_DP, N_TENSOR, N_DP, BLK, width)
    return jnp.transpose(reordered, (2, 1, 0, 3, 4)).reshape(TOKENS, width)

def from_dealt(dealt_rows, dealing):
    width = dealt_rows.shape[-1]
    blocks = dealt_rows.reshape(N_DP, N_TENSOR, N_DP, BLK, width)
    reordered = jnp.transpose(blocks, (2, 1, 0, 3, 4)).reshape(N_DP * N_TENSOR, TOK_DEV, width)
    restored = jax.vmap(lambda piece, row_order: jnp.zeros_like(piece).at[row_order].set(piece))(reordered, dealing)
    return restored.reshape(TOKENS, width)

def reference(tokens, grad_tokens, dealing, segment_ids, ln1_gain, ln1_bias, w_qkv, b_qv, w_out, b_out, ln2_gain, ln2_bias, w_up, b_up, w_down, b_down):
    params = tuple((p.astype(jnp.float32) for p in (ln1_gain, ln1_bias, w_qkv, b_qv, w_out, b_out, ln2_gain, ln2_bias, w_up, b_up, w_down, b_down)))
    dealt = to_dealt(tokens.astype(jnp.float32), dealing).reshape(N_DP, GROUP, D)
    dealt_grad = to_dealt(grad_tokens.astype(jnp.float32), dealing).reshape(N_DP, GROUP, D)
    seg_groups = segment_ids.reshape(N_DP, GROUP)

    def one_group(totals, pieces):
        resid, grad_rows, seg_ids = pieces
        result, pull = jax.vjp(lambda rows_in, *weights: group_forward(rows_in, seg_ids, weights), resid, *params)
        grads = pull(grad_rows)
        return (tuple((t + g for t, g in zip(totals, grads[1:]))), (result, grads[0]))
    totals, (results, input_grads) = lax.scan(one_group, tuple((jnp.zeros_like(p) for p in params)), (dealt, dealt_grad, seg_groups))
    output = from_dealt(results.reshape(TOKENS, D), dealing).astype(jnp.bfloat16)
    input_grad = from_dealt(input_grads.reshape(TOKENS, D), dealing).astype(jnp.bfloat16)
    return (output, input_grad, totals[0], totals[1], totals[2], totals[3], totals[4], totals[5], totals[6], totals[7], totals[8], totals[9], totals[10], totals[11])
```

```python
import functools

import jax
import jax.numpy as jnp
from jax import lax
from jax.experimental import pallas as pl
from jax.experimental.pallas import tpu as pltpu
from jax.sharding import PartitionSpec as P

HD = 64
LANES = 128
EPS = 1e-06
LN2 = 0.6931471805599453
LOG2E = 1.4426950408889634
F32 = jnp.float32
BF16 = jnp.bfloat16


def normalize(values, gain_row, bias_row):
    centred = values - jnp.mean(values, axis=-1, keepdims=True)
    factor = lax.rsqrt(jnp.mean(centred * centred, axis=-1, keepdims=True) + EPS)
    normed = centred * factor
    return (normed * gain_row + bias_row, normed, factor)


def norm_back(grad_rows, normed, factor, gain_row):
    scaled = grad_rows * gain_row
    centred = scaled - jnp.mean(scaled, axis=-1, keepdims=True)
    return factor * (centred - normed * jnp.mean(scaled * normed, axis=-1, keepdims=True))


def mm(left, right, left_dim=1, right_dim=0):
    return lax.dot_general(
        left, right, (((left_dim,), (right_dim,)), ((), ())), preferred_element_type=F32
    )


def head_lanes(head):
    return (lax.broadcasted_iota(jnp.int32, (1, LANES), 1) // HD) == head


def attend_rows(q, keys, values):
    outs, lses = [], []
    one = jnp.ones((), BF16)
    for head in range(2):
        mine = head_lanes(head)
        scores = mm(jnp.where(mine, q, jnp.zeros_like(q)), keys, 1, 1)
        row_max = jnp.max(scores, axis=1, keepdims=True)
        weights = jnp.exp2(scores - row_max).astype(BF16)
        mixed = mm(weights, jnp.where(mine, values, one))
        total = jnp.sum(jnp.where(mine, 0.0, mixed), axis=1, keepdims=True) * (1.0 / HD)
        outs.append(mixed / total)
        lses.append(row_max + jnp.log2(total))
    first = head_lanes(0)
    return (jnp.where(first, outs[0], outs[1]), jnp.where(first, lses[0], lses[1]))


def own_forward(q_ref, kv_ref, mixed_ref, lse_ref, *, qblock):
    for block in range(q_ref.shape[0] // qblock):
        rows = pl.ds(block * qblock, qblock)
        mixed, lse = attend_rows(q_ref[rows, :], kv_ref[:, :LANES], kv_ref[:, LANES:])
        mixed_ref[rows, :] = mixed
        lse_ref[rows, :] = lse


def pair_forward(joined_ref, q_ref, kv_ref, own_ref, own_lse_ref, mixed_ref, lse_ref, *, qblock):
    joined = joined_ref[0] > 0

    @pl.when(joined)
    def _():
        for block in range(q_ref.shape[0] // qblock):
            rows = pl.ds(block * qblock, qblock)
            mixed, lse = attend_rows(q_ref[rows, :], kv_ref[:, :LANES], kv_ref[:, LANES:])
            own_lse = own_lse_ref[rows, :]
            top = jnp.maximum(own_lse, lse)
            own_share = jnp.exp2(own_lse - top)
            pair_share = jnp.exp2(lse - top)
            total = own_share + pair_share
            mixed_ref[rows, :] = (
                (own_ref[rows, :] * own_share + mixed * pair_share) / total
            ).astype(BF16)
            lse_ref[rows, :] = top + jnp.log2(total)

    @pl.when(jnp.logical_not(joined))
    def _():
        mixed_ref[...] = own_ref[...].astype(BF16)
        lse_ref[...] = own_lse_ref[...]


def split_three(values):
    high = values.astype(BF16)
    rest = values - high.astype(F32)
    middle = rest.astype(BF16)
    return high, middle, (rest - middle.astype(F32)).astype(BF16)


def attend_back(q_ref, grad_ref, mixed_ref, lse_ref, kv_ref, dkv_ref, dq_sum, kblock):
    lane = lax.broadcasted_iota(jnp.int32, (1, LANES), 1)
    q = q_ref[...]
    grad = grad_ref[...]
    products = grad.astype(F32) * mixed_ref[...].astype(F32)
    wide_q, wide_grad = [], []
    for head in range(2):
        mine = head_lanes(head)
        spare = (1 - head) * HD
        inner = jnp.sum(jnp.where(mine, products, 0.0), axis=1, keepdims=True)
        lse_parts = split_three(-lse_ref[:, head * HD : head * HD + 1])
        inner_parts = split_three(-inner)
        q_head = jnp.where(mine, q, jnp.zeros_like(q))
        grad_head = jnp.where(mine, grad, jnp.zeros_like(grad))
        for part in range(3):
            q_head = jnp.where(lane == spare + part, lse_parts[part], q_head)
            grad_head = jnp.where(lane == spare + part, inner_parts[part], grad_head)
        wide_q.append(q_head)
        wide_grad.append(grad_head)
    one = jnp.ones((), BF16)
    first = head_lanes(0)
    for block in range(kv_ref.shape[0] // kblock):
        rows = pl.ds(block * kblock, kblock)
        keys = kv_ref[rows, :LANES]
        values = kv_ref[rows, LANES:]
        key_grads, value_grads = [], []
        for head in range(2):
            mine = head_lanes(head)
            weights = jnp.exp2(mm(jnp.where(mine, keys, one), wide_q[head], 1, 1))
            grad_weights = mm(jnp.where(mine, values, one), wide_grad[head], 1, 1)
            grad_scores = (weights * grad_weights).astype(BF16)
            value_grads.append(mm(weights.astype(BF16), grad))
            key_grads.append(mm(grad_scores, q))
            dq_sum[head] += mm(keys, grad_scores, 0, 0)
        dkv_ref[rows, :LANES] = (jnp.where(first, key_grads[0], key_grads[1]) * LN2).astype(BF16)
        dkv_ref[rows, LANES:] = jnp.where(first, value_grads[0], value_grads[1]).astype(BF16)


def query_grad(dq_sum):
    return jnp.concatenate([dq_sum[0, :HD, :], dq_sum[1, HD:, :]], axis=0)


def pair_backward(
    joined_ref, q_ref, grad_ref, mixed_ref, lse_ref, kv_ref, dq_ref, dkv_ref, dq_sum, *, kblock
):
    joined = joined_ref[0] > 0
    dq_sum[...] = jnp.zeros_like(dq_sum)

    @pl.when(joined)
    def _():
        attend_back(q_ref, grad_ref, mixed_ref, lse_ref, kv_ref, dkv_ref, dq_sum, kblock)

    @pl.when(jnp.logical_not(joined))
    def _():
        dkv_ref[...] = jnp.zeros_like(dkv_ref)

    dq_ref[...] = query_grad(dq_sum)


def own_backward(
    q_ref, grad_ref, mixed_ref, lse_ref, kv_ref, pair_dq_ref, dq_ref, dkv_ref, dq_sum, *, kblock
):
    dq_sum[...] = jnp.zeros_like(dq_sum)
    attend_back(q_ref, grad_ref, mixed_ref, lse_ref, kv_ref, dkv_ref, dq_sum, kblock)
    total = query_grad(dq_sum) + pair_dq_ref[...]
    dq_ref[...] = (total.T * HD**-0.5).astype(BF16)


def params(**extra):
    return pltpu.CompilerParams(vmem_limit_bytes=56 << 20, **extra)


def cost(rows, keys, width, products):
    return pl.CostEstimate(
        flops=2 * rows * keys * width * products * 4,
        bytes_accessed=2 * width * (rows + 2 * keys),
        transcendentals=rows * keys * width // HD,
    )


def attention(joined, qkv, kv_of_pair):
    rows = qkv.shape[0]
    width = qkv.shape[1] // 3
    pairs = width // LANES
    column = pl.BlockSpec((rows, LANES), lambda p: (0, p))
    own_kv = pl.BlockSpec((rows, 2 * LANES), lambda p: (0, pairs // 2 + p))
    pair_kv = pl.BlockSpec((rows, 2 * LANES), lambda p: (0, p))
    flag = pl.BlockSpec(memory_space=pltpu.SMEM)
    qblock = min(512, rows)
    shape = jax.ShapeDtypeStruct((rows, width), F32)
    own, own_lse = pl.pallas_call(
        functools.partial(own_forward, qblock=qblock),
        grid=(pairs,),
        in_specs=[column, own_kv],
        out_specs=[column, column],
        out_shape=[shape, shape],
        compiler_params=params(),
        cost_estimate=cost(rows, rows, width, 2),
        name="attend_own",
    )(qkv, qkv)
    return pl.pallas_call(
        functools.partial(pair_forward, qblock=qblock),
        grid=(pairs,),
        in_specs=[flag, column, pair_kv, column, column],
        out_specs=[column, column],
        out_shape=[jax.ShapeDtypeStruct((rows, width), BF16), shape],
        compiler_params=params(),
        cost_estimate=cost(rows, rows, width, 2),
        name="attend_pair",
    )(joined, qkv, kv_of_pair, own, own_lse)


def attention_back_pair(joined, qkv, kv_of_pair, grad, mixed, lse):
    rows, width = grad.shape
    pairs = width // LANES
    column = pl.BlockSpec((rows, LANES), lambda p: (0, p))
    pair_kv = pl.BlockSpec((rows, 2 * LANES), lambda p: (0, p))
    across = pl.BlockSpec((LANES, rows), lambda p: (p, 0))
    return pl.pallas_call(
        functools.partial(pair_backward, kblock=min(512, rows)),
        grid=(pairs,),
        in_specs=[pl.BlockSpec(memory_space=pltpu.SMEM)] + [column] * 4 + [pair_kv],
        out_specs=[across, pair_kv],
        out_shape=[
            jax.ShapeDtypeStruct((width, rows), F32),
            jax.ShapeDtypeStruct((rows, 2 * width), BF16),
        ],
        scratch_shapes=[pltpu.VMEM((2, LANES, rows), F32)],
        compiler_params=params(),
        cost_estimate=cost(rows, rows, width, 5),
        name="attend_back_pair",
    )(joined, qkv, grad, mixed, lse, kv_of_pair)


def attention_back_own(qkv, grad, mixed, lse, pair_dq):
    rows, width = grad.shape
    pairs = width // LANES
    column = pl.BlockSpec((rows, LANES), lambda p: (0, p))
    own_kv = pl.BlockSpec((rows, 2 * LANES), lambda p: (0, pairs // 2 + p))
    kv_out = pl.BlockSpec((rows, 2 * LANES), lambda p: (0, p))
    across = pl.BlockSpec((LANES, rows), lambda p: (p, 0))
    return pl.pallas_call(
        functools.partial(own_backward, kblock=min(512, rows)),
        grid=(pairs,),
        in_specs=[column] * 4 + [own_kv, across],
        out_specs=[column, kv_out],
        out_shape=[
            jax.ShapeDtypeStruct((rows, width), BF16),
            jax.ShapeDtypeStruct((rows, 2 * width), BF16),
        ],
        scratch_shapes=[pltpu.VMEM((2, LANES, rows), F32)],
        compiler_params=params(),
        cost_estimate=cost(rows, rows, width, 5),
        name="attend_back_own",
    )(qkv, grad, mixed, lse, qkv, pair_dq)


def small_kernel(n_dp, slice_ref, bias_ref, all_ref, partner_ref, send_sem, recv_sem):
    me = lax.axis_index("dp")
    t = lax.axis_index("tensor")

    barrier = pltpu.get_barrier_semaphore()

    def greet(step, carry):
        peer = lax.rem(me + step, n_dp)
        pl.semaphore_signal(
            barrier, inc=1, device_id=(peer, t), device_id_type=pl.DeviceIdType.MESH
        )
        return carry

    lax.fori_loop(1, n_dp, greet, 0)
    pl.semaphore_signal(
        barrier, inc=1, device_id=(me, 1 - t), device_id_type=pl.DeviceIdType.MESH
    )
    pl.semaphore_wait(barrier, n_dp)

    def to_peer(step):
        return pltpu.make_async_remote_copy(
            src_ref=slice_ref,
            dst_ref=all_ref.at[me],
            send_sem=send_sem.at[step],
            recv_sem=recv_sem.at[step],
            device_id=(lax.rem(me + step, n_dp), t),
            device_id_type=pl.DeviceIdType.MESH,
        )

    to_partner = pltpu.make_async_remote_copy(
        src_ref=bias_ref,
        dst_ref=partner_ref,
        send_sem=send_sem.at[0],
        recv_sem=recv_sem.at[0],
        device_id=(me, 1 - t),
        device_id_type=pl.DeviceIdType.MESH,
    )
    to_partner.start()

    def start(step, carry):
        to_peer(step).start()
        return carry

    def finish(step, carry):
        to_peer(step).wait()
        return carry

    lax.fori_loop(1, n_dp, start, 0)
    all_ref[me] = slice_ref[...]
    lax.fori_loop(1, n_dp, finish, 0)
    to_partner.wait()


def share_small(n_dp, slices, biases):
    vmem = pl.BlockSpec(memory_space=pltpu.VMEM)
    return pl.pallas_call(
        functools.partial(small_kernel, n_dp),
        in_specs=[vmem, vmem],
        out_specs=[vmem, vmem],
        out_shape=[
            jax.ShapeDtypeStruct((n_dp,) + slices.shape, F32),
            jax.ShapeDtypeStruct(biases.shape, F32),
        ],
        scratch_shapes=[
            pltpu.SemaphoreType.DMA((n_dp,)),
            pltpu.SemaphoreType.DMA((n_dp,)),
        ],
        compiler_params=pltpu.CompilerParams(collective_id=0, has_side_effects=True),
        name="share_small",
    )(slices, biases)


def swap(values):
    return lax.ppermute(values, "tensor", [(0, 1), (1, 0)])


def per_device(
    tokens,
    grad_tokens,
    dealing,
    segment_ids,
    ln1_gain,
    ln1_bias,
    w_qkv,
    b_qv,
    w_out,
    b_out,
    ln2_gain,
    ln2_bias,
    w_up,
    b_up,
    w_down,
    b_down,
):
    n_dp = lax.axis_size("dp")
    t = lax.axis_index("tensor")
    rows, width = tokens.shape
    piece = ln1_gain.shape[0]
    half = b_qv.shape[1]
    hidden_half = b_up.shape[0]
    pairs = width // LANES

    def join(own, other, axis):
        return jnp.where(
            t == 0,
            jnp.concatenate([own, other], axis=axis),
            jnp.concatenate([other, own], axis=axis),
        )

    def mine_of(values, axis):
        size = values.shape[axis] // 2
        low, high = (
            lax.slice_in_dim(values, 0, size, axis=axis),
            lax.slice_in_dim(values, size, 2 * size, axis=axis),
        )
        return jnp.where(t == 0, low, high), jnp.where(t == 0, high, low)

    qkv_local = join(w_qkv, swap(w_qkv), 2)
    kv_local = (
        qkv_local[:, 1:].reshape(piece, 2, pairs, LANES).transpose(0, 2, 1, 3).reshape(piece, -1)
    )
    qkv_local = jnp.concatenate([qkv_local[:, 0], kv_local], axis=1)
    rest_local = jnp.concatenate([w_out.T, w_up, w_down.T], axis=1)
    other_rest = swap(rest_local)
    up_at, down_at = half, half + hidden_half
    rest_local = jnp.concatenate(
        [
            join(rest_local[:, :up_at], other_rest[:, :up_at], 1),
            join(rest_local[:, up_at:down_at], other_rest[:, up_at:down_at], 1),
            join(rest_local[:, down_at:], other_rest[:, down_at:], 1),
        ],
        axis=1,
    )
    wqkv = lax.all_gather(qkv_local, "dp", axis=0, tiled=True)
    rest = lax.all_gather(rest_local, "dp", axis=0, tiled=True)
    wout_t = rest[:, :width]
    wup = rest[:, width : width + 2 * hidden_half]
    wdown_t = rest[:, width + 2 * hidden_half :]
    wkv = wqkv[:, width:]
    wq = wqkv[:, :width]

    small = jnp.stack([ln1_gain, ln1_bias, b_out, ln2_gain, ln2_bias, b_down])
    small = jnp.pad(small, ((0, 2), (0, LANES - piece)))
    biases = jnp.concatenate([b_qv.reshape(-1), b_up])
    bias_rows = -(-biases.shape[0] // (8 * LANES)) * 8
    biases = jnp.pad(biases, (0, bias_rows * LANES - biases.shape[0]))
    biases = biases.reshape(bias_rows, LANES)
    small_all, other_biases = share_small(n_dp, small, biases)
    small_full = small_all[:, :6, :piece].transpose(1, 0, 2).reshape(6, width)
    flat, other_flat = biases.reshape(-1), other_biases.reshape(-1)
    bqv_full = join(flat[: 2 * half].reshape(2, half), other_flat[: 2 * half].reshape(2, half), 1)
    bup_full = join(
        flat[2 * half : 2 * half + hidden_half],
        other_flat[2 * half : 2 * half + hidden_half],
        0,
    )

    row_order = dealing[0]
    picks = (row_order[:, None] == jnp.arange(rows, dtype=jnp.int32)[None, :]).astype(BF16)
    sent_rows = mm(picks, tokens).astype(BF16)
    sent_grads = mm(picks, grad_tokens).astype(BF16)
    dealt = lax.all_to_all(sent_rows, "dp", split_axis=0, concat_axis=0, tiled=True)
    grad_out = lax.all_to_all(sent_grads, "dp", split_axis=0, concat_axis=0, tiled=True)
    dealt_of_pair = swap(dealt)
    joined = (segment_ids[:1] == segment_ids[-1:]).astype(jnp.int32)

    resid = dealt.astype(F32)
    ln_one, normed_one, factor_one = normalize(resid, small_full[0], small_full[1])
    ln_one = ln_one.astype(BF16)
    ln_of_pair = normalize(dealt_of_pair.astype(F32), small_full[0], small_full[1])[0].astype(BF16)
    kv_bias = jnp.stack(
        [jnp.zeros((pairs, LANES), F32), bqv_full[1].reshape(pairs, LANES)], axis=1
    ).reshape(-1)
    score_scale = HD**-0.5 * LOG2E
    shift = jnp.concatenate([bqv_full[0] * score_scale, kv_bias])
    scale = jnp.concatenate([jnp.full((width,), score_scale, F32), jnp.ones((2 * width,), F32)])
    qkv = (mm(ln_one, wqkv) * scale + shift).astype(BF16)
    kv_of_pair = (mm(ln_of_pair, wkv) + kv_bias).astype(BF16)
    attended, lse = attention(joined, qkv, kv_of_pair)
    hidden = resid + mm(attended, wout_t, 1, 1) + small_full[2]

    ln_two, normed_two, factor_two = normalize(hidden, small_full[3], small_full[4])
    ln_two = ln_two.astype(BF16)
    pre_act = mm(ln_two, wup) + bup_full
    activated, gelu_pull = jax.vjp(lambda values: jax.nn.gelu(values, approximate=True), pre_act)
    slope = gelu_pull(jnp.ones_like(pre_act))[0].astype(BF16)
    act = activated.astype(BF16)
    output = (hidden + mm(act, wdown_t, 1, 1) + small_full[5]).astype(BF16)

    grad_down_t = mm(grad_out, act, 0, 0).astype(BF16)
    grad_pre = (mm(grad_out, wdown_t) * slope.astype(F32)).astype(BF16)
    bias_up_grad = jnp.sum(grad_pre, axis=0, dtype=F32)
    grad_up = mm(ln_two, grad_pre, 0, 0).astype(BF16)
    grad_ln_two = mm(grad_pre, wup, 1, 1)
    grad_hidden = grad_out.astype(F32) + norm_back(
        grad_ln_two, normed_two, factor_two, small_full[3]
    )
    grad_branch = grad_hidden.astype(BF16)
    grad_wout_t = mm(grad_branch, attended, 0, 0).astype(BF16)
    grad_att = mm(grad_branch, wout_t).astype(BF16)

    pair_dq, pair_dkv = attention_back_pair(joined, qkv, kv_of_pair, grad_att, attended, lse)
    for_pair = swap(mm(pair_dkv, wkv, 1, 1).astype(BF16))
    dq, dkv = attention_back_own(qkv, grad_att, attended, lse, pair_dq)
    grad_wq = mm(ln_one, dq, 0, 0).astype(BF16)
    grad_wkv = (mm(ln_one, dkv, 0, 0) + mm(ln_of_pair, pair_dkv, 0, 0)).astype(BF16)
    bias_q_grad = jnp.sum(dq, axis=0, dtype=F32)
    kv_sum = jnp.sum(dkv, axis=0, dtype=F32) + jnp.sum(pair_dkv, axis=0, dtype=F32)
    bias_v_grad = kv_sum.reshape(pairs, 2, LANES)[:, 1].reshape(-1)
    grad_ln_one = mm(dq, wq, 1, 1) + mm(dkv, wkv, 1, 1) + for_pair.astype(F32)
    grad_input = (
        grad_hidden + norm_back(grad_ln_one, normed_one, factor_one, small_full[0])
    ).astype(BF16)

    def reduced(values):
        total = lax.psum_scatter(values, "dp", scatter_dimension=0, tiled=True)
        return total

    down_sum = reduced(grad_down_t)
    up_out_sum = reduced(jnp.concatenate([grad_up, grad_wout_t], axis=1))
    qkv_sum = reduced(jnp.concatenate([grad_wq, grad_wkv], axis=1))

    def paired(values):
        mine, other = mine_of(values, 1)
        return mine.astype(F32) + swap(other).astype(F32)

    down_part = paired(down_sum).T
    up_part = paired(up_out_sum[:, : 2 * hidden_half])
    wout_part = paired(up_out_sum[:, 2 * hidden_half :]).T
    q_part = paired(qkv_sum[:, :width])
    kv_part = paired(qkv_sum[:, width:])
    kv_part = kv_part.reshape(piece, pairs // 2, 2, LANES).transpose(0, 2, 1, 3)
    qkv_part = jnp.concatenate(
        [q_part.reshape(piece, 1, half), kv_part.reshape(piece, 2, half)], axis=1
    )

    small_grads = jnp.stack(
        [
            jnp.sum(grad_ln_one * normed_one, axis=0),
            jnp.sum(grad_ln_one, axis=0),
            jnp.sum(grad_hidden, axis=0),
            jnp.sum(grad_ln_two * normed_two, axis=0),
            jnp.sum(grad_ln_two, axis=0),
            jnp.sum(grad_out, axis=0, dtype=F32),
            bias_q_grad,
            bias_v_grad,
        ]
    )
    small_total, up_total = lax.psum((small_grads, bias_up_grad), ("dp", "tensor"))
    small_part = lax.dynamic_slice_in_dim(
        small_total[:6], lax.axis_index("dp") * piece, piece, 1
    )
    qv_part = mine_of(small_total[6:], 1)[0]
    bias_up_part = mine_of(up_total, 0)[0]

    sent_out = lax.all_to_all(output, "dp", split_axis=0, concat_axis=0, tiled=True)
    sent_grad = lax.all_to_all(grad_input, "dp", split_axis=0, concat_axis=0, tiled=True)
    restored_out = mm(picks, sent_out, 0, 0).astype(BF16)
    restored_grad = mm(picks, sent_grad, 0, 0).astype(BF16)
    return (
        restored_out,
        restored_grad,
        small_part[0],
        small_part[1],
        qkv_part,
        qv_part,
        wout_part,
        small_part[2],
        small_part[3],
        small_part[4],
        up_part,
        bias_up_part,
        down_part,
        small_part[5],
    )


def solution(mesh):
    placed = (
        P(("dp", "tensor"), None),
        P(("dp", "tensor"), None),
        P(("dp", "tensor"), None),
        P("dp"),
        P("dp"),
        P("dp"),
        P("dp", None, "tensor"),
        P(None, "tensor"),
        P("tensor", "dp"),
        P("dp"),
        P("dp"),
        P("dp"),
        P("dp", "tensor"),
        P("tensor"),
        P("tensor", "dp"),
        P("dp"),
    )
    return jax.shard_map(
        per_device,
        mesh=mesh,
        in_specs=placed,
        out_specs=(
            P(("dp", "tensor"), None),
            P(("dp", "tensor"), None),
            P("dp"),
            P("dp"),
            P("dp", None, "tensor"),
            P(None, "tensor"),
            P("tensor", "dp"),
            P("dp"),
            P("dp"),
            P("dp"),
            P("dp", "tensor"),
            P("tensor"),
            P("tensor", "dp"),
            P("dp"),
        ),
        check_vma=False,
    )
```

```python
import functools

import jax
import jax.numpy as jnp
from jax import lax
from jax.experimental import pallas as pl
from jax.experimental.pallas import tpu as pltpu
from jax.sharding import PartitionSpec as P


HD = 64
LANES = 128
EPS = 1e-06
LN2 = 0.6931471805599453
LOG2E = 1.4426950408889634
F32 = jnp.float32
BF16 = jnp.bfloat16


def normalize(values, gain_row, bias_row):
    centred = values - jnp.mean(values, axis=-1, keepdims=True)
    factor = lax.rsqrt(jnp.mean(centred * centred, axis=-1, keepdims=True) + EPS)
    normed = centred * factor
    return (normed * gain_row + bias_row, normed, factor)


def norm_back(grad_rows, normed, factor, gain_row):
    scaled = grad_rows * gain_row
    centred = scaled - jnp.mean(scaled, axis=-1, keepdims=True)
    return factor * (centred - normed * jnp.mean(scaled * normed, axis=-1, keepdims=True))


def mm(left, right, left_dim=1, right_dim=0):
    return lax.dot_general(
        left, right, (((left_dim,), (right_dim,)), ((), ())), preferred_element_type=F32
    )


def head_lanes(head):
    return (lax.broadcasted_iota(jnp.int32, (1, LANES), 1) // HD) == head


def attend_rows(q, keys, values):
    outs, lses = [], []
    one = jnp.ones((), BF16)
    for head in range(2):
        mine = head_lanes(head)
        scores = mm(jnp.where(mine, q, jnp.zeros_like(q)), keys, 1, 1)
        row_max = jnp.max(scores, axis=1, keepdims=True)
        weights = jnp.exp2(scores - row_max).astype(BF16)
        mixed = mm(weights, jnp.where(mine, values, one))
        total = jnp.sum(jnp.where(mine, 0.0, mixed), axis=1, keepdims=True) * (1.0 / HD)
        outs.append(mixed / total)
        lses.append(row_max + jnp.log2(total))
    first = head_lanes(0)
    return (jnp.where(first, outs[0], outs[1]), jnp.where(first, lses[0], lses[1]))


def own_forward(q_ref, kv_ref, mixed_ref, lse_ref, *, qblock):
    for block in range(q_ref.shape[0] // qblock):
        rows = pl.ds(block * qblock, qblock)
        mixed, lse = attend_rows(q_ref[rows, :], kv_ref[:, :LANES], kv_ref[:, LANES:])
        mixed_ref[rows, :] = mixed
        lse_ref[rows, :] = lse


def pair_forward(joined_ref, q_ref, kv_ref, own_ref, own_lse_ref, mixed_ref, lse_ref, *, qblock):
    joined = joined_ref[0] > 0

    @pl.when(joined)
    def _():
        for block in range(q_ref.shape[0] // qblock):
            rows = pl.ds(block * qblock, qblock)
            mixed, lse = attend_rows(q_ref[rows, :], kv_ref[:, :LANES], kv_ref[:, LANES:])
            own_lse = own_lse_ref[rows, :]
            top = jnp.maximum(own_lse, lse)
            own_share = jnp.exp2(own_lse - top)
            pair_share = jnp.exp2(lse - top)
            total = own_share + pair_share
            mixed_ref[rows, :] = (
                (own_ref[rows, :] * own_share + mixed * pair_share) / total
            ).astype(BF16)
            lse_ref[rows, :] = top + jnp.log2(total)

    @pl.when(jnp.logical_not(joined))
    def _():
        mixed_ref[...] = own_ref[...].astype(BF16)
        lse_ref[...] = own_lse_ref[...]


def split_three(values):
    high = values.astype(BF16)
    rest = values - high.astype(F32)
    middle = rest.astype(BF16)
    return high, middle, (rest - middle.astype(F32)).astype(BF16)


def attend_back(q_ref, grad_ref, mixed_ref, lse_ref, kv_ref, dkv_ref, dq_sum, kblock):
    lane = lax.broadcasted_iota(jnp.int32, (1, LANES), 1)
    q = q_ref[...]
    grad = grad_ref[...]
    products = grad.astype(F32) * mixed_ref[...].astype(F32)
    wide_q, wide_grad = [], []
    for head in range(2):
        mine = head_lanes(head)
        spare = (1 - head) * HD
        inner = jnp.sum(jnp.where(mine, products, 0.0), axis=1, keepdims=True)
        lse_parts = split_three(-lse_ref[:, head * HD : head * HD + 1])
        inner_parts = split_three(-inner)
        q_head = jnp.where(mine, q, jnp.zeros_like(q))
        grad_head = jnp.where(mine, grad, jnp.zeros_like(grad))
        for part in range(3):
            q_head = jnp.where(lane == spare + part, lse_parts[part], q_head)
            grad_head = jnp.where(lane == spare + part, inner_parts[part], grad_head)
        wide_q.append(q_head)
        wide_grad.append(grad_head)
    one = jnp.ones((), BF16)
    first = head_lanes(0)
    for block in range(kv_ref.shape[0] // kblock):
        rows = pl.ds(block * kblock, kblock)
        keys = kv_ref[rows, :LANES]
        values = kv_ref[rows, LANES:]
        key_grads, value_grads = [], []
        for head in range(2):
            mine = head_lanes(head)
            weights = jnp.exp2(mm(jnp.where(mine, keys, one), wide_q[head], 1, 1))
            grad_weights = mm(jnp.where(mine, values, one), wide_grad[head], 1, 1)
            grad_scores = (weights * grad_weights).astype(BF16)
            value_grads.append(mm(weights.astype(BF16), grad))
            key_grads.append(mm(grad_scores, q))
            dq_sum[head] += mm(keys, grad_scores, 0, 0)
        dkv_ref[rows, :LANES] = (jnp.where(first, key_grads[0], key_grads[1]) * LN2).astype(BF16)
        dkv_ref[rows, LANES:] = jnp.where(first, value_grads[0], value_grads[1]).astype(BF16)


def query_grad(dq_sum):
    return jnp.concatenate([dq_sum[0, :HD, :], dq_sum[1, HD:, :]], axis=0)


def pair_backward(
    joined_ref, q_ref, grad_ref, mixed_ref, lse_ref, kv_ref, dq_ref, dkv_ref, dq_sum, *, kblock
):
    joined = joined_ref[0] > 0
    dq_sum[...] = jnp.zeros_like(dq_sum)

    @pl.when(joined)
    def _():
        attend_back(q_ref, grad_ref, mixed_ref, lse_ref, kv_ref, dkv_ref, dq_sum, kblock)

    @pl.when(jnp.logical_not(joined))
    def _():
        dkv_ref[...] = jnp.zeros_like(dkv_ref)

    dq_ref[...] = query_grad(dq_sum)


def own_backward(
    q_ref, grad_ref, mixed_ref, lse_ref, kv_ref, pair_dq_ref, dq_ref, dkv_ref, dq_sum, *, kblock
):
    dq_sum[...] = jnp.zeros_like(dq_sum)
    attend_back(q_ref, grad_ref, mixed_ref, lse_ref, kv_ref, dkv_ref, dq_sum, kblock)
    total = query_grad(dq_sum) + pair_dq_ref[...]
    dq_ref[...] = (total.T * HD**-0.5).astype(BF16)


def params(**extra):
    return pltpu.CompilerParams(vmem_limit_bytes=56 << 20, **extra)


def cost(rows, keys, width, products):
    return pl.CostEstimate(
        flops=2 * rows * keys * width * products * 4,
        bytes_accessed=2 * width * (rows + 2 * keys),
        transcendentals=rows * keys * width // HD,
    )


def attention_own(qkv):
    rows = qkv.shape[0]
    width = qkv.shape[1] // 3
    pairs = width // LANES
    column = pl.BlockSpec((rows, LANES), lambda p: (0, p))
    own_kv = pl.BlockSpec((rows, 2 * LANES), lambda p: (0, pairs // 2 + p))
    shape = jax.ShapeDtypeStruct((rows, width), F32)
    return pl.pallas_call(
        functools.partial(own_forward, qblock=min(512, rows)),
        grid=(pairs,),
        in_specs=[column, own_kv],
        out_specs=[column, column],
        out_shape=[shape, shape],
        compiler_params=params(),
        cost_estimate=cost(rows, rows, width, 2),
        name="attend_own",
    )(qkv, qkv)


def attention_pair(joined, qkv, kv_of_pair, own, own_lse):
    rows, width = own.shape
    pairs = width // LANES
    column = pl.BlockSpec((rows, LANES), lambda p: (0, p))
    pair_kv = pl.BlockSpec((rows, 2 * LANES), lambda p: (0, p))
    return pl.pallas_call(
        functools.partial(pair_forward, qblock=min(512, rows)),
        grid=(pairs,),
        in_specs=[pl.BlockSpec(memory_space=pltpu.SMEM), column, pair_kv, column, column],
        out_specs=[column, column],
        out_shape=[
            jax.ShapeDtypeStruct((rows, width), BF16),
            jax.ShapeDtypeStruct((rows, width), F32),
        ],
        compiler_params=params(),
        cost_estimate=cost(rows, rows, width, 2),
        name="attend_pair",
    )(joined, qkv, kv_of_pair, own, own_lse)


def attention_back_pair(joined, qkv, kv_of_pair, grad, mixed, lse):
    rows, width = grad.shape
    pairs = width // LANES
    column = pl.BlockSpec((rows, LANES), lambda p: (0, p))
    pair_kv = pl.BlockSpec((rows, 2 * LANES), lambda p: (0, p))
    across = pl.BlockSpec((LANES, rows), lambda p: (p, 0))
    return pl.pallas_call(
        functools.partial(pair_backward, kblock=min(512, rows)),
        grid=(pairs,),
        in_specs=[pl.BlockSpec(memory_space=pltpu.SMEM)] + [column] * 4 + [pair_kv],
        out_specs=[across, pair_kv],
        out_shape=[
            jax.ShapeDtypeStruct((width, rows), F32),
            jax.ShapeDtypeStruct((rows, 2 * width), BF16),
        ],
        scratch_shapes=[pltpu.VMEM((2, LANES, rows), F32)],
        compiler_params=params(),
        cost_estimate=cost(rows, rows, width, 5),
        name="attend_back_pair",
    )(joined, qkv, grad, mixed, lse, kv_of_pair)


def attention_back_own(qkv, grad, mixed, lse, pair_dq):
    rows, width = grad.shape
    pairs = width // LANES
    column = pl.BlockSpec((rows, LANES), lambda p: (0, p))
    own_kv = pl.BlockSpec((rows, 2 * LANES), lambda p: (0, pairs // 2 + p))
    kv_out = pl.BlockSpec((rows, 2 * LANES), lambda p: (0, p))
    across = pl.BlockSpec((LANES, rows), lambda p: (p, 0))
    return pl.pallas_call(
        functools.partial(own_backward, kblock=min(512, rows)),
        grid=(pairs,),
        in_specs=[column] * 4 + [own_kv, across],
        out_specs=[column, kv_out],
        out_shape=[
            jax.ShapeDtypeStruct((rows, width), BF16),
            jax.ShapeDtypeStruct((rows, 2 * width), BF16),
        ],
        scratch_shapes=[pltpu.VMEM((2, LANES, rows), F32)],
        compiler_params=params(),
        cost_estimate=cost(rows, rows, width, 5),
        name="attend_back_own",
    )(qkv, grad, mixed, lse, qkv, pair_dq)


def small_kernel(n_dp, slice_ref, bias_ref, all_ref, partner_ref, send_sem, recv_sem):
    me = lax.axis_index("dp")
    t = lax.axis_index("tensor")

    barrier = pltpu.get_barrier_semaphore()

    def greet(step, carry):
        peer = lax.rem(me + step, n_dp)
        pl.semaphore_signal(
            barrier, inc=1, device_id=(peer, t), device_id_type=pl.DeviceIdType.MESH
        )
        return carry

    lax.fori_loop(1, n_dp, greet, 0)
    pl.semaphore_signal(
        barrier, inc=1, device_id=(me, 1 - t), device_id_type=pl.DeviceIdType.MESH
    )
    pl.semaphore_wait(barrier, n_dp)

    def to_peer(step):
        return pltpu.make_async_remote_copy(
            src_ref=slice_ref,
            dst_ref=all_ref.at[me],
            send_sem=send_sem.at[step],
            recv_sem=recv_sem.at[step],
            device_id=(lax.rem(me + step, n_dp), t),
            device_id_type=pl.DeviceIdType.MESH,
        )

    to_partner = pltpu.make_async_remote_copy(
        src_ref=bias_ref,
        dst_ref=partner_ref,
        send_sem=send_sem.at[0],
        recv_sem=recv_sem.at[0],
        device_id=(me, 1 - t),
        device_id_type=pl.DeviceIdType.MESH,
    )
    to_partner.start()

    def start(step, carry):
        to_peer(step).start()
        return carry

    def finish(step, carry):
        to_peer(step).wait()
        return carry

    lax.fori_loop(1, n_dp, start, 0)
    all_ref[me] = slice_ref[...]
    lax.fori_loop(1, n_dp, finish, 0)
    to_partner.wait()


def share_small(n_dp, slices, biases):
    vmem = pl.BlockSpec(memory_space=pltpu.VMEM)
    return pl.pallas_call(
        functools.partial(small_kernel, n_dp),
        in_specs=[vmem, vmem],
        out_specs=[vmem, vmem],
        out_shape=[
            jax.ShapeDtypeStruct((n_dp,) + slices.shape, F32),
            jax.ShapeDtypeStruct(biases.shape, F32),
        ],
        scratch_shapes=[
            pltpu.SemaphoreType.DMA((n_dp,)),
            pltpu.SemaphoreType.DMA((n_dp,)),
        ],
        compiler_params=pltpu.CompilerParams(collective_id=0, has_side_effects=True),
        name="share_small",
    )(slices, biases)


def sum_small_kernel(
    n_dp, parts_ref, total_ref, bias_ref, landed, pair_sum, pair_in, own_bias, send_sem, recv_sem
):
    me = lax.axis_index("dp")
    t = lax.axis_index("tensor")
    mesh_id = pl.DeviceIdType.MESH

    barrier = pltpu.get_barrier_semaphore()

    def greet(step, carry):
        pl.semaphore_signal(
            barrier, inc=1, device_id=(lax.rem(me + step, n_dp), t), device_id_type=mesh_id
        )
        return carry

    lax.fori_loop(1, n_dp, greet, 0)
    pl.semaphore_signal(barrier, inc=1, device_id=(me, 1 - t), device_id_type=mesh_id)
    pl.semaphore_wait(barrier, n_dp)

    def part_to(step):
        peer = lax.rem(me + step, n_dp)
        return pltpu.make_async_remote_copy(
            src_ref=parts_ref.at[peer],
            dst_ref=landed.at[step],
            send_sem=send_sem.at[0, step],
            recv_sem=recv_sem.at[0, step],
            device_id=(peer, t),
            device_id_type=mesh_id,
        )

    def bias_to(step):
        return pltpu.make_async_remote_copy(
            src_ref=own_bias,
            dst_ref=bias_ref.at[me],
            send_sem=send_sem.at[1, step],
            recv_sem=recv_sem.at[1, step],
            device_id=(lax.rem(me + step, n_dp), t),
            device_id_type=mesh_id,
        )

    def start_part(step, carry):
        part_to(step).start()
        return carry

    def add_part(step, carry):
        part_to(step).wait()
        return carry + landed[step]

    lax.fori_loop(1, n_dp, start_part, 0)
    pair_sum[...] = lax.fori_loop(1, n_dp, add_part, parts_ref[me])
    to_partner = pltpu.make_async_remote_copy(
        src_ref=pair_sum,
        dst_ref=pair_in,
        send_sem=send_sem.at[1, 0],
        recv_sem=recv_sem.at[1, 0],
        device_id=(me, 1 - t),
        device_id_type=mesh_id,
    )
    to_partner.start()
    to_partner.wait()
    total = pair_sum[...] + pair_in[...]
    total_ref[...] = total
    own_bias[...] = total[:8]
    bias_ref[me] = total[:8]

    def start_bias(step, carry):
        bias_to(step).start()
        return carry

    def finish_bias(step, carry):
        bias_to(step).wait()
        return carry

    lax.fori_loop(1, n_dp, start_bias, 0)
    lax.fori_loop(1, n_dp, finish_bias, 0)


def sum_small(n_dp, parts):
    vmem = pl.BlockSpec(memory_space=pltpu.VMEM)
    block = parts.shape[1:]
    return pl.pallas_call(
        functools.partial(sum_small_kernel, n_dp),
        in_specs=[vmem],
        out_specs=[vmem, vmem],
        out_shape=[
            jax.ShapeDtypeStruct(block, F32),
            jax.ShapeDtypeStruct((n_dp, 8, LANES), F32),
        ],
        scratch_shapes=[
            pltpu.VMEM(parts.shape, F32),
            pltpu.VMEM(block, F32),
            pltpu.VMEM(block, F32),
            pltpu.VMEM((8, LANES), F32),
            pltpu.SemaphoreType.DMA((2, n_dp)),
            pltpu.SemaphoreType.DMA((2, n_dp)),
        ],
        compiler_params=pltpu.CompilerParams(collective_id=1, has_side_effects=True),
        name="sum_small",
    )(parts)


def after(*values):
    return lax.optimization_barrier(values)


def swap(values):
    return lax.ppermute(values, "tensor", [(0, 1), (1, 0)])


def per_device(
    tokens,
    grad_tokens,
    dealing,
    segment_ids,
    ln1_gain,
    ln1_bias,
    w_qkv,
    b_qv,
    w_out,
    b_out,
    ln2_gain,
    ln2_bias,
    w_up,
    b_up,
    w_down,
    b_down,
):
    n_dp = lax.axis_size("dp")
    t = lax.axis_index("tensor")
    rows, width = tokens.shape
    piece = ln1_gain.shape[0]
    half = b_qv.shape[1]
    hidden_half = b_up.shape[0]
    pairs = width // LANES

    def join(own, other, axis):
        return jnp.where(
            t == 0,
            jnp.concatenate([own, other], axis=axis),
            jnp.concatenate([other, own], axis=axis),
        )

    def reduced(values):
        return lax.psum_scatter(values, "dp", scatter_dimension=0, tiled=True)

    def mine_of(values, axis):
        size = values.shape[axis] // 2
        low, high = (
            lax.slice_in_dim(values, 0, size, axis=axis),
            lax.slice_in_dim(values, size, 2 * size, axis=axis),
        )
        return jnp.where(t == 0, low, high), jnp.where(t == 0, high, low)

    qkv_local = join(w_qkv, swap(w_qkv), 2)
    kv_local = (
        qkv_local[:, 1:].reshape(piece, 2, pairs, LANES).transpose(0, 2, 1, 3).reshape(piece, -1)
    )
    qkv_local = jnp.concatenate([qkv_local[:, 0], kv_local], axis=1)
    rest_local = jnp.concatenate([w_out.T, w_up, w_down.T], axis=1)
    other_rest = swap(rest_local)
    up_at, down_at = half, half + hidden_half
    rest_local = jnp.concatenate(
        [
            join(rest_local[:, :up_at], other_rest[:, :up_at], 1),
            join(rest_local[:, up_at:down_at], other_rest[:, up_at:down_at], 1),
            join(rest_local[:, down_at:], other_rest[:, down_at:], 1),
        ],
        axis=1,
    )
    wqkv = lax.all_gather(qkv_local, "dp", axis=0, tiled=True)
    rest = lax.all_gather(rest_local, "dp", axis=0, tiled=True)
    wout_t = rest[:, :width]
    wup = rest[:, width : width + 2 * hidden_half]
    wdown_t = rest[:, width + 2 * hidden_half :]
    wkv = wqkv[:, width:]
    wq = wqkv[:, :width]

    small = jnp.stack([ln1_gain, ln1_bias, b_out, ln2_gain, ln2_bias, b_down])
    small = jnp.pad(small, ((0, 2), (0, LANES - piece)))
    biases = jnp.concatenate([b_qv.reshape(-1), b_up])
    bias_rows = -(-biases.shape[0] // (8 * LANES)) * 8
    biases = jnp.pad(biases, (0, bias_rows * LANES - biases.shape[0]))
    biases = biases.reshape(bias_rows, LANES)
    small_all, other_biases = share_small(n_dp, small, biases)
    row_order = dealing[0]
    picks = (row_order[:, None] == jnp.arange(rows, dtype=jnp.int32)[None, :]).astype(BF16)
    sent_rows = mm(picks, tokens).astype(BF16)
    sent_rows, small_all = after(sent_rows, small_all)
    dealt = lax.all_to_all(sent_rows, "dp", split_axis=0, concat_axis=0, tiled=True)
    grad_tokens, dealt = after(grad_tokens, dealt)
    sent_grads = mm(picks, grad_tokens).astype(BF16)
    grad_out = lax.all_to_all(sent_grads, "dp", split_axis=0, concat_axis=0, tiled=True)
    dealt_of_pair = swap(dealt)
    joined = (segment_ids[:1] == segment_ids[-1:]).astype(jnp.int32)

    small_full = small_all[:, :6, :piece].transpose(1, 0, 2).reshape(6, width)
    flat, other_flat = biases.reshape(-1), other_biases.reshape(-1)
    bqv_full = join(flat[: 2 * half].reshape(2, half), other_flat[: 2 * half].reshape(2, half), 1)
    bup_full = join(
        flat[2 * half : 2 * half + hidden_half],
        other_flat[2 * half : 2 * half + hidden_half],
        0,
    )

    resid = dealt.astype(F32)
    ln_one, normed_one, factor_one = normalize(resid, small_full[0], small_full[1])
    ln_one = ln_one.astype(BF16)
    kv_bias = jnp.stack(
        [jnp.zeros((pairs, LANES), F32), bqv_full[1].reshape(pairs, LANES)], axis=1
    ).reshape(-1)
    score_scale = HD**-0.5 * LOG2E
    shift = jnp.concatenate([bqv_full[0] * score_scale, kv_bias])
    scale = jnp.concatenate([jnp.full((width,), score_scale, F32), jnp.ones((2 * width,), F32)])
    qkv = (mm(ln_one, wqkv) * scale + shift).astype(BF16)
    own, own_lse = attention_own(qkv)
    dealt_of_pair, own = after(dealt_of_pair, own)
    ln_of_pair = normalize(dealt_of_pair.astype(F32), small_full[0], small_full[1])[0].astype(BF16)
    kv_of_pair = (mm(ln_of_pair, wkv) + kv_bias).astype(BF16)
    attended, lse = attention_pair(joined, qkv, kv_of_pair, own, own_lse)
    hidden = resid + mm(attended, wout_t, 1, 1) + small_full[2]

    ln_two, normed_two, factor_two = normalize(hidden, small_full[3], small_full[4])
    ln_two = ln_two.astype(BF16)
    pre_act = mm(ln_two, wup) + bup_full
    activated, gelu_pull = jax.vjp(lambda values: jax.nn.gelu(values, approximate=True), pre_act)
    slope = gelu_pull(jnp.ones_like(pre_act))[0].astype(BF16)
    act, slope = after(activated.astype(BF16), slope)
    output = (hidden + mm(act, wdown_t, 1, 1) + small_full[5]).astype(BF16)

    grad_down_t = mm(grad_out, act, 0, 0).astype(BF16)
    grad_pre = (mm(grad_out, wdown_t) * slope.astype(F32)).astype(BF16)
    bias_up_grad = jnp.sum(grad_pre, axis=0, dtype=F32)
    grad_up = mm(ln_two, grad_pre, 0, 0).astype(BF16)
    grad_down_t, grad_up, grad_pre = after(grad_down_t, grad_up, grad_pre)
    grad_ln_two = mm(grad_pre, wup, 1, 1)
    grad_hidden = grad_out.astype(F32) + norm_back(
        grad_ln_two, normed_two, factor_two, small_full[3]
    )
    grad_branch = grad_hidden.astype(BF16)
    grad_wout_t = mm(grad_branch, attended, 0, 0).astype(BF16)
    mlp_grads = jnp.concatenate([grad_down_t, grad_up, grad_wout_t], axis=1)
    grad_att = mm(grad_branch, wout_t).astype(BF16)
    grad_att, mlp_grads, output = after(grad_att, mlp_grads, output)
    mlp_sum = reduced(mlp_grads)

    pair_dq, pair_dkv = attention_back_pair(
        joined, qkv, kv_of_pair, grad_att, attended, lse
    )
    for_pair = mm(pair_dkv, wkv, 1, 1).astype(BF16)
    for_pair = swap(for_pair)
    dq, dkv = attention_back_own(qkv, grad_att, attended, lse, pair_dq)
    grad_wq = mm(ln_one, dq, 0, 0).astype(BF16)
    grad_wkv = (mm(ln_one, dkv, 0, 0) + mm(ln_of_pair, pair_dkv, 0, 0)).astype(BF16)
    bias_q_grad = jnp.sum(dq, axis=0, dtype=F32)
    kv_sum = jnp.sum(dkv, axis=0, dtype=F32) + jnp.sum(pair_dkv, axis=0, dtype=F32)
    bias_v_grad = kv_sum.reshape(pairs, 2, LANES)[:, 1].reshape(-1)
    grad_ln_one = mm(dq, wq, 1, 1) + mm(dkv, wkv, 1, 1) + for_pair.astype(F32)
    grad_input = (
        grad_hidden + norm_back(grad_ln_one, normed_one, factor_one, small_full[0])
    ).astype(BF16)

    qkv_sum = reduced(jnp.concatenate([grad_wq, grad_wkv], axis=1))

    def paired(values, sizes):
        columns, start = [], 0
        for size in sizes:
            columns.append(mine_of(values[:, start : start + size], 1))
            start += size
        mine = jnp.concatenate([c[0] for c in columns], axis=1)
        other = jnp.concatenate([c[1] for c in columns], axis=1)
        total = mine.astype(F32) + swap(other).astype(F32)
        cuts = [sum(sizes[:i]) // 2 for i in range(1, len(sizes))]
        return jnp.split(total, cuts, axis=1)

    down_part, up_part, wout_part = paired(mlp_sum, (2 * hidden_half, 2 * hidden_half, width))
    down_part, wout_part = down_part.T, wout_part.T
    q_part, kv_part = paired(qkv_sum, (width, 2 * width))
    kv_part = kv_part.reshape(piece, pairs // 2, 2, LANES).transpose(0, 2, 1, 3)
    qkv_part = jnp.concatenate(
        [q_part.reshape(piece, 1, half), kv_part.reshape(piece, 2, half)], axis=1
    )

    row_sums = jnp.concatenate(
        [
            jnp.stack([bias_q_grad, bias_v_grad]),
            bias_up_grad.reshape(-1, width),
            jnp.zeros((2, width), F32),
            jnp.stack(
                [
                    jnp.sum(grad_ln_one * normed_one, axis=0),
                    jnp.sum(grad_ln_one, axis=0),
                    jnp.sum(grad_hidden, axis=0),
                    jnp.sum(grad_ln_two * normed_two, axis=0),
                    jnp.sum(grad_ln_two, axis=0),
                    jnp.sum(grad_out, axis=0, dtype=F32),
                ]
            ),
            jnp.zeros((2, width), F32),
        ]
    )
    row_sums = row_sums.reshape(16, n_dp, piece).transpose(1, 0, 2)
    row_sums = jnp.pad(row_sums, ((0, 0), (0, 0), (0, LANES - piece)))
    slice_total, bias_total = sum_small(n_dp, row_sums)
    small_part = slice_total[8:14, :piece]
    bias_total = bias_total[:, :6, :piece].transpose(1, 0, 2).reshape(6, width)
    qv_part = mine_of(bias_total[:2], 1)[0]
    bias_up_part = mine_of(bias_total[2:].reshape(-1), 0)[0]

    sent_out = lax.all_to_all(output, "dp", split_axis=0, concat_axis=0, tiled=True)
    sent_grad = lax.all_to_all(grad_input, "dp", split_axis=0, concat_axis=0, tiled=True)
    restored_out = mm(picks, sent_out, 0, 0).astype(BF16)
    restored_grad = mm(picks, sent_grad, 0, 0).astype(BF16)
    return (
        restored_out,
        restored_grad,
        small_part[0],
        small_part[1],
        qkv_part,
        qv_part,
        wout_part,
        small_part[2],
        small_part[3],
        small_part[4],
        up_part,
        bias_up_part,
        down_part,
        small_part[5],
    )


def solution(mesh):
    placed = (
        P(("dp", "tensor"), None),
        P(("dp", "tensor"), None),
        P(("dp", "tensor"), None),
        P("dp"),
        P("dp"),
        P("dp"),
        P("dp", None, "tensor"),
        P(None, "tensor"),
        P("tensor", "dp"),
        P("dp"),
        P("dp"),
        P("dp"),
        P("dp", "tensor"),
        P("tensor"),
        P("tensor", "dp"),
        P("dp"),
    )

    return jax.shard_map(
        per_device,
        mesh=mesh,
        in_specs=placed,
        out_specs=(
            P(("dp", "tensor"), None),
            P(("dp", "tensor"), None),
            P("dp"),
            P("dp"),
            P("dp", None, "tensor"),
            P(None, "tensor"),
            P("tensor", "dp"),
            P("dp"),
            P("dp"),
            P("dp"),
            P("dp", "tensor"),
            P("tensor"),
            P("tensor", "dp"),
            P("dp"),
        ),
        check_vma=False,
    )
```

```python
import functools

import jax
import jax.numpy as jnp
from jax import lax
from jax.experimental import pallas as pl
from jax.experimental.pallas import tpu as pltpu
from jax.sharding import PartitionSpec as P


HD = 64
LANES = 128
EPS = 1e-06
LN2 = 0.6931471805599453
LOG2E = 1.4426950408889634
GELU_ONE = 0.7978845608028654
GELU_THREE = 0.7978845608028654 * 0.044715
F32 = jnp.float32
BF16 = jnp.bfloat16


def normalize(values, gain_row, bias_row):
    centred = values - jnp.mean(values, axis=-1, keepdims=True)
    factor = lax.rsqrt(jnp.mean(centred * centred, axis=-1, keepdims=True) + EPS)
    normed = centred * factor
    return (normed * gain_row + bias_row, normed, factor)


def norm_back(grad_rows, normed, factor, gain_row):
    scaled = grad_rows * gain_row
    centred = scaled - jnp.mean(scaled, axis=-1, keepdims=True)
    return factor * (centred - normed * jnp.mean(scaled * normed, axis=-1, keepdims=True))


def mm(left, right, left_dim=1, right_dim=0):
    return lax.dot_general(
        left, right, (((left_dim,), (right_dim,)), ((), ())), preferred_element_type=F32
    )


def head_lanes(head):
    return (lax.broadcasted_iota(jnp.int32, (1, LANES), 1) // HD) == head


def attend_rows(q, keys, values):
    outs, lses = [], []
    one = jnp.ones((), BF16)
    for head in range(2):
        mine = head_lanes(head)
        scores = mm(jnp.where(mine, q, jnp.zeros_like(q)), keys, 1, 1)
        row_max = jnp.max(scores, axis=1, keepdims=True)
        weights = jnp.exp2(scores - row_max).astype(BF16)
        mixed = mm(weights, jnp.where(mine, values, one))
        total = jnp.sum(jnp.where(mine, 0.0, mixed), axis=1, keepdims=True) * (1.0 / HD)
        outs.append(mixed / total)
        lses.append(row_max + jnp.log2(total))
    first = head_lanes(0)
    return (jnp.where(first, outs[0], outs[1]), jnp.where(first, lses[0], lses[1]))


def own_forward(q_ref, kv_ref, mixed_ref, lse_ref, *, qblock):
    for block in range(q_ref.shape[0] // qblock):
        rows = pl.ds(block * qblock, qblock)
        mixed, lse = attend_rows(q_ref[rows, :], kv_ref[:, :LANES], kv_ref[:, LANES:])
        mixed_ref[rows, :] = mixed
        lse_ref[rows, :] = lse


def pair_forward(joined_ref, q_ref, kv_ref, own_ref, own_lse_ref, mixed_ref, lse_ref, *, qblock):
    joined = joined_ref[0] > 0

    @pl.when(joined)
    def _():
        for block in range(q_ref.shape[0] // qblock):
            rows = pl.ds(block * qblock, qblock)
            mixed, lse = attend_rows(q_ref[rows, :], kv_ref[:, :LANES], kv_ref[:, LANES:])
            own_lse = own_lse_ref[rows, :]
            top = jnp.maximum(own_lse, lse)
            own_share = jnp.exp2(own_lse - top)
            pair_share = jnp.exp2(lse - top)
            total = own_share + pair_share
            mixed_ref[rows, :] = (
                (own_ref[rows, :] * own_share + mixed * pair_share) / total
            ).astype(BF16)
            lse_ref[rows, :] = top + jnp.log2(total)

    @pl.when(jnp.logical_not(joined))
    def _():
        mixed_ref[...] = own_ref[...].astype(BF16)
        lse_ref[...] = own_lse_ref[...]


def split_three(values):
    high = values.astype(BF16)
    rest = values - high.astype(F32)
    middle = rest.astype(BF16)
    return high, middle, (rest - middle.astype(F32)).astype(BF16)


def attend_back(q_ref, grad_ref, mixed_ref, lse_ref, kv_ref, dkv_ref, dq_sum, kblock):
    lane = lax.broadcasted_iota(jnp.int32, (1, LANES), 1)
    q = q_ref[...]
    grad = grad_ref[...]
    products = grad.astype(F32) * mixed_ref[...].astype(F32)
    wide_q, wide_grad = [], []
    for head in range(2):
        mine = head_lanes(head)
        spare = (1 - head) * HD
        inner = jnp.sum(jnp.where(mine, products, 0.0), axis=1, keepdims=True)
        lse_parts = split_three(-lse_ref[:, head * HD : head * HD + 1])
        inner_parts = split_three(-inner)
        q_head = jnp.where(mine, q, jnp.zeros_like(q))
        grad_head = jnp.where(mine, grad, jnp.zeros_like(grad))
        for part in range(3):
            q_head = jnp.where(lane == spare + part, lse_parts[part], q_head)
            grad_head = jnp.where(lane == spare + part, inner_parts[part], grad_head)
        wide_q.append(q_head)
        wide_grad.append(grad_head)
    one = jnp.ones((), BF16)
    first = head_lanes(0)
    for block in range(kv_ref.shape[0] // kblock):
        rows = pl.ds(block * kblock, kblock)
        keys = kv_ref[rows, :LANES]
        values = kv_ref[rows, LANES:]
        key_grads, value_grads = [], []
        for head in range(2):
            mine = head_lanes(head)
            weights = jnp.exp2(mm(jnp.where(mine, keys, one), wide_q[head], 1, 1))
            grad_weights = mm(jnp.where(mine, values, one), wide_grad[head], 1, 1)
            grad_scores = (weights * grad_weights).astype(BF16)
            value_grads.append(mm(weights.astype(BF16), grad))
            key_grads.append(mm(grad_scores, q))
            dq_sum[head] += mm(keys, grad_scores, 0, 0)
        dkv_ref[rows, :LANES] = (jnp.where(first, key_grads[0], key_grads[1]) * LN2).astype(BF16)
        dkv_ref[rows, LANES:] = jnp.where(first, value_grads[0], value_grads[1]).astype(BF16)


def query_grad(dq_sum):
    return jnp.concatenate([dq_sum[0, :HD, :], dq_sum[1, HD:, :]], axis=0)


def pair_backward(
    joined_ref, q_ref, grad_ref, mixed_ref, lse_ref, kv_ref, dq_ref, dkv_ref, dq_sum, *, kblock
):
    joined = joined_ref[0] > 0
    dq_sum[...] = jnp.zeros_like(dq_sum)

    @pl.when(joined)
    def _():
        attend_back(q_ref, grad_ref, mixed_ref, lse_ref, kv_ref, dkv_ref, dq_sum, kblock)

    @pl.when(jnp.logical_not(joined))
    def _():
        dkv_ref[...] = jnp.zeros_like(dkv_ref)

    dq_ref[...] = query_grad(dq_sum)


def own_backward(
    q_ref, grad_ref, mixed_ref, lse_ref, kv_ref, pair_dq_ref, dq_ref, dkv_ref, dq_sum, *, kblock
):
    dq_sum[...] = jnp.zeros_like(dq_sum)
    attend_back(q_ref, grad_ref, mixed_ref, lse_ref, kv_ref, dkv_ref, dq_sum, kblock)
    total = query_grad(dq_sum) + pair_dq_ref[...]
    dq_ref[...] = (total.T * HD**-0.5).astype(BF16)


def params(**extra):
    return pltpu.CompilerParams(vmem_limit_bytes=56 << 20, **extra)


def cost(rows, keys, width, products):
    return pl.CostEstimate(
        flops=2 * rows * keys * width * products * 4,
        bytes_accessed=2 * width * (rows + 2 * keys),
        transcendentals=rows * keys * width // HD,
    )


def attention_own(qkv):
    rows = qkv.shape[0]
    width = qkv.shape[1] // 3
    pairs = width // LANES
    column = pl.BlockSpec((rows, LANES), lambda p: (0, p))
    own_kv = pl.BlockSpec((rows, 2 * LANES), lambda p: (0, pairs // 2 + p))
    shape = jax.ShapeDtypeStruct((rows, width), F32)
    return pl.pallas_call(
        functools.partial(own_forward, qblock=min(512, rows)),
        grid=(pairs,),
        in_specs=[column, own_kv],
        out_specs=[column, column],
        out_shape=[shape, shape],
        compiler_params=params(),
        cost_estimate=cost(rows, rows, width, 2),
        name="attend_own",
    )(qkv, qkv)


def attention_pair(joined, qkv, kv_of_pair, own, own_lse):
    rows, width = own.shape
    pairs = width // LANES
    column = pl.BlockSpec((rows, LANES), lambda p: (0, p))
    pair_kv = pl.BlockSpec((rows, 2 * LANES), lambda p: (0, p))
    return pl.pallas_call(
        functools.partial(pair_forward, qblock=min(512, rows)),
        grid=(pairs,),
        in_specs=[pl.BlockSpec(memory_space=pltpu.SMEM), column, pair_kv, column, column],
        out_specs=[column, column],
        out_shape=[
            jax.ShapeDtypeStruct((rows, width), BF16),
            jax.ShapeDtypeStruct((rows, width), F32),
        ],
        compiler_params=params(),
        cost_estimate=cost(rows, rows, width, 2),
        name="attend_pair",
    )(joined, qkv, kv_of_pair, own, own_lse)


def attention_back_pair(joined, qkv, kv_of_pair, grad, mixed, lse):
    rows, width = grad.shape
    pairs = width // LANES
    column = pl.BlockSpec((rows, LANES), lambda p: (0, p))
    pair_kv = pl.BlockSpec((rows, 2 * LANES), lambda p: (0, p))
    across = pl.BlockSpec((LANES, rows), lambda p: (p, 0))
    return pl.pallas_call(
        functools.partial(pair_backward, kblock=min(512, rows)),
        grid=(pairs,),
        in_specs=[pl.BlockSpec(memory_space=pltpu.SMEM)] + [column] * 4 + [pair_kv],
        out_specs=[across, pair_kv],
        out_shape=[
            jax.ShapeDtypeStruct((width, rows), F32),
            jax.ShapeDtypeStruct((rows, 2 * width), BF16),
        ],
        scratch_shapes=[pltpu.VMEM((2, LANES, rows), F32)],
        compiler_params=params(),
        cost_estimate=cost(rows, rows, width, 5),
        name="attend_back_pair",
    )(joined, qkv, grad, mixed, lse, kv_of_pair)


def attention_back_own(qkv, grad, mixed, lse, pair_dq):
    rows, width = grad.shape
    pairs = width // LANES
    column = pl.BlockSpec((rows, LANES), lambda p: (0, p))
    own_kv = pl.BlockSpec((rows, 2 * LANES), lambda p: (0, pairs // 2 + p))
    kv_out = pl.BlockSpec((rows, 2 * LANES), lambda p: (0, p))
    across = pl.BlockSpec((LANES, rows), lambda p: (p, 0))
    return pl.pallas_call(
        functools.partial(own_backward, kblock=min(512, rows)),
        grid=(pairs,),
        in_specs=[column] * 4 + [own_kv, across],
        out_specs=[column, kv_out],
        out_shape=[
            jax.ShapeDtypeStruct((rows, width), BF16),
            jax.ShapeDtypeStruct((rows, 2 * width), BF16),
        ],
        scratch_shapes=[pltpu.VMEM((2, LANES, rows), F32)],
        compiler_params=params(),
        cost_estimate=cost(rows, rows, width, 5),
        name="attend_back_own",
    )(qkv, grad, mixed, lse, qkv, pair_dq)


def small_kernel(n_dp, slice_ref, bias_ref, all_ref, partner_ref, send_sem, recv_sem):
    me = lax.axis_index("dp")
    t = lax.axis_index("tensor")

    barrier = pltpu.get_barrier_semaphore()

    def greet(step, carry):
        peer = lax.rem(me + step, n_dp)
        pl.semaphore_signal(
            barrier, inc=1, device_id=(peer, t), device_id_type=pl.DeviceIdType.MESH
        )
        return carry

    lax.fori_loop(1, n_dp, greet, 0)
    pl.semaphore_signal(
        barrier, inc=1, device_id=(me, 1 - t), device_id_type=pl.DeviceIdType.MESH
    )
    pl.semaphore_wait(barrier, n_dp)

    def to_peer(step):
        return pltpu.make_async_remote_copy(
            src_ref=slice_ref,
            dst_ref=all_ref.at[me],
            send_sem=send_sem.at[step],
            recv_sem=recv_sem.at[step],
            device_id=(lax.rem(me + step, n_dp), t),
            device_id_type=pl.DeviceIdType.MESH,
        )

    to_partner = pltpu.make_async_remote_copy(
        src_ref=bias_ref,
        dst_ref=partner_ref,
        send_sem=send_sem.at[0],
        recv_sem=recv_sem.at[0],
        device_id=(me, 1 - t),
        device_id_type=pl.DeviceIdType.MESH,
    )
    to_partner.start()

    def start(step, carry):
        to_peer(step).start()
        return carry

    def finish(step, carry):
        to_peer(step).wait()
        return carry

    lax.fori_loop(1, n_dp, start, 0)
    all_ref[me] = slice_ref[...]
    lax.fori_loop(1, n_dp, finish, 0)
    to_partner.wait()


def share_small(n_dp, slices, biases):
    vmem = pl.BlockSpec(memory_space=pltpu.VMEM)
    return pl.pallas_call(
        functools.partial(small_kernel, n_dp),
        in_specs=[vmem, vmem],
        out_specs=[vmem, vmem],
        out_shape=[
            jax.ShapeDtypeStruct((n_dp,) + slices.shape, F32),
            jax.ShapeDtypeStruct(biases.shape, F32),
        ],
        scratch_shapes=[
            pltpu.SemaphoreType.DMA((n_dp,)),
            pltpu.SemaphoreType.DMA((n_dp,)),
        ],
        compiler_params=pltpu.CompilerParams(collective_id=0, has_side_effects=True),
        name="share_small",
    )(slices, biases)


def sum_small_kernel(
    n_dp, parts_ref, total_ref, bias_ref, landed, pair_sum, pair_in, own_bias, send_sem, recv_sem
):
    me = lax.axis_index("dp")
    t = lax.axis_index("tensor")
    mesh_id = pl.DeviceIdType.MESH

    barrier = pltpu.get_barrier_semaphore()

    def greet(step, carry):
        pl.semaphore_signal(
            barrier, inc=1, device_id=(lax.rem(me + step, n_dp), t), device_id_type=mesh_id
        )
        return carry

    lax.fori_loop(1, n_dp, greet, 0)
    pl.semaphore_signal(barrier, inc=1, device_id=(me, 1 - t), device_id_type=mesh_id)
    pl.semaphore_wait(barrier, n_dp)

    def part_to(step):
        peer = lax.rem(me + step, n_dp)
        return pltpu.make_async_remote_copy(
            src_ref=parts_ref.at[peer],
            dst_ref=landed.at[step],
            send_sem=send_sem.at[0, step],
            recv_sem=recv_sem.at[0, step],
            device_id=(peer, t),
            device_id_type=mesh_id,
        )

    def bias_to(step):
        return pltpu.make_async_remote_copy(
            src_ref=own_bias,
            dst_ref=bias_ref.at[me],
            send_sem=send_sem.at[1, step],
            recv_sem=recv_sem.at[1, step],
            device_id=(lax.rem(me + step, n_dp), t),
            device_id_type=mesh_id,
        )

    def start_part(step, carry):
        part_to(step).start()
        return carry

    def add_part(step, carry):
        part_to(step).wait()
        return carry + landed[step]

    lax.fori_loop(1, n_dp, start_part, 0)
    pair_sum[...] = lax.fori_loop(1, n_dp, add_part, parts_ref[me])
    to_partner = pltpu.make_async_remote_copy(
        src_ref=pair_sum,
        dst_ref=pair_in,
        send_sem=send_sem.at[1, 0],
        recv_sem=recv_sem.at[1, 0],
        device_id=(me, 1 - t),
        device_id_type=mesh_id,
    )
    to_partner.start()
    to_partner.wait()
    total = pair_sum[...] + pair_in[...]
    total_ref[...] = total
    own_bias[...] = total[:8]
    bias_ref[me] = total[:8]

    def start_bias(step, carry):
        bias_to(step).start()
        return carry

    def finish_bias(step, carry):
        bias_to(step).wait()
        return carry

    lax.fori_loop(1, n_dp, start_bias, 0)
    lax.fori_loop(1, n_dp, finish_bias, 0)


def sum_small(n_dp, parts):
    vmem = pl.BlockSpec(memory_space=pltpu.VMEM)
    block = parts.shape[1:]
    return pl.pallas_call(
        functools.partial(sum_small_kernel, n_dp),
        in_specs=[vmem],
        out_specs=[vmem, vmem],
        out_shape=[
            jax.ShapeDtypeStruct(block, F32),
            jax.ShapeDtypeStruct((n_dp, 8, LANES), F32),
        ],
        scratch_shapes=[
            pltpu.VMEM(parts.shape, F32),
            pltpu.VMEM(block, F32),
            pltpu.VMEM(block, F32),
            pltpu.VMEM((8, LANES), F32),
            pltpu.SemaphoreType.DMA((2, n_dp)),
            pltpu.SemaphoreType.DMA((2, n_dp)),
        ],
        compiler_params=pltpu.CompilerParams(collective_id=1, has_side_effects=True),
        name="sum_small",
    )(parts)


def after(*values):
    return lax.optimization_barrier(values)


def swap(values):
    return lax.ppermute(values, "tensor", [(0, 1), (1, 0)])


def tree_sum(n_dp, piece, t, values):
    me = lax.axis_index("dp")
    columns = values.shape[1]

    def add(first, second, upper, exchange):
        mine = jnp.where(upper, second, first)
        arrived = exchange(jnp.where(upper, first, second))
        return mine.astype(F32) + arrived.astype(F32)

    def along_dp(total, step):
        blocks = total.reshape(-1, 2, piece, total.shape[-1])
        partners = [(i, i ^ step) for i in range(n_dp)]
        return add(
            blocks[:, 0],
            blocks[:, 1],
            (me // step) % 2 == 1,
            lambda v: lax.ppermute(v, "dp", partners),
        ).astype(BF16)

    total = along_dp(values, 1)
    total = add(total[..., : columns // 2], total[..., columns // 2 :], t == 1, swap).astype(BF16)
    step = 2
    while step < n_dp:
        total = along_dp(total, step)
        step *= 2
    return total.reshape(piece, columns // 2).astype(F32)


def per_device(
    tokens,
    grad_tokens,
    dealing,
    segment_ids,
    ln1_gain,
    ln1_bias,
    w_qkv,
    b_qv,
    w_out,
    b_out,
    ln2_gain,
    ln2_bias,
    w_up,
    b_up,
    w_down,
    b_down,
):
    n_dp = lax.axis_size("dp")
    t = lax.axis_index("tensor")
    rows, width = tokens.shape
    piece = ln1_gain.shape[0]
    half = b_qv.shape[1]
    hidden_half = b_up.shape[0]
    pairs = width // LANES

    def join(own, other, axis):
        return jnp.where(
            t == 0,
            jnp.concatenate([own, other], axis=axis),
            jnp.concatenate([other, own], axis=axis),
        )

    def reduced(values):
        return lax.psum_scatter(values, "dp", scatter_dimension=0, tiled=True)

    def mine_of(values, axis):
        size = values.shape[axis] // 2
        low, high = (
            lax.slice_in_dim(values, 0, size, axis=axis),
            lax.slice_in_dim(values, size, 2 * size, axis=axis),
        )
        return jnp.where(t == 0, low, high), jnp.where(t == 0, high, low)

    other_qkv = swap(w_qkv)
    qkv_local = join(w_qkv, other_qkv, 2)
    kv_local = (
        qkv_local[:, 1:].reshape(piece, 2, pairs, LANES).transpose(0, 2, 1, 3).reshape(piece, -1)
    )
    qkv_local = jnp.concatenate([qkv_local[:, 0], kv_local], axis=1)
    rest_local = jnp.concatenate([w_out.T, w_up, w_down.T], axis=1)
    other_rest = swap(rest_local)
    up_at, down_at = half, half + hidden_half
    rest_local = jnp.concatenate(
        [
            join(rest_local[:, :up_at], other_rest[:, :up_at], 1),
            join(rest_local[:, up_at:down_at], other_rest[:, up_at:down_at], 1),
            join(rest_local[:, down_at:], other_rest[:, down_at:], 1),
        ],
        axis=1,
    )
    wqkv = lax.all_gather(qkv_local, "dp", axis=0, tiled=True)
    rest = lax.all_gather(rest_local, "dp", axis=0, tiled=True)
    wout_t = rest[:, :width]
    wup = rest[:, width : width + 2 * hidden_half]
    wdown_t = rest[:, width + 2 * hidden_half :]
    wkv = wqkv[:, width:]
    wq = wqkv[:, :width]

    small = jnp.stack([ln1_gain, ln1_bias, b_out, ln2_gain, ln2_bias, b_down])
    small = jnp.pad(small, ((0, 2), (0, LANES - piece)))
    biases = jnp.concatenate([b_qv.reshape(-1), b_up])
    bias_rows = -(-biases.shape[0] // (8 * LANES)) * 8
    biases = jnp.pad(biases, (0, bias_rows * LANES - biases.shape[0]))
    biases = biases.reshape(bias_rows, LANES)
    small_all, other_biases = share_small(n_dp, small, biases)
    row_order = dealing[0]
    picks = (row_order[:, None] == jnp.arange(rows, dtype=jnp.int32)[None, :]).astype(BF16)
    sent_rows = mm(picks, tokens).astype(BF16)
    dealt = lax.all_to_all(sent_rows, "dp", split_axis=0, concat_axis=0, tiled=True)
    grad_tokens, dealt = after(grad_tokens, dealt)
    sent_grads = mm(picks, grad_tokens).astype(BF16)
    grad_out = lax.all_to_all(sent_grads, "dp", split_axis=0, concat_axis=0, tiled=True)
    dealt_of_pair = swap(dealt)
    joined = (segment_ids[:1] == segment_ids[-1:]).astype(jnp.int32)

    small_full = small_all[:, :6, :piece].transpose(1, 0, 2).reshape(6, width)
    flat, other_flat = biases.reshape(-1), other_biases.reshape(-1)
    bqv_full = join(flat[: 2 * half].reshape(2, half), other_flat[: 2 * half].reshape(2, half), 1)
    bup_full = join(
        flat[2 * half : 2 * half + hidden_half],
        other_flat[2 * half : 2 * half + hidden_half],
        0,
    )

    resid = dealt.astype(F32)
    ln_one, normed_one, factor_one = normalize(resid, small_full[0], small_full[1])
    ln_one = ln_one.astype(BF16)
    kv_bias = jnp.stack(
        [jnp.zeros((pairs, LANES), F32), bqv_full[1].reshape(pairs, LANES)], axis=1
    ).reshape(-1)
    score_scale = HD**-0.5 * LOG2E
    shift = jnp.concatenate([bqv_full[0] * score_scale, kv_bias])
    scale = jnp.concatenate([jnp.full((width,), score_scale, F32), jnp.ones((2 * width,), F32)])
    qkv = (mm(ln_one, wqkv) * scale + shift).astype(BF16)
    own, own_lse = attention_own(qkv)
    dealt_of_pair, own = after(dealt_of_pair, own)
    ln_of_pair = normalize(dealt_of_pair.astype(F32), small_full[0], small_full[1])[0].astype(BF16)
    kv_of_pair = (mm(ln_of_pair, wkv) + kv_bias).astype(BF16)
    attended, lse = attention_pair(joined, qkv, kv_of_pair, own, own_lse)
    hidden = resid + mm(attended, wout_t, 1, 1) + small_full[2]

    ln_two, normed_two, factor_two = normalize(hidden, small_full[3], small_full[4])
    ln_two = ln_two.astype(BF16)
    pre_act = mm(ln_two, wup) + bup_full
    square = pre_act * pre_act
    bend = jnp.tanh(pre_act * (GELU_ONE + GELU_THREE * square))
    gate = 0.5 + 0.5 * bend
    slope = gate + (0.5 * pre_act) * (1.0 - bend * bend) * (GELU_ONE + 3.0 * GELU_THREE * square)
    act, slope = after((pre_act * gate).astype(BF16), slope.astype(BF16))
    output = (hidden + mm(act, wdown_t, 1, 1) + small_full[5]).astype(BF16)

    grad_down_t = mm(grad_out, act, 0, 0).astype(BF16)
    grad_pre = (mm(grad_out, wdown_t) * slope.astype(F32)).astype(BF16)
    bias_up_grad = jnp.sum(grad_pre, axis=0, dtype=F32)
    grad_up = mm(ln_two, grad_pre, 0, 0).astype(BF16)
    mlp_grads = jnp.concatenate([grad_down_t, grad_up], axis=1)
    mlp_grads, grad_pre = after(mlp_grads, grad_pre)
    mlp_sum = reduced(mlp_grads)
    grad_ln_two = mm(grad_pre, wup, 1, 1)
    gain_two_grad = jnp.sum(grad_ln_two * normed_two, axis=0)
    bias_two_grad = jnp.sum(grad_ln_two, axis=0)
    grad_hidden = grad_out.astype(F32) + norm_back(
        grad_ln_two, normed_two, factor_two, small_full[3]
    )
    grad_branch = grad_hidden.astype(BF16)
    grad_wout_t = mm(grad_branch, attended, 0, 0).astype(BF16)
    wout_sum = reduced(grad_wout_t)
    grad_att = mm(grad_branch, wout_t).astype(BF16)
    grad_att, output = after(grad_att, output)

    pair_dq, pair_dkv = attention_back_pair(
        joined, qkv, kv_of_pair, grad_att, attended, lse
    )
    for_pair = mm(pair_dkv, wkv, 1, 1).astype(BF16)
    for_pair = swap(for_pair)
    dq, dkv = attention_back_own(qkv, grad_att, attended, lse, pair_dq)
    grad_wq = mm(ln_one, dq, 0, 0).astype(BF16)
    grad_wkv = (mm(ln_one, dkv, 0, 0) + mm(ln_of_pair, pair_dkv, 0, 0)).astype(BF16)
    bias_q_grad = jnp.sum(dq, axis=0, dtype=F32)
    kv_sum = jnp.sum(dkv, axis=0, dtype=F32) + jnp.sum(pair_dkv, axis=0, dtype=F32)
    bias_v_grad = kv_sum.reshape(pairs, 2, LANES)[:, 1].reshape(-1)
    grad_ln_one = mm(dq, wq, 1, 1) + mm(dkv, wkv, 1, 1) + for_pair.astype(F32)
    grad_input = (
        grad_hidden + norm_back(grad_ln_one, normed_one, factor_one, small_full[0])
    ).astype(BF16)

    grad_wqkv = jnp.concatenate(
        [grad_wq[:, :half], grad_wkv[:, : 2 * half], grad_wq[:, half:], grad_wkv[:, 2 * half :]],
        axis=1,
    )
    qkv_part = tree_sum(n_dp, piece, t, grad_wqkv)

    def paired(values, sizes):
        columns, start = [], 0
        for size in sizes:
            columns.append(mine_of(values[:, start : start + size], 1))
            start += size
        mine = jnp.concatenate([c[0] for c in columns], axis=1)
        other = jnp.concatenate([c[1] for c in columns], axis=1)
        total = mine.astype(F32) + swap(other).astype(F32)
        cuts = [sum(sizes[:i]) // 2 for i in range(1, len(sizes))]
        return jnp.split(total, cuts, axis=1)

    down_part, up_part = paired(mlp_sum, (2 * hidden_half, 2 * hidden_half))
    wout_part = paired(wout_sum, (width,))[0].T
    down_part = down_part.T
    q_part, kv_part = qkv_part[:, :half], qkv_part[:, half:]
    kv_part = kv_part.reshape(piece, pairs // 2, 2, LANES).transpose(0, 2, 1, 3)
    qkv_part = jnp.concatenate(
        [q_part.reshape(piece, 1, half), kv_part.reshape(piece, 2, half)], axis=1
    )

    row_sums = jnp.concatenate(
        [
            jnp.stack([bias_q_grad, bias_v_grad]),
            bias_up_grad.reshape(-1, width),
            jnp.zeros((2, width), F32),
            jnp.stack(
                [
                    jnp.sum(grad_ln_one * normed_one, axis=0),
                    jnp.sum(grad_ln_one, axis=0),
                    jnp.sum(grad_hidden, axis=0),
                    gain_two_grad,
                    bias_two_grad,
                    jnp.sum(grad_out, axis=0, dtype=F32),
                ]
            ),
            jnp.zeros((2, width), F32),
        ]
    )
    row_sums = row_sums.reshape(16, n_dp, piece).transpose(1, 0, 2)
    row_sums = jnp.pad(row_sums, ((0, 0), (0, 0), (0, LANES - piece)))
    slice_total, bias_total = sum_small(n_dp, row_sums)
    grad_input, slice_total = after(grad_input, slice_total)
    small_part = slice_total[8:14, :piece]
    bias_total = bias_total[:, :6, :piece].transpose(1, 0, 2).reshape(6, width)
    qv_part = mine_of(bias_total[:2], 1)[0]
    bias_up_part = mine_of(bias_total[2:].reshape(-1), 0)[0]

    sent_out = lax.all_to_all(output, "dp", split_axis=0, concat_axis=0, tiled=True)
    sent_grad = lax.all_to_all(grad_input, "dp", split_axis=0, concat_axis=0, tiled=True)
    restored_out = mm(picks, sent_out, 0, 0).astype(BF16)
    restored_grad = mm(picks, sent_grad, 0, 0).astype(BF16)
    return (
        restored_out,
        restored_grad,
        small_part[0],
        small_part[1],
        qkv_part,
        qv_part,
        wout_part,
        small_part[2],
        small_part[3],
        small_part[4],
        up_part,
        bias_up_part,
        down_part,
        small_part[5],
    )


def solution(mesh):
    placed = (
        P(("dp", "tensor"), None),
        P(("dp", "tensor"), None),
        P(("dp", "tensor"), None),
        P("dp"),
        P("dp"),
        P("dp"),
        P("dp", None, "tensor"),
        P(None, "tensor"),
        P("tensor", "dp"),
        P("dp"),
        P("dp"),
        P("dp"),
        P("dp", "tensor"),
        P("tensor"),
        P("tensor", "dp"),
        P("dp"),
    )

    return jax.shard_map(
        per_device,
        mesh=mesh,
        in_specs=placed,
        out_specs=(
            P(("dp", "tensor"), None),
            P(("dp", "tensor"), None),
            P("dp"),
            P("dp"),
            P("dp", None, "tensor"),
            P(None, "tensor"),
            P("tensor", "dp"),
            P("dp"),
            P("dp"),
            P("dp"),
            P("dp", "tensor"),
            P("tensor"),
            P("tensor", "dp"),
            P("dp"),
        ),
        check_vma=False,
    )
```

```python
import functools

import jax
import jax.numpy as jnp
from jax import lax
from jax.experimental import pallas as pl
from jax.experimental.layout import Layout, with_layout_constraint
from jax.experimental.pallas import tpu as pltpu
from jax.sharding import PartitionSpec as P


HD = 64
LANES = 128
EPS = 1e-06
LN2 = 0.6931471805599453
LOG2E = 1.4426950408889634
GELU_ONE = 0.7978845608028654
GELU_THREE = 0.7978845608028654 * 0.044715
F32 = jnp.float32
BF16 = jnp.bfloat16


def normalize(values, gain_row, bias_row):
    centred = values - jnp.mean(values, axis=-1, keepdims=True)
    factor = lax.rsqrt(jnp.mean(centred * centred, axis=-1, keepdims=True) + EPS)
    normed = centred * factor
    return (normed * gain_row + bias_row, normed, factor)


def norm_back(grad_rows, normed, factor, gain_row):
    scaled = grad_rows * gain_row
    centred = scaled - jnp.mean(scaled, axis=-1, keepdims=True)
    return factor * (centred - normed * jnp.mean(scaled * normed, axis=-1, keepdims=True))


def mm(left, right, left_dim=1, right_dim=0):
    return lax.dot_general(
        left, right, (((left_dim,), (right_dim,)), ((), ())), preferred_element_type=F32
    )


def head_lanes(head):
    return (lax.broadcasted_iota(jnp.int32, (1, LANES), 1) // HD) == head


def attend_rows(q, keys, values):
    outs, lses = [], []
    one = jnp.ones((), BF16)
    for head in range(2):
        mine = head_lanes(head)
        scores = mm(jnp.where(mine, q, jnp.zeros_like(q)), keys, 1, 1)
        row_max = jnp.max(scores, axis=1, keepdims=True)
        weights = jnp.exp2(scores - row_max).astype(BF16)
        mixed = mm(weights, jnp.where(mine, values, one))
        total = jnp.sum(jnp.where(mine, 0.0, mixed), axis=1, keepdims=True) * (1.0 / HD)
        outs.append(mixed / total)
        lses.append(row_max + jnp.log2(total))
    first = head_lanes(0)
    return (jnp.where(first, outs[0], outs[1]), jnp.where(first, lses[0], lses[1]))


def own_forward(q_ref, kv_ref, mixed_ref, lse_ref, *, qblock):
    for block in range(q_ref.shape[0] // qblock):
        rows = pl.ds(block * qblock, qblock)
        mixed, lse = attend_rows(q_ref[rows, :], kv_ref[:, :LANES], kv_ref[:, LANES:])
        mixed_ref[rows, :] = mixed
        lse_ref[rows, :] = lse


def pair_forward(joined_ref, q_ref, kv_ref, own_ref, own_lse_ref, mixed_ref, lse_ref, *, qblock):
    joined = joined_ref[0] > 0

    @pl.when(joined)
    def _():
        for block in range(q_ref.shape[0] // qblock):
            rows = pl.ds(block * qblock, qblock)
            mixed, lse = attend_rows(q_ref[rows, :], kv_ref[:, :LANES], kv_ref[:, LANES:])
            own_lse = own_lse_ref[rows, :]
            top = jnp.maximum(own_lse, lse)
            own_share = jnp.exp2(own_lse - top)
            pair_share = jnp.exp2(lse - top)
            total = own_share + pair_share
            mixed_ref[rows, :] = (
                (own_ref[rows, :] * own_share + mixed * pair_share) / total
            ).astype(BF16)
            lse_ref[rows, :] = top + jnp.log2(total)

    @pl.when(jnp.logical_not(joined))
    def _():
        mixed_ref[...] = own_ref[...].astype(BF16)
        lse_ref[...] = own_lse_ref[...]


def split_three(values):
    high = values.astype(BF16)
    rest = values - high.astype(F32)
    middle = rest.astype(BF16)
    return high, middle, (rest - middle.astype(F32)).astype(BF16)


def attend_back(q_ref, grad_ref, mixed_ref, lse_ref, kv_ref, dkv_ref, dq_sum, kblock):
    lane = lax.broadcasted_iota(jnp.int32, (1, LANES), 1)
    q = q_ref[...]
    grad = grad_ref[...]
    products = grad.astype(F32) * mixed_ref[...].astype(F32)
    wide_q, wide_grad = [], []
    for head in range(2):
        mine = head_lanes(head)
        spare = (1 - head) * HD
        inner = jnp.sum(jnp.where(mine, products, 0.0), axis=1, keepdims=True)
        lse_parts = split_three(-lse_ref[:, head * HD : head * HD + 1])
        inner_parts = split_three(-inner)
        q_head = jnp.where(mine, q, jnp.zeros_like(q))
        grad_head = jnp.where(mine, grad, jnp.zeros_like(grad))
        for part in range(3):
            q_head = jnp.where(lane == spare + part, lse_parts[part], q_head)
            grad_head = jnp.where(lane == spare + part, inner_parts[part], grad_head)
        wide_q.append(q_head)
        wide_grad.append(grad_head)
    one = jnp.ones((), BF16)
    first = head_lanes(0)
    for block in range(kv_ref.shape[0] // kblock):
        rows = pl.ds(block * kblock, kblock)
        keys = kv_ref[rows, :LANES]
        values = kv_ref[rows, LANES:]
        key_grads, value_grads = [], []
        for head in range(2):
            mine = head_lanes(head)
            weights = jnp.exp2(mm(jnp.where(mine, keys, one), wide_q[head], 1, 1))
            grad_weights = mm(jnp.where(mine, values, one), wide_grad[head], 1, 1)
            grad_scores = (weights * grad_weights).astype(BF16)
            value_grads.append(mm(weights.astype(BF16), grad))
            key_grads.append(mm(grad_scores, q))
            dq_sum[head] += mm(keys, grad_scores, 0, 0)
        dkv_ref[rows, :LANES] = (jnp.where(first, key_grads[0], key_grads[1]) * LN2).astype(BF16)
        dkv_ref[rows, LANES:] = jnp.where(first, value_grads[0], value_grads[1]).astype(BF16)


def query_grad(dq_sum):
    return jnp.concatenate([dq_sum[0, :HD, :], dq_sum[1, HD:, :]], axis=0)


def pair_backward(
    joined_ref, q_ref, grad_ref, mixed_ref, lse_ref, kv_ref, dq_ref, dkv_ref, dq_sum, *, kblock
):
    joined = joined_ref[0] > 0
    dq_sum[...] = jnp.zeros_like(dq_sum)

    @pl.when(joined)
    def _():
        attend_back(q_ref, grad_ref, mixed_ref, lse_ref, kv_ref, dkv_ref, dq_sum, kblock)

    @pl.when(jnp.logical_not(joined))
    def _():
        dkv_ref[...] = jnp.zeros_like(dkv_ref)

    dq_ref[...] = query_grad(dq_sum)


def own_backward(
    q_ref, grad_ref, mixed_ref, lse_ref, kv_ref, pair_dq_ref, dq_ref, dkv_ref, dq_sum, *, kblock
):
    dq_sum[...] = jnp.zeros_like(dq_sum)
    attend_back(q_ref, grad_ref, mixed_ref, lse_ref, kv_ref, dkv_ref, dq_sum, kblock)
    total = query_grad(dq_sum) + pair_dq_ref[...]
    dq_ref[...] = (total.T * HD**-0.5).astype(BF16)


def params(**extra):
    return pltpu.CompilerParams(vmem_limit_bytes=56 << 20, **extra)


def cost(rows, keys, width, products):
    return pl.CostEstimate(
        flops=2 * rows * keys * width * products * 4,
        bytes_accessed=2 * width * (rows + 2 * keys),
        transcendentals=rows * keys * width // HD,
    )


def attention_own(qkv):
    rows = qkv.shape[0]
    width = qkv.shape[1] // 3
    pairs = width // LANES
    column = pl.BlockSpec((rows, LANES), lambda p: (0, p))
    own_kv = pl.BlockSpec((rows, 2 * LANES), lambda p: (0, pairs // 2 + p))
    shape = jax.ShapeDtypeStruct((rows, width), F32)
    return pl.pallas_call(
        functools.partial(own_forward, qblock=min(512, rows)),
        grid=(pairs,),
        in_specs=[column, own_kv],
        out_specs=[column, column],
        out_shape=[shape, shape],
        compiler_params=params(),
        cost_estimate=cost(rows, rows, width, 2),
        name="attend_own",
    )(qkv, qkv)


def attention_pair(joined, qkv, kv_of_pair, own, own_lse):
    rows, width = own.shape
    pairs = width // LANES
    column = pl.BlockSpec((rows, LANES), lambda p: (0, p))
    pair_kv = pl.BlockSpec((rows, 2 * LANES), lambda p: (0, p))
    return pl.pallas_call(
        functools.partial(pair_forward, qblock=min(512, rows)),
        grid=(pairs,),
        in_specs=[pl.BlockSpec(memory_space=pltpu.SMEM), column, pair_kv, column, column],
        out_specs=[column, column],
        out_shape=[
            jax.ShapeDtypeStruct((rows, width), BF16),
            jax.ShapeDtypeStruct((rows, width), F32),
        ],
        compiler_params=params(),
        cost_estimate=cost(rows, rows, width, 2),
        name="attend_pair",
    )(joined, qkv, kv_of_pair, own, own_lse)


def attention_back_pair(joined, qkv, kv_of_pair, grad, mixed, lse):
    rows, width = grad.shape
    pairs = width // LANES
    column = pl.BlockSpec((rows, LANES), lambda p: (0, p))
    pair_kv = pl.BlockSpec((rows, 2 * LANES), lambda p: (0, p))
    across = pl.BlockSpec((LANES, rows), lambda p: (p, 0))
    return pl.pallas_call(
        functools.partial(pair_backward, kblock=min(512, rows)),
        grid=(pairs,),
        in_specs=[pl.BlockSpec(memory_space=pltpu.SMEM)] + [column] * 4 + [pair_kv],
        out_specs=[across, pair_kv],
        out_shape=[
            jax.ShapeDtypeStruct((width, rows), F32),
            jax.ShapeDtypeStruct((rows, 2 * width), BF16),
        ],
        scratch_shapes=[pltpu.VMEM((2, LANES, rows), F32)],
        compiler_params=params(),
        cost_estimate=cost(rows, rows, width, 5),
        name="attend_back_pair",
    )(joined, qkv, grad, mixed, lse, kv_of_pair)


def attention_back_own(qkv, grad, mixed, lse, pair_dq):
    rows, width = grad.shape
    pairs = width // LANES
    column = pl.BlockSpec((rows, LANES), lambda p: (0, p))
    own_kv = pl.BlockSpec((rows, 2 * LANES), lambda p: (0, pairs // 2 + p))
    kv_out = pl.BlockSpec((rows, 2 * LANES), lambda p: (0, p))
    across = pl.BlockSpec((LANES, rows), lambda p: (p, 0))
    return pl.pallas_call(
        functools.partial(own_backward, kblock=min(512, rows)),
        grid=(pairs,),
        in_specs=[column] * 4 + [own_kv, across],
        out_specs=[column, kv_out],
        out_shape=[
            jax.ShapeDtypeStruct((rows, width), BF16),
            jax.ShapeDtypeStruct((rows, 2 * width), BF16),
        ],
        scratch_shapes=[pltpu.VMEM((2, LANES, rows), F32)],
        compiler_params=params(),
        cost_estimate=cost(rows, rows, width, 5),
        name="attend_back_own",
    )(qkv, grad, mixed, lse, qkv, pair_dq)


def small_kernel(n_dp, slice_ref, bias_ref, all_ref, partner_ref, send_sem, recv_sem):
    me = lax.axis_index("dp")
    t = lax.axis_index("tensor")

    barrier = pltpu.get_barrier_semaphore()

    def greet(step, carry):
        peer = lax.rem(me + step, n_dp)
        pl.semaphore_signal(
            barrier, inc=1, device_id=(peer, t), device_id_type=pl.DeviceIdType.MESH
        )
        return carry

    lax.fori_loop(1, n_dp, greet, 0)
    pl.semaphore_signal(
        barrier, inc=1, device_id=(me, 1 - t), device_id_type=pl.DeviceIdType.MESH
    )
    pl.semaphore_wait(barrier, n_dp)

    def to_peer(step):
        return pltpu.make_async_remote_copy(
            src_ref=slice_ref,
            dst_ref=all_ref.at[me],
            send_sem=send_sem.at[step],
            recv_sem=recv_sem.at[step],
            device_id=(lax.rem(me + step, n_dp), t),
            device_id_type=pl.DeviceIdType.MESH,
        )

    to_partner = pltpu.make_async_remote_copy(
        src_ref=bias_ref,
        dst_ref=partner_ref,
        send_sem=send_sem.at[0],
        recv_sem=recv_sem.at[0],
        device_id=(me, 1 - t),
        device_id_type=pl.DeviceIdType.MESH,
    )
    to_partner.start()

    def start(step, carry):
        to_peer(step).start()
        return carry

    def finish(step, carry):
        to_peer(step).wait()
        return carry

    lax.fori_loop(1, n_dp, start, 0)
    all_ref[me] = slice_ref[...]
    lax.fori_loop(1, n_dp, finish, 0)
    to_partner.wait()


def share_small(n_dp, slices, biases):
    vmem = pl.BlockSpec(memory_space=pltpu.VMEM)
    return pl.pallas_call(
        functools.partial(small_kernel, n_dp),
        in_specs=[vmem, vmem],
        out_specs=[vmem, vmem],
        out_shape=[
            jax.ShapeDtypeStruct((n_dp,) + slices.shape, F32),
            jax.ShapeDtypeStruct(biases.shape, F32),
        ],
        scratch_shapes=[
            pltpu.SemaphoreType.DMA((n_dp,)),
            pltpu.SemaphoreType.DMA((n_dp,)),
        ],
        compiler_params=pltpu.CompilerParams(collective_id=0, has_side_effects=True),
        name="share_small",
    )(slices, biases)


def sum_small_kernel(
    n_dp, parts_ref, total_ref, bias_ref, landed, pair_sum, pair_in, own_bias, send_sem, recv_sem
):
    me = lax.axis_index("dp")
    t = lax.axis_index("tensor")
    mesh_id = pl.DeviceIdType.MESH

    barrier = pltpu.get_barrier_semaphore()

    def greet(step, carry):
        pl.semaphore_signal(
            barrier, inc=1, device_id=(lax.rem(me + step, n_dp), t), device_id_type=mesh_id
        )
        return carry

    lax.fori_loop(1, n_dp, greet, 0)
    pl.semaphore_signal(barrier, inc=1, device_id=(me, 1 - t), device_id_type=mesh_id)
    pl.semaphore_wait(barrier, n_dp)

    def part_to(step):
        peer = lax.rem(me + step, n_dp)
        return pltpu.make_async_remote_copy(
            src_ref=parts_ref.at[peer],
            dst_ref=landed.at[step],
            send_sem=send_sem.at[0, step],
            recv_sem=recv_sem.at[0, step],
            device_id=(peer, t),
            device_id_type=mesh_id,
        )

    def bias_to(step):
        return pltpu.make_async_remote_copy(
            src_ref=own_bias,
            dst_ref=bias_ref.at[me],
            send_sem=send_sem.at[1, step],
            recv_sem=recv_sem.at[1, step],
            device_id=(lax.rem(me + step, n_dp), t),
            device_id_type=mesh_id,
        )

    def start_part(step, carry):
        part_to(step).start()
        return carry

    def add_part(step, carry):
        part_to(step).wait()
        return carry + landed[step]

    lax.fori_loop(1, n_dp, start_part, 0)
    pair_sum[...] = lax.fori_loop(1, n_dp, add_part, parts_ref[me])
    to_partner = pltpu.make_async_remote_copy(
        src_ref=pair_sum,
        dst_ref=pair_in,
        send_sem=send_sem.at[1, 0],
        recv_sem=recv_sem.at[1, 0],
        device_id=(me, 1 - t),
        device_id_type=mesh_id,
    )
    to_partner.start()
    to_partner.wait()
    total = pair_sum[...] + pair_in[...]
    total_ref[...] = total
    own_bias[...] = total[:8]
    bias_ref[me] = total[:8]

    def start_bias(step, carry):
        bias_to(step).start()
        return carry

    def finish_bias(step, carry):
        bias_to(step).wait()
        return carry

    lax.fori_loop(1, n_dp, start_bias, 0)
    lax.fori_loop(1, n_dp, finish_bias, 0)


def sum_small(n_dp, parts):
    vmem = pl.BlockSpec(memory_space=pltpu.VMEM)
    block = parts.shape[1:]
    return pl.pallas_call(
        functools.partial(sum_small_kernel, n_dp),
        in_specs=[vmem],
        out_specs=[vmem, vmem],
        out_shape=[
            jax.ShapeDtypeStruct(block, F32),
            jax.ShapeDtypeStruct((n_dp, 8, LANES), F32),
        ],
        scratch_shapes=[
            pltpu.VMEM(parts.shape, F32),
            pltpu.VMEM(block, F32),
            pltpu.VMEM(block, F32),
            pltpu.VMEM((8, LANES), F32),
            pltpu.SemaphoreType.DMA((2, n_dp)),
            pltpu.SemaphoreType.DMA((2, n_dp)),
        ],
        compiler_params=pltpu.CompilerParams(collective_id=1, has_side_effects=True),
        name="sum_small",
    )(parts)


def by_rows(values):
    return with_layout_constraint(values, Layout((0, 1)))


def after(*values):
    return lax.optimization_barrier(values)


def swap(values):
    return lax.ppermute(values, "tensor", [(0, 1), (1, 0)])


def tree_gather(n_dp, t, values, split):
    me = lax.axis_index("dp")

    def joined(own, other, upper, axis):
        return jnp.where(
            upper, jnp.concatenate([other, own], axis=axis), jnp.concatenate([own, other], axis=axis)
        )

    blocks = values[None]
    steps = [1 << bit for bit in range(n_dp.bit_length() - 1)]
    for step in reversed(steps[1:]):
        other = lax.ppermute(blocks, "dp", [(i, i ^ step) for i in range(n_dp)])
        upper = (me // step) % 2 == 1
        blocks = joined(blocks[:, None], other[:, None], upper, 1).reshape((-1,) + values.shape)
    other = swap(blocks)
    blocks = jnp.concatenate(
        [
            joined(blocks[..., :split], other[..., :split], t == 1, 2),
            joined(blocks[..., split:], other[..., split:], t == 1, 2),
        ],
        axis=2,
    )
    other = lax.ppermute(blocks, "dp", [(i, i ^ 1) for i in range(n_dp)])
    full = joined(blocks[:, None], other[:, None], me % 2 == 1, 1)
    full = full.reshape(n_dp * values.shape[0], 2 * values.shape[1])
    return full


def tree_sum(n_dp, piece, t, values):
    me = lax.axis_index("dp")
    columns = values.shape[1]

    def add(first, second, upper, exchange):
        mine = jnp.where(upper, second, first)
        arrived = exchange(jnp.where(upper, first, second))
        return mine.astype(F32) + arrived.astype(F32)

    def along_dp(total, step):
        blocks = total.reshape(-1, 2, piece, total.shape[-1])
        partners = [(i, i ^ step) for i in range(n_dp)]
        return add(
            blocks[:, 0],
            blocks[:, 1],
            (me // step) % 2 == 1,
            lambda v: lax.ppermute(v, "dp", partners),
        ).astype(BF16)

    total = along_dp(values, 1)
    total = add(total[..., : columns // 2], total[..., columns // 2 :], t == 1, swap).astype(BF16)
    step = 2
    while step < n_dp:
        total = along_dp(total, step)
        step *= 2
    return total.reshape(piece, columns // 2).astype(F32)


def per_device(
    tokens,
    grad_tokens,
    dealing,
    segment_ids,
    ln1_gain,
    ln1_bias,
    w_qkv,
    b_qv,
    w_out,
    b_out,
    ln2_gain,
    ln2_bias,
    w_up,
    b_up,
    w_down,
    b_down,
):
    n_dp = lax.axis_size("dp")
    t = lax.axis_index("tensor")
    rows, width = tokens.shape
    piece = ln1_gain.shape[0]
    half = b_qv.shape[1]
    hidden_half = b_up.shape[0]
    pairs = width // LANES

    def join(own, other, axis):
        return jnp.where(
            t == 0,
            jnp.concatenate([own, other], axis=axis),
            jnp.concatenate([other, own], axis=axis),
        )

    def reduced(values):
        return lax.psum_scatter(values, "dp", scatter_dimension=0, tiled=True)

    def mine_of(values, axis):
        size = values.shape[axis] // 2
        low, high = (
            lax.slice_in_dim(values, 0, size, axis=axis),
            lax.slice_in_dim(values, size, 2 * size, axis=axis),
        )
        return jnp.where(t == 0, low, high), jnp.where(t == 0, high, low)

    kv_local = (
        w_qkv[:, 1:]
        .reshape(piece, 2, pairs // 2, LANES)
        .transpose(0, 2, 1, 3)
        .reshape(piece, 2 * half)
    )
    wqkv = tree_gather(n_dp, t, jnp.concatenate([w_qkv[:, 0], kv_local], axis=1), half)
    wq, wkv = wqkv[:, :width], wqkv[:, width:]
    rest_local = jnp.concatenate([w_out.T, w_up, w_down.T], axis=1)
    other_rest = swap(rest_local)
    up_at, down_at = half, half + hidden_half
    rest_local = jnp.concatenate(
        [
            join(rest_local[:, :up_at], other_rest[:, :up_at], 1),
            join(rest_local[:, up_at:down_at], other_rest[:, up_at:down_at], 1),
            join(rest_local[:, down_at:], other_rest[:, down_at:], 1),
        ],
        axis=1,
    )
    rest = lax.all_gather(rest_local, "dp", axis=0, tiled=True)
    wout_t = rest[:, :width]
    wup = rest[:, width : width + 2 * hidden_half]
    wdown_t = rest[:, width + 2 * hidden_half :]

    small = jnp.stack([ln1_gain, ln1_bias, b_out, ln2_gain, ln2_bias, b_down])
    small = jnp.pad(small, ((0, 2), (0, LANES - piece)))
    biases = jnp.concatenate([b_qv.reshape(-1), b_up])
    bias_rows = -(-biases.shape[0] // (8 * LANES)) * 8
    biases = jnp.pad(biases, (0, bias_rows * LANES - biases.shape[0]))
    biases = biases.reshape(bias_rows, LANES)
    small_all, other_biases = share_small(n_dp, small, biases)
    row_order = dealing[0]
    picks = (row_order[:, None] == jnp.arange(rows, dtype=jnp.int32)[None, :]).astype(BF16)
    sent_rows = mm(picks, tokens).astype(BF16)
    dealt = lax.all_to_all(sent_rows, "dp", split_axis=0, concat_axis=0, tiled=True)
    grad_tokens, dealt = after(grad_tokens, dealt)
    sent_grads = mm(picks, grad_tokens).astype(BF16)
    grad_out = lax.all_to_all(sent_grads, "dp", split_axis=0, concat_axis=0, tiled=True)
    dealt_of_pair = by_rows(swap(dealt))
    joined = (segment_ids[:1] == segment_ids[-1:]).astype(jnp.int32)

    small_full = small_all[:, :6, :piece].transpose(1, 0, 2).reshape(6, width)
    flat, other_flat = biases.reshape(-1), other_biases.reshape(-1)
    bqv_full = join(flat[: 2 * half].reshape(2, half), other_flat[: 2 * half].reshape(2, half), 1)
    bup_full = join(
        flat[2 * half : 2 * half + hidden_half],
        other_flat[2 * half : 2 * half + hidden_half],
        0,
    )

    resid = by_rows(dealt.astype(F32))
    ln_one, normed_one, factor_one = normalize(resid, small_full[0], small_full[1])
    ln_one = ln_one.astype(BF16)
    kv_bias = jnp.stack(
        [jnp.zeros((pairs, LANES), F32), bqv_full[1].reshape(pairs, LANES)], axis=1
    ).reshape(-1)
    score_scale = HD**-0.5 * LOG2E
    shift = jnp.concatenate([bqv_full[0] * score_scale, kv_bias])
    scale = jnp.concatenate([jnp.full((width,), score_scale, F32), jnp.ones((2 * width,), F32)])
    qkv = (mm(ln_one, wqkv) * scale + shift).astype(BF16)
    own, own_lse = attention_own(qkv)
    dealt_of_pair, own = after(dealt_of_pair, own)
    ln_of_pair = normalize(dealt_of_pair.astype(F32), small_full[0], small_full[1])[0].astype(BF16)
    kv_of_pair = (mm(ln_of_pair, wkv) + kv_bias).astype(BF16)
    attended, lse = attention_pair(joined, qkv, kv_of_pair, own, own_lse)
    hidden = by_rows(resid + mm(attended, wout_t, 1, 1) + small_full[2])

    ln_two, normed_two, factor_two = normalize(hidden, small_full[3], small_full[4])
    ln_two = ln_two.astype(BF16)
    pre_act = mm(ln_two, wup) + bup_full
    square = pre_act * pre_act
    bend = jnp.tanh(pre_act * (GELU_ONE + GELU_THREE * square))
    gate = 0.5 + 0.5 * bend
    slope = gate + (0.5 * pre_act) * (1.0 - bend * bend) * (GELU_ONE + 3.0 * GELU_THREE * square)
    act, slope = after((pre_act * gate).astype(BF16), slope.astype(BF16))
    output = by_rows((hidden + mm(act, wdown_t, 1, 1) + small_full[5]).astype(BF16))

    grad_down_t = mm(grad_out, act, 0, 0).astype(BF16)
    grad_pre = (mm(grad_out, wdown_t) * slope.astype(F32)).astype(BF16)
    bias_up_grad = jnp.sum(grad_pre, axis=0, dtype=F32)
    grad_up = mm(ln_two, grad_pre, 0, 0).astype(BF16)
    mlp_grads = jnp.concatenate([grad_down_t, grad_up], axis=1)
    mlp_grads, grad_pre = after(mlp_grads, grad_pre)
    mlp_sum = reduced(mlp_grads)
    grad_ln_two = by_rows(mm(grad_pre, wup, 1, 1))
    gain_two_grad = jnp.sum(grad_ln_two * normed_two, axis=0)
    bias_two_grad = jnp.sum(grad_ln_two, axis=0)
    grad_hidden = grad_out.astype(F32) + norm_back(
        grad_ln_two, normed_two, factor_two, small_full[3]
    )
    grad_branch = grad_hidden.astype(BF16)
    grad_wout_t = mm(grad_branch, attended, 0, 0).astype(BF16)
    wout_sum = reduced(grad_wout_t)
    grad_att = mm(grad_branch, wout_t).astype(BF16)
    grad_att, output = after(grad_att, output)

    pair_dq, pair_dkv = attention_back_pair(
        joined, qkv, kv_of_pair, grad_att, attended, lse
    )
    for_pair = mm(pair_dkv, wkv, 1, 1).astype(BF16)
    for_pair = swap(for_pair)
    dq, dkv = attention_back_own(qkv, grad_att, attended, lse, pair_dq)
    grad_ln_one = by_rows(mm(dq, wq, 1, 1) + mm(dkv, wkv, 1, 1) + for_pair.astype(F32))
    grad_input = (
        grad_hidden + norm_back(grad_ln_one, normed_one, factor_one, small_full[0])
    ).astype(BF16)
    dq, dkv, grad_input = after(dq, dkv, grad_input)
    grad_wq = mm(ln_one, dq, 0, 0).astype(BF16)
    grad_wkv = (mm(ln_one, dkv, 0, 0) + mm(ln_of_pair, pair_dkv, 0, 0)).astype(BF16)
    bias_q_grad = jnp.sum(dq, axis=0, dtype=F32)
    kv_sum = jnp.sum(dkv, axis=0, dtype=F32) + jnp.sum(pair_dkv, axis=0, dtype=F32)
    bias_v_grad = kv_sum.reshape(pairs, 2, LANES)[:, 1].reshape(-1)
    grad_wqkv = jnp.concatenate(
        [grad_wq[:, :half], grad_wkv[:, : 2 * half], grad_wq[:, half:], grad_wkv[:, 2 * half :]],
        axis=1,
    )
    qkv_part = tree_sum(n_dp, piece, t, grad_wqkv)

    def paired(values, sizes):
        columns, start = [], 0
        for size in sizes:
            columns.append(mine_of(values[:, start : start + size], 1))
            start += size
        mine = jnp.concatenate([c[0] for c in columns], axis=1)
        other = jnp.concatenate([c[1] for c in columns], axis=1)
        total = mine.astype(F32) + swap(other).astype(F32)
        cuts = [sum(sizes[:i]) // 2 for i in range(1, len(sizes))]
        return jnp.split(total, cuts, axis=1)

    down_part, up_part = paired(mlp_sum, (2 * hidden_half, 2 * hidden_half))
    wout_part = paired(wout_sum, (width,))[0].T
    down_part = down_part.T
    q_part, kv_part = qkv_part[:, :half], qkv_part[:, half:]
    kv_part = kv_part.reshape(piece, pairs // 2, 2, LANES).transpose(0, 2, 1, 3)
    qkv_part = jnp.concatenate(
        [q_part.reshape(piece, 1, half), kv_part.reshape(piece, 2, half)], axis=1
    )

    row_sums = jnp.concatenate(
        [
            jnp.stack([bias_q_grad, bias_v_grad]),
            bias_up_grad.reshape(-1, width),
            jnp.zeros((2, width), F32),
            jnp.stack(
                [
                    jnp.sum(grad_ln_one * normed_one, axis=0),
                    jnp.sum(grad_ln_one, axis=0),
                    jnp.sum(grad_hidden, axis=0),
                    gain_two_grad,
                    bias_two_grad,
                    jnp.sum(grad_out, axis=0, dtype=F32),
                ]
            ),
            jnp.zeros((2, width), F32),
        ]
    )
    row_sums = row_sums.reshape(16, n_dp, piece).transpose(1, 0, 2)
    row_sums = jnp.pad(row_sums, ((0, 0), (0, 0), (0, LANES - piece)))
    slice_total, bias_total = sum_small(n_dp, row_sums)
    small_part = slice_total[8:14, :piece]
    bias_total = bias_total[:, :6, :piece].transpose(1, 0, 2).reshape(6, width)
    qv_part = mine_of(bias_total[:2], 1)[0]
    bias_up_part = mine_of(bias_total[2:].reshape(-1), 0)[0]

    sent_out = lax.all_to_all(output, "dp", split_axis=0, concat_axis=0, tiled=True)
    sent_grad = lax.all_to_all(grad_input, "dp", split_axis=0, concat_axis=0, tiled=True)
    restored_out = mm(picks, sent_out, 0, 0).astype(BF16)
    restored_grad = mm(picks, sent_grad, 0, 0).astype(BF16)
    return (
        restored_out,
        restored_grad,
        small_part[0],
        small_part[1],
        qkv_part,
        qv_part,
        wout_part,
        small_part[2],
        small_part[3],
        small_part[4],
        up_part,
        bias_up_part,
        down_part,
        small_part[5],
    )


def solution(mesh):
    placed = (
        P(("dp", "tensor"), None),
        P(("dp", "tensor"), None),
        P(("dp", "tensor"), None),
        P("dp"),
        P("dp"),
        P("dp"),
        P("dp", None, "tensor"),
        P(None, "tensor"),
        P("tensor", "dp"),
        P("dp"),
        P("dp"),
        P("dp"),
        P("dp", "tensor"),
        P("tensor"),
        P("tensor", "dp"),
        P("dp"),
    )

    return jax.shard_map(
        per_device,
        mesh=mesh,
        in_specs=placed,
        out_specs=(
            P(("dp", "tensor"), None),
            P(("dp", "tensor"), None),
            P("dp"),
            P("dp"),
            P("dp", None, "tensor"),
            P(None, "tensor"),
            P("tensor", "dp"),
            P("dp"),
            P("dp"),
            P("dp"),
            P("dp", "tensor"),
            P("tensor"),
            P("tensor", "dp"),
            P("dp"),
        ),
        check_vma=False,
    )
```

```python
import functools

import jax
import jax.numpy as jnp
from jax import lax
from jax.experimental import pallas as pl
from jax.experimental.layout import Layout, with_layout_constraint
from jax.experimental.pallas import tpu as pltpu
from jax.sharding import PartitionSpec as P


HD = 64
LANES = 128
EPS = 1e-06
LN2 = 0.6931471805599453
LOG2E = 1.4426950408889634
GELU_ONE = 0.7978845608028654
GELU_THREE = 0.7978845608028654 * 0.044715
F32 = jnp.float32
BF16 = jnp.bfloat16


def normalize(values, gain_row, bias_row):
    centred = values - jnp.mean(values, axis=-1, keepdims=True)
    factor = lax.rsqrt(jnp.mean(centred * centred, axis=-1, keepdims=True) + EPS)
    normed = centred * factor
    return (normed * gain_row + bias_row, normed, factor)


def norm_back(grad_rows, normed, factor, gain_row):
    scaled = grad_rows * gain_row
    centred = scaled - jnp.mean(scaled, axis=-1, keepdims=True)
    return factor * (centred - normed * jnp.mean(scaled * normed, axis=-1, keepdims=True))


def mm(left, right, left_dim=1, right_dim=0):
    return lax.dot_general(
        left, right, (((left_dim,), (right_dim,)), ((), ())), preferred_element_type=F32
    )


def head_lanes(head):
    return (lax.broadcasted_iota(jnp.int32, (1, LANES), 1) // HD) == head


def attend_rows(q, keys, values):
    outs, lses = [], []
    one = jnp.ones((), BF16)
    for head in range(2):
        mine = head_lanes(head)
        scores = mm(jnp.where(mine, q, jnp.zeros_like(q)), keys, 1, 1)
        row_max = jnp.max(scores, axis=1, keepdims=True)
        weights = jnp.exp2(scores - row_max).astype(BF16)
        mixed = mm(weights, jnp.where(mine, values, one))
        total = jnp.sum(jnp.where(mine, 0.0, mixed), axis=1, keepdims=True) * (1.0 / HD)
        outs.append(mixed / total)
        lses.append(row_max + jnp.log2(total))
    first = head_lanes(0)
    return (jnp.where(first, outs[0], outs[1]), jnp.where(first, lses[0], lses[1]))


def own_forward(q_ref, kv_ref, mixed_ref, lse_ref, *, qblock):
    for block in range(q_ref.shape[0] // qblock):
        rows = pl.ds(block * qblock, qblock)
        mixed, lse = attend_rows(q_ref[rows, :], kv_ref[:, :LANES], kv_ref[:, LANES:])
        mixed_ref[rows, :] = mixed
        lse_ref[rows, :] = lse


def pair_forward(joined_ref, q_ref, kv_ref, own_ref, own_lse_ref, mixed_ref, lse_ref, *, qblock):
    joined = joined_ref[0] > 0

    @pl.when(joined)
    def _():
        for block in range(q_ref.shape[0] // qblock):
            rows = pl.ds(block * qblock, qblock)
            mixed, lse = attend_rows(q_ref[rows, :], kv_ref[:, :LANES], kv_ref[:, LANES:])
            own_lse = own_lse_ref[rows, :]
            top = jnp.maximum(own_lse, lse)
            own_share = jnp.exp2(own_lse - top)
            pair_share = jnp.exp2(lse - top)
            total = own_share + pair_share
            mixed_ref[rows, :] = (
                (own_ref[rows, :] * own_share + mixed * pair_share) / total
            ).astype(BF16)
            lse_ref[rows, :] = top + jnp.log2(total)

    @pl.when(jnp.logical_not(joined))
    def _():
        mixed_ref[...] = own_ref[...].astype(BF16)
        lse_ref[...] = own_lse_ref[...]


def split_three(values):
    high = values.astype(BF16)
    rest = values - high.astype(F32)
    middle = rest.astype(BF16)
    return high, middle, (rest - middle.astype(F32)).astype(BF16)


def attend_back(q_ref, grad_ref, mixed_ref, lse_ref, kv_ref, dkv_ref, dq_sum, kblock):
    lane = lax.broadcasted_iota(jnp.int32, (1, LANES), 1)
    q = q_ref[...]
    grad = grad_ref[...]
    products = grad.astype(F32) * mixed_ref[...].astype(F32)
    wide_q, wide_grad = [], []
    for head in range(2):
        mine = head_lanes(head)
        spare = (1 - head) * HD
        inner = jnp.sum(jnp.where(mine, products, 0.0), axis=1, keepdims=True)
        lse_parts = split_three(-lse_ref[:, head * HD : head * HD + 1])
        inner_parts = split_three(-inner)
        q_head = jnp.where(mine, q, jnp.zeros_like(q))
        grad_head = jnp.where(mine, grad, jnp.zeros_like(grad))
        for part in range(3):
            q_head = jnp.where(lane == spare + part, lse_parts[part], q_head)
            grad_head = jnp.where(lane == spare + part, inner_parts[part], grad_head)
        wide_q.append(q_head)
        wide_grad.append(grad_head)
    one = jnp.ones((), BF16)
    first = head_lanes(0)
    for block in range(kv_ref.shape[0] // kblock):
        rows = pl.ds(block * kblock, kblock)
        keys = kv_ref[rows, :LANES]
        values = kv_ref[rows, LANES:]
        key_grads, value_grads = [], []
        for head in range(2):
            mine = head_lanes(head)
            weights = jnp.exp2(mm(jnp.where(mine, keys, one), wide_q[head], 1, 1))
            grad_weights = mm(jnp.where(mine, values, one), wide_grad[head], 1, 1)
            grad_scores = (weights * grad_weights).astype(BF16)
            value_grads.append(mm(weights.astype(BF16), grad))
            key_grads.append(mm(grad_scores, q))
            dq_sum[head] += mm(keys, grad_scores, 0, 0)
        dkv_ref[rows, :LANES] = (jnp.where(first, key_grads[0], key_grads[1]) * LN2).astype(BF16)
        dkv_ref[rows, LANES:] = jnp.where(first, value_grads[0], value_grads[1]).astype(BF16)


def query_grad(dq_sum):
    return jnp.concatenate([dq_sum[0, :HD, :], dq_sum[1, HD:, :]], axis=0)


def pair_backward(
    joined_ref, q_ref, grad_ref, mixed_ref, lse_ref, kv_ref, dq_ref, dkv_ref, dq_sum, *, kblock
):
    joined = joined_ref[0] > 0
    dq_sum[...] = jnp.zeros_like(dq_sum)

    @pl.when(joined)
    def _():
        attend_back(q_ref, grad_ref, mixed_ref, lse_ref, kv_ref, dkv_ref, dq_sum, kblock)

    @pl.when(jnp.logical_not(joined))
    def _():
        dkv_ref[...] = jnp.zeros_like(dkv_ref)

    dq_ref[...] = query_grad(dq_sum)


def own_backward(
    q_ref, grad_ref, mixed_ref, lse_ref, kv_ref, pair_dq_ref, dq_ref, dkv_ref, dq_sum, *, kblock
):
    dq_sum[...] = jnp.zeros_like(dq_sum)
    attend_back(q_ref, grad_ref, mixed_ref, lse_ref, kv_ref, dkv_ref, dq_sum, kblock)
    total = query_grad(dq_sum) + pair_dq_ref[...]
    dq_ref[...] = (total.T * HD**-0.5).astype(BF16)


def params(**extra):
    return pltpu.CompilerParams(vmem_limit_bytes=56 << 20, **extra)


def cost(rows, keys, width, products):
    return pl.CostEstimate(
        flops=2 * rows * keys * width * products * 4,
        bytes_accessed=2 * width * (rows + 2 * keys),
        transcendentals=rows * keys * width // HD,
    )


def attention_own(qkv):
    rows = qkv.shape[0]
    width = qkv.shape[1] // 3
    pairs = width // LANES
    column = pl.BlockSpec((rows, LANES), lambda p: (0, p))
    own_kv = pl.BlockSpec((rows, 2 * LANES), lambda p: (0, pairs // 2 + p))
    shape = jax.ShapeDtypeStruct((rows, width), F32)
    return pl.pallas_call(
        functools.partial(own_forward, qblock=min(512, rows)),
        grid=(pairs,),
        in_specs=[column, own_kv],
        out_specs=[column, column],
        out_shape=[shape, shape],
        compiler_params=params(),
        cost_estimate=cost(rows, rows, width, 2),
        name="attend_own",
    )(qkv, qkv)


def attention_pair(joined, qkv, kv_of_pair, own, own_lse):
    rows, width = own.shape
    pairs = width // LANES
    column = pl.BlockSpec((rows, LANES), lambda p: (0, p))
    pair_kv = pl.BlockSpec((rows, 2 * LANES), lambda p: (0, p))
    return pl.pallas_call(
        functools.partial(pair_forward, qblock=min(512, rows)),
        grid=(pairs,),
        in_specs=[pl.BlockSpec(memory_space=pltpu.SMEM), column, pair_kv, column, column],
        out_specs=[column, column],
        out_shape=[
            jax.ShapeDtypeStruct((rows, width), BF16),
            jax.ShapeDtypeStruct((rows, width), F32),
        ],
        compiler_params=params(),
        cost_estimate=cost(rows, rows, width, 2),
        name="attend_pair",
    )(joined, qkv, kv_of_pair, own, own_lse)


def attention_back_pair(joined, qkv, kv_of_pair, grad, mixed, lse):
    rows, width = grad.shape
    pairs = width // LANES
    column = pl.BlockSpec((rows, LANES), lambda p: (0, p))
    pair_kv = pl.BlockSpec((rows, 2 * LANES), lambda p: (0, p))
    across = pl.BlockSpec((LANES, rows), lambda p: (p, 0))
    return pl.pallas_call(
        functools.partial(pair_backward, kblock=min(512, rows)),
        grid=(pairs,),
        in_specs=[pl.BlockSpec(memory_space=pltpu.SMEM)] + [column] * 4 + [pair_kv],
        out_specs=[across, pair_kv],
        out_shape=[
            jax.ShapeDtypeStruct((width, rows), F32),
            jax.ShapeDtypeStruct((rows, 2 * width), BF16),
        ],
        scratch_shapes=[pltpu.VMEM((2, LANES, rows), F32)],
        compiler_params=params(),
        cost_estimate=cost(rows, rows, width, 5),
        name="attend_back_pair",
    )(joined, qkv, grad, mixed, lse, kv_of_pair)


def attention_back_own(qkv, grad, mixed, lse, pair_dq):
    rows, width = grad.shape
    pairs = width // LANES
    column = pl.BlockSpec((rows, LANES), lambda p: (0, p))
    own_kv = pl.BlockSpec((rows, 2 * LANES), lambda p: (0, pairs // 2 + p))
    kv_out = pl.BlockSpec((rows, 2 * LANES), lambda p: (0, p))
    across = pl.BlockSpec((LANES, rows), lambda p: (p, 0))
    return pl.pallas_call(
        functools.partial(own_backward, kblock=min(512, rows)),
        grid=(pairs,),
        in_specs=[column] * 4 + [own_kv, across],
        out_specs=[column, kv_out],
        out_shape=[
            jax.ShapeDtypeStruct((rows, width), BF16),
            jax.ShapeDtypeStruct((rows, 2 * width), BF16),
        ],
        scratch_shapes=[pltpu.VMEM((2, LANES, rows), F32)],
        compiler_params=params(),
        cost_estimate=cost(rows, rows, width, 5),
        name="attend_back_own",
    )(qkv, grad, mixed, lse, qkv, pair_dq)


def small_kernel(n_dp, slice_ref, bias_ref, all_ref, partner_ref, send_sem, recv_sem):
    me = lax.axis_index("dp")
    t = lax.axis_index("tensor")

    barrier = pltpu.get_barrier_semaphore()

    def greet(step, carry):
        peer = lax.rem(me + step, n_dp)
        pl.semaphore_signal(
            barrier, inc=1, device_id=(peer, t), device_id_type=pl.DeviceIdType.MESH
        )
        return carry

    lax.fori_loop(1, n_dp, greet, 0)
    pl.semaphore_signal(
        barrier, inc=1, device_id=(me, 1 - t), device_id_type=pl.DeviceIdType.MESH
    )
    pl.semaphore_wait(barrier, n_dp)

    def to_peer(step):
        return pltpu.make_async_remote_copy(
            src_ref=slice_ref,
            dst_ref=all_ref.at[me],
            send_sem=send_sem.at[step],
            recv_sem=recv_sem.at[step],
            device_id=(lax.rem(me + step, n_dp), t),
            device_id_type=pl.DeviceIdType.MESH,
        )

    to_partner = pltpu.make_async_remote_copy(
        src_ref=bias_ref,
        dst_ref=partner_ref,
        send_sem=send_sem.at[0],
        recv_sem=recv_sem.at[0],
        device_id=(me, 1 - t),
        device_id_type=pl.DeviceIdType.MESH,
    )
    to_partner.start()

    def start(step, carry):
        to_peer(step).start()
        return carry

    def finish(step, carry):
        to_peer(step).wait()
        return carry

    lax.fori_loop(1, n_dp, start, 0)
    all_ref[me] = slice_ref[...]
    lax.fori_loop(1, n_dp, finish, 0)
    to_partner.wait()


def share_small(n_dp, slices, biases):
    vmem = pl.BlockSpec(memory_space=pltpu.VMEM)
    return pl.pallas_call(
        functools.partial(small_kernel, n_dp),
        in_specs=[vmem, vmem],
        out_specs=[vmem, vmem],
        out_shape=[
            jax.ShapeDtypeStruct((n_dp,) + slices.shape, F32),
            jax.ShapeDtypeStruct(biases.shape, F32),
        ],
        scratch_shapes=[
            pltpu.SemaphoreType.DMA((n_dp,)),
            pltpu.SemaphoreType.DMA((n_dp,)),
        ],
        compiler_params=pltpu.CompilerParams(collective_id=0, has_side_effects=True),
        name="share_small",
    )(slices, biases)


def by_rows(values):
    return with_layout_constraint(values, Layout((0, 1)))


def after(*values):
    return lax.optimization_barrier(values)


def swap(values):
    return lax.ppermute(values, "tensor", [(0, 1), (1, 0)])


def tree_gather(n_dp, t, values, split):
    me = lax.axis_index("dp")

    def joined(own, other, upper, axis):
        return jnp.where(
            upper, jnp.concatenate([other, own], axis=axis), jnp.concatenate([own, other], axis=axis)
        )

    blocks = values[None]
    steps = [1 << bit for bit in range(n_dp.bit_length() - 1)]
    for step in reversed(steps[1:]):
        other = lax.ppermute(blocks, "dp", [(i, i ^ step) for i in range(n_dp)])
        upper = (me // step) % 2 == 1
        blocks = joined(blocks[:, None], other[:, None], upper, 1).reshape((-1,) + values.shape)
    other = swap(blocks)
    blocks = jnp.concatenate(
        [
            joined(blocks[..., :split], other[..., :split], t == 1, 2),
            joined(blocks[..., split:], other[..., split:], t == 1, 2),
        ],
        axis=2,
    )
    other = lax.ppermute(blocks, "dp", [(i, i ^ 1) for i in range(n_dp)])
    full = joined(blocks[:, None], other[:, None], me % 2 == 1, 1)
    full = full.reshape(n_dp * values.shape[0], 2 * values.shape[1])
    return full


def tree_sum(n_dp, piece, t, values, rows):
    me = lax.axis_index("dp")
    columns = values.shape[1]

    def add(first, second, upper, rows, exchange):
        mine = jnp.where(upper, second, first)
        sent, rows = after(jnp.where(upper, first, second), rows)
        arrived, arrived_rows = after(exchange(sent), exchange(rows))
        total = (mine.astype(F32) + arrived.astype(F32)).astype(BF16)
        return total, rows + arrived_rows

    def along_dp(total, rows, step):
        blocks = total.reshape(-1, 2, piece, total.shape[-1])
        partners = [(i, i ^ step) for i in range(n_dp)]
        return add(
            blocks[:, 0],
            blocks[:, 1],
            (me // step) % 2 == 1,
            rows,
            lambda v: lax.ppermute(v, "dp", partners),
        )

    total, rows = along_dp(values, rows, 1)
    low, high = total[..., : columns // 2], total[..., columns // 2 :]
    total, rows = add(low, high, t == 1, rows, swap)
    step = 2
    while step < n_dp:
        total, rows = along_dp(total, rows, step)
        step *= 2
    return total.reshape(piece, columns // 2).astype(F32), rows


def per_device(
    tokens,
    grad_tokens,
    dealing,
    segment_ids,
    ln1_gain,
    ln1_bias,
    w_qkv,
    b_qv,
    w_out,
    b_out,
    ln2_gain,
    ln2_bias,
    w_up,
    b_up,
    w_down,
    b_down,
):
    n_dp = lax.axis_size("dp")
    t = lax.axis_index("tensor")
    rows, width = tokens.shape
    piece = ln1_gain.shape[0]
    half = b_qv.shape[1]
    hidden_half = b_up.shape[0]
    pairs = width // LANES

    def join(own, other, axis):
        return jnp.where(
            t == 0,
            jnp.concatenate([own, other], axis=axis),
            jnp.concatenate([other, own], axis=axis),
        )

    def reduced(values):
        return lax.psum_scatter(values, "dp", scatter_dimension=0, tiled=True)

    def mine_of(values, axis):
        size = values.shape[axis] // 2
        low, high = (
            lax.slice_in_dim(values, 0, size, axis=axis),
            lax.slice_in_dim(values, size, 2 * size, axis=axis),
        )
        return jnp.where(t == 0, low, high), jnp.where(t == 0, high, low)

    kv_local = (
        w_qkv[:, 1:]
        .reshape(piece, 2, pairs // 2, LANES)
        .transpose(0, 2, 1, 3)
        .reshape(piece, 2 * half)
    )
    wqkv = tree_gather(n_dp, t, jnp.concatenate([w_qkv[:, 0], kv_local], axis=1), half)
    wq, wkv = wqkv[:, :width], wqkv[:, width:]
    rest_local = jnp.concatenate([w_out.T, w_up, w_down.T], axis=1)
    other_rest = swap(rest_local)
    up_at, down_at = half, half + hidden_half
    rest_local = jnp.concatenate(
        [
            join(rest_local[:, :up_at], other_rest[:, :up_at], 1),
            join(rest_local[:, up_at:down_at], other_rest[:, up_at:down_at], 1),
            join(rest_local[:, down_at:], other_rest[:, down_at:], 1),
        ],
        axis=1,
    )
    rest = lax.all_gather(rest_local, "dp", axis=0, tiled=True)
    wout_t = rest[:, :width]
    wup = rest[:, width : width + 2 * hidden_half]
    wdown_t = rest[:, width + 2 * hidden_half :]

    small = jnp.stack([ln1_gain, ln1_bias, b_out, ln2_gain, ln2_bias, b_down])
    small = jnp.pad(small, ((0, 2), (0, LANES - piece)))
    biases = jnp.concatenate([b_qv.reshape(-1), b_up])
    bias_rows = -(-biases.shape[0] // (8 * LANES)) * 8
    biases = jnp.pad(biases, (0, bias_rows * LANES - biases.shape[0]))
    biases = biases.reshape(bias_rows, LANES)
    small_all, other_biases = share_small(n_dp, small, biases)
    row_order = dealing[0]
    picks = (row_order[:, None] == jnp.arange(rows, dtype=jnp.int32)[None, :]).astype(BF16)
    sent_rows = mm(picks, tokens).astype(BF16)
    dealt = lax.all_to_all(sent_rows, "dp", split_axis=0, concat_axis=0, tiled=True)
    grad_tokens, dealt = after(grad_tokens, dealt)
    sent_grads = mm(picks, grad_tokens).astype(BF16)
    grad_out = lax.all_to_all(sent_grads, "dp", split_axis=0, concat_axis=0, tiled=True)
    dealt_of_pair = by_rows(swap(dealt))
    joined = (segment_ids[:1] == segment_ids[-1:]).astype(jnp.int32)

    small_full = small_all[:, :6, :piece].transpose(1, 0, 2).reshape(6, width)
    flat, other_flat = biases.reshape(-1), other_biases.reshape(-1)
    bqv_full = join(flat[: 2 * half].reshape(2, half), other_flat[: 2 * half].reshape(2, half), 1)
    bup_full = join(
        flat[2 * half : 2 * half + hidden_half],
        other_flat[2 * half : 2 * half + hidden_half],
        0,
    )

    resid = by_rows(dealt.astype(F32))
    ln_one, normed_one, factor_one = normalize(resid, small_full[0], small_full[1])
    ln_one = ln_one.astype(BF16)
    kv_bias = jnp.stack(
        [jnp.zeros((pairs, LANES), F32), bqv_full[1].reshape(pairs, LANES)], axis=1
    ).reshape(-1)
    score_scale = HD**-0.5 * LOG2E
    shift = jnp.concatenate([bqv_full[0] * score_scale, kv_bias])
    scale = jnp.concatenate([jnp.full((width,), score_scale, F32), jnp.ones((2 * width,), F32)])
    qkv = (mm(ln_one, wqkv) * scale + shift).astype(BF16)
    own, own_lse = attention_own(qkv)
    dealt_of_pair, own = after(dealt_of_pair, own)
    ln_of_pair = normalize(dealt_of_pair.astype(F32), small_full[0], small_full[1])[0].astype(BF16)
    kv_of_pair = (mm(ln_of_pair, wkv) + kv_bias).astype(BF16)
    attended, lse = attention_pair(joined, qkv, kv_of_pair, own, own_lse)
    hidden = by_rows(resid + mm(attended, wout_t, 1, 1) + small_full[2])

    ln_two, normed_two, factor_two = normalize(hidden, small_full[3], small_full[4])
    ln_two = ln_two.astype(BF16)
    pre_act = mm(ln_two, wup) + bup_full
    square = pre_act * pre_act
    bend = jnp.tanh(pre_act * (GELU_ONE + GELU_THREE * square))
    gate = 0.5 + 0.5 * bend
    slope = gate + (0.5 * pre_act) * (1.0 - bend * bend) * (GELU_ONE + 3.0 * GELU_THREE * square)
    act, slope = after((pre_act * gate).astype(BF16), slope.astype(BF16))

    grad_down_t = mm(grad_out, act, 0, 0).astype(BF16)
    grad_pre = (mm(grad_out, wdown_t) * slope.astype(F32)).astype(BF16)
    bias_up_grad = jnp.sum(grad_pre, axis=0, dtype=F32)
    grad_up = mm(ln_two, grad_pre, 0, 0).astype(BF16)
    grad_down_t, grad_up, grad_pre = after(grad_down_t, grad_up, grad_pre)
    grad_ln_two = by_rows(mm(grad_pre, wup, 1, 1))
    gain_two_grad = jnp.sum(grad_ln_two * normed_two, axis=0)
    bias_two_grad = jnp.sum(grad_ln_two, axis=0)
    grad_hidden = grad_out.astype(F32) + norm_back(
        grad_ln_two, normed_two, factor_two, small_full[3]
    )
    grad_branch = grad_hidden.astype(BF16)
    grad_wout_t = mm(grad_branch, attended, 0, 0).astype(BF16)
    mlp_grads = jnp.concatenate([grad_down_t, grad_up, grad_wout_t], axis=1)
    mlp_grads, grad_branch, act = after(mlp_grads, grad_branch, act)
    mlp_sum = reduced(mlp_grads)
    grad_att = mm(grad_branch, wout_t).astype(BF16)
    output = by_rows((hidden + mm(act, wdown_t, 1, 1) + small_full[5]).astype(BF16))
    grad_att, output = after(grad_att, output)

    pair_dq, pair_dkv = attention_back_pair(
        joined, qkv, kv_of_pair, grad_att, attended, lse
    )
    for_pair = mm(pair_dkv, wkv, 1, 1).astype(BF16)
    for_pair = swap(for_pair)
    dq, dkv = attention_back_own(qkv, grad_att, attended, lse, pair_dq)
    grad_ln_one = by_rows(mm(dq, wq, 1, 1) + mm(dkv, wkv, 1, 1) + for_pair.astype(F32))
    grad_input = (
        grad_hidden + norm_back(grad_ln_one, normed_one, factor_one, small_full[0])
    ).astype(BF16)
    dq, dkv, grad_input = after(dq, dkv, grad_input)
    grad_wq = mm(ln_one, dq, 0, 0).astype(BF16)
    grad_wkv = (mm(ln_one, dkv, 0, 0) + mm(ln_of_pair, pair_dkv, 0, 0)).astype(BF16)
    bias_q_grad = jnp.sum(dq, axis=0, dtype=F32)
    kv_sum = jnp.sum(dkv, axis=0, dtype=F32) + jnp.sum(pair_dkv, axis=0, dtype=F32)
    bias_v_grad = kv_sum.reshape(pairs, 2, LANES)[:, 1].reshape(-1)
    grad_wqkv = jnp.concatenate(
        [grad_wq[:, :half], grad_wkv[:, : 2 * half], grad_wq[:, half:], grad_wkv[:, 2 * half :]],
        axis=1,
    )
    row_sums = jnp.concatenate(
        [
            jnp.stack(
                [
                    jnp.sum(grad_ln_one * normed_one, axis=0),
                    jnp.sum(grad_ln_one, axis=0),
                    jnp.sum(grad_hidden, axis=0),
                    gain_two_grad,
                    bias_two_grad,
                    jnp.sum(grad_out, axis=0, dtype=F32),
                    bias_q_grad,
                    bias_v_grad,
                ]
            ),
            bias_up_grad.reshape(-1, width),
        ]
    )
    qkv_part, row_sums = tree_sum(n_dp, piece, t, grad_wqkv, row_sums)
    small_part = lax.dynamic_slice_in_dim(
        row_sums[:6], lax.axis_index("dp") * piece, piece, 1
    )
    qv_part = mine_of(row_sums[6:8], 1)[0]
    bias_up_part = mine_of(row_sums[8:].reshape(-1), 0)[0]

    def paired(values, sizes):
        columns, start = [], 0
        for size in sizes:
            columns.append(mine_of(values[:, start : start + size], 1))
            start += size
        mine = jnp.concatenate([c[0] for c in columns], axis=1)
        other = jnp.concatenate([c[1] for c in columns], axis=1)
        total = mine.astype(F32) + swap(other).astype(F32)
        cuts = [sum(sizes[:i]) // 2 for i in range(1, len(sizes))]
        return jnp.split(total, cuts, axis=1)

    down_part, up_part, wout_part = paired(mlp_sum, (2 * hidden_half, 2 * hidden_half, width))
    down_part, wout_part = down_part.T, wout_part.T
    q_part, kv_part = qkv_part[:, :half], qkv_part[:, half:]
    kv_part = kv_part.reshape(piece, pairs // 2, 2, LANES).transpose(0, 2, 1, 3)
    qkv_part = jnp.concatenate(
        [q_part.reshape(piece, 1, half), kv_part.reshape(piece, 2, half)], axis=1
    )

    sent_out = lax.all_to_all(output, "dp", split_axis=0, concat_axis=0, tiled=True)
    sent_grad = lax.all_to_all(grad_input, "dp", split_axis=0, concat_axis=0, tiled=True)
    restored_out = mm(picks, sent_out, 0, 0).astype(BF16)
    restored_grad = mm(picks, sent_grad, 0, 0).astype(BF16)
    return (
        restored_out,
        restored_grad,
        small_part[0],
        small_part[1],
        qkv_part,
        qv_part,
        wout_part,
        small_part[2],
        small_part[3],
        small_part[4],
        up_part,
        bias_up_part,
        down_part,
        small_part[5],
    )


def solution(mesh):
    placed = (
        P(("dp", "tensor"), None),
        P(("dp", "tensor"), None),
        P(("dp", "tensor"), None),
        P("dp"),
        P("dp"),
        P("dp"),
        P("dp", None, "tensor"),
        P(None, "tensor"),
        P("tensor", "dp"),
        P("dp"),
        P("dp"),
        P("dp"),
        P("dp", "tensor"),
        P("tensor"),
        P("tensor", "dp"),
        P("dp"),
    )

    return jax.shard_map(
        per_device,
        mesh=mesh,
        in_specs=placed,
        out_specs=(
            P(("dp", "tensor"), None),
            P(("dp", "tensor"), None),
            P("dp"),
            P("dp"),
            P("dp", None, "tensor"),
            P(None, "tensor"),
            P("tensor", "dp"),
            P("dp"),
            P("dp"),
            P("dp"),
            P("dp", "tensor"),
            P("tensor"),
            P("tensor", "dp"),
            P("dp"),
        ),
        check_vma=False,
    )
```

```python
import functools

import jax
import jax.numpy as jnp
from jax import lax
from jax.experimental import pallas as pl
from jax.experimental.layout import Layout, with_layout_constraint
from jax.experimental.pallas import tpu as pltpu
from jax.sharding import PartitionSpec as P


HD = 64
LANES = 128
EPS = 1e-06
LN2 = 0.6931471805599453
LOG2E = 1.4426950408889634
GELU_ONE = 0.7978845608028654
GELU_THREE = 0.7978845608028654 * 0.044715
F32 = jnp.float32
BF16 = jnp.bfloat16


def normalize(values, gain_row, bias_row):
    centred = values - jnp.mean(values, axis=-1, keepdims=True)
    factor = lax.rsqrt(jnp.mean(centred * centred, axis=-1, keepdims=True) + EPS)
    normed = centred * factor
    return (normed * gain_row + bias_row, normed, factor)


def norm_back(grad_rows, normed, factor, gain_row):
    scaled = grad_rows * gain_row
    centred = scaled - jnp.mean(scaled, axis=-1, keepdims=True)
    return factor * (centred - normed * jnp.mean(scaled * normed, axis=-1, keepdims=True))


def mm(left, right, left_dim=1, right_dim=0):
    return lax.dot_general(
        left, right, (((left_dim,), (right_dim,)), ((), ())), preferred_element_type=F32
    )


def head_lanes(head):
    return (lax.broadcasted_iota(jnp.int32, (1, LANES), 1) // HD) == head


def attend_rows(q, keys, values):
    outs, lses = [], []
    one = jnp.ones((), BF16)
    for head in range(2):
        mine = head_lanes(head)
        scores = mm(jnp.where(mine, q, jnp.zeros_like(q)), keys, 1, 1)
        row_max = jnp.max(scores, axis=1, keepdims=True)
        weights = jnp.exp2(scores - row_max).astype(BF16)
        mixed = mm(weights, jnp.where(mine, values, one))
        total = jnp.sum(jnp.where(mine, 0.0, mixed), axis=1, keepdims=True) * (1.0 / HD)
        outs.append(mixed / total)
        lses.append(row_max + jnp.log2(total))
    first = head_lanes(0)
    return (jnp.where(first, outs[0], outs[1]), jnp.where(first, lses[0], lses[1]))


def own_forward(q_ref, kv_ref, mixed_ref, lse_ref, *, qblock):
    for block in range(q_ref.shape[0] // qblock):
        rows = pl.ds(block * qblock, qblock)
        mixed, lse = attend_rows(q_ref[rows, :], kv_ref[:, :LANES], kv_ref[:, LANES:])
        mixed_ref[rows, :] = mixed
        lse_ref[rows, :] = lse


def pair_forward(joined_ref, q_ref, kv_ref, own_ref, own_lse_ref, mixed_ref, lse_ref, *, qblock):
    joined = joined_ref[0] > 0

    @pl.when(joined)
    def _():
        for block in range(q_ref.shape[0] // qblock):
            rows = pl.ds(block * qblock, qblock)
            mixed, lse = attend_rows(q_ref[rows, :], kv_ref[:, :LANES], kv_ref[:, LANES:])
            own_lse = own_lse_ref[rows, :]
            top = jnp.maximum(own_lse, lse)
            own_share = jnp.exp2(own_lse - top)
            pair_share = jnp.exp2(lse - top)
            total = own_share + pair_share
            mixed_ref[rows, :] = (
                (own_ref[rows, :] * own_share + mixed * pair_share) / total
            ).astype(BF16)
            lse_ref[rows, :] = top + jnp.log2(total)

    @pl.when(jnp.logical_not(joined))
    def _():
        mixed_ref[...] = own_ref[...].astype(BF16)
        lse_ref[...] = own_lse_ref[...]


def split_three(values):
    high = values.astype(BF16)
    rest = values - high.astype(F32)
    middle = rest.astype(BF16)
    return high, middle, (rest - middle.astype(F32)).astype(BF16)


def attend_back(q_ref, grad_ref, mixed_ref, lse_ref, kv_ref, dkv_ref, dq_sum, kblock):
    lane = lax.broadcasted_iota(jnp.int32, (1, LANES), 1)
    q = q_ref[...]
    grad = grad_ref[...]
    products = grad.astype(F32) * mixed_ref[...].astype(F32)
    wide_q, wide_grad = [], []
    for head in range(2):
        mine = head_lanes(head)
        spare = (1 - head) * HD
        inner = jnp.sum(jnp.where(mine, products, 0.0), axis=1, keepdims=True)
        lse_parts = split_three(-lse_ref[:, head * HD : head * HD + 1])
        inner_parts = split_three(-inner)
        q_head = jnp.where(mine, q, jnp.zeros_like(q))
        grad_head = jnp.where(mine, grad, jnp.zeros_like(grad))
        for part in range(3):
            q_head = jnp.where(lane == spare + part, lse_parts[part], q_head)
            grad_head = jnp.where(lane == spare + part, inner_parts[part], grad_head)
        wide_q.append(q_head)
        wide_grad.append(grad_head)
    one = jnp.ones((), BF16)
    first = head_lanes(0)
    for block in range(kv_ref.shape[0] // kblock):
        rows = pl.ds(block * kblock, kblock)
        keys = kv_ref[rows, :LANES]
        values = kv_ref[rows, LANES:]
        key_grads, value_grads = [], []
        for head in range(2):
            mine = head_lanes(head)
            weights = jnp.exp2(mm(jnp.where(mine, keys, one), wide_q[head], 1, 1))
            grad_weights = mm(jnp.where(mine, values, one), wide_grad[head], 1, 1)
            grad_scores = (weights * grad_weights).astype(BF16)
            value_grads.append(mm(weights.astype(BF16), grad))
            key_grads.append(mm(grad_scores, q))
            dq_sum[head] += mm(keys, grad_scores, 0, 0)
        dkv_ref[rows, :LANES] = (jnp.where(first, key_grads[0], key_grads[1]) * LN2).astype(BF16)
        dkv_ref[rows, LANES:] = jnp.where(first, value_grads[0], value_grads[1]).astype(BF16)


def query_grad(dq_sum):
    return jnp.concatenate([dq_sum[0, :HD, :], dq_sum[1, HD:, :]], axis=0)


def pair_backward(
    joined_ref, q_ref, grad_ref, mixed_ref, lse_ref, kv_ref, dq_ref, dkv_ref, dq_sum, *, kblock
):
    joined = joined_ref[0] > 0
    dq_sum[...] = jnp.zeros_like(dq_sum)

    @pl.when(joined)
    def _():
        attend_back(q_ref, grad_ref, mixed_ref, lse_ref, kv_ref, dkv_ref, dq_sum, kblock)

    @pl.when(jnp.logical_not(joined))
    def _():
        dkv_ref[...] = jnp.zeros_like(dkv_ref)

    dq_ref[...] = query_grad(dq_sum)


def own_backward(
    q_ref, grad_ref, mixed_ref, lse_ref, kv_ref, pair_dq_ref, dq_ref, dkv_ref, dq_sum, *, kblock
):
    dq_sum[...] = jnp.zeros_like(dq_sum)
    attend_back(q_ref, grad_ref, mixed_ref, lse_ref, kv_ref, dkv_ref, dq_sum, kblock)
    total = query_grad(dq_sum) + pair_dq_ref[...]
    dq_ref[...] = (total.T * HD**-0.5).astype(BF16)


def params(**extra):
    return pltpu.CompilerParams(vmem_limit_bytes=56 << 20, **extra)


def cost(rows, keys, width, products):
    return pl.CostEstimate(
        flops=2 * rows * keys * width * products * 4,
        bytes_accessed=2 * width * (rows + 2 * keys),
        transcendentals=rows * keys * width // HD,
    )


def attention_own(qkv):
    rows = qkv.shape[0]
    width = qkv.shape[1] // 3
    pairs = width // LANES
    column = pl.BlockSpec((rows, LANES), lambda p: (0, p))
    own_kv = pl.BlockSpec((rows, 2 * LANES), lambda p: (0, pairs // 2 + p))
    shape = jax.ShapeDtypeStruct((rows, width), F32)
    return pl.pallas_call(
        functools.partial(own_forward, qblock=min(512, rows)),
        grid=(pairs,),
        in_specs=[column, own_kv],
        out_specs=[column, column],
        out_shape=[shape, shape],
        compiler_params=params(),
        cost_estimate=cost(rows, rows, width, 2),
        name="attend_own",
    )(qkv, qkv)


def attention_pair(joined, qkv, kv_of_pair, own, own_lse):
    rows, width = own.shape
    pairs = width // LANES
    column = pl.BlockSpec((rows, LANES), lambda p: (0, p))
    pair_kv = pl.BlockSpec((rows, 2 * LANES), lambda p: (0, p))
    return pl.pallas_call(
        functools.partial(pair_forward, qblock=min(512, rows)),
        grid=(pairs,),
        in_specs=[pl.BlockSpec(memory_space=pltpu.SMEM), column, pair_kv, column, column],
        out_specs=[column, column],
        out_shape=[
            jax.ShapeDtypeStruct((rows, width), BF16),
            jax.ShapeDtypeStruct((rows, width), F32),
        ],
        compiler_params=params(),
        cost_estimate=cost(rows, rows, width, 2),
        name="attend_pair",
    )(joined, qkv, kv_of_pair, own, own_lse)


def attention_back_pair(joined, qkv, kv_of_pair, grad, mixed, lse):
    rows, width = grad.shape
    pairs = width // LANES
    column = pl.BlockSpec((rows, LANES), lambda p: (0, p))
    pair_kv = pl.BlockSpec((rows, 2 * LANES), lambda p: (0, p))
    across = pl.BlockSpec((LANES, rows), lambda p: (p, 0))
    return pl.pallas_call(
        functools.partial(pair_backward, kblock=min(512, rows)),
        grid=(pairs,),
        in_specs=[pl.BlockSpec(memory_space=pltpu.SMEM)] + [column] * 4 + [pair_kv],
        out_specs=[across, pair_kv],
        out_shape=[
            jax.ShapeDtypeStruct((width, rows), F32),
            jax.ShapeDtypeStruct((rows, 2 * width), BF16),
        ],
        scratch_shapes=[pltpu.VMEM((2, LANES, rows), F32)],
        compiler_params=params(),
        cost_estimate=cost(rows, rows, width, 5),
        name="attend_back_pair",
    )(joined, qkv, grad, mixed, lse, kv_of_pair)


def attention_back_own(qkv, grad, mixed, lse, pair_dq):
    rows, width = grad.shape
    pairs = width // LANES
    column = pl.BlockSpec((rows, LANES), lambda p: (0, p))
    own_kv = pl.BlockSpec((rows, 2 * LANES), lambda p: (0, pairs // 2 + p))
    kv_out = pl.BlockSpec((rows, 2 * LANES), lambda p: (0, p))
    across = pl.BlockSpec((LANES, rows), lambda p: (p, 0))
    return pl.pallas_call(
        functools.partial(own_backward, kblock=min(512, rows)),
        grid=(pairs,),
        in_specs=[column] * 4 + [own_kv, across],
        out_specs=[column, kv_out],
        out_shape=[
            jax.ShapeDtypeStruct((rows, width), BF16),
            jax.ShapeDtypeStruct((rows, 2 * width), BF16),
        ],
        scratch_shapes=[pltpu.VMEM((2, LANES, rows), F32)],
        compiler_params=params(),
        cost_estimate=cost(rows, rows, width, 5),
        name="attend_back_own",
    )(qkv, grad, mixed, lse, qkv, pair_dq)


def small_kernel(n_dp, slice_ref, bias_ref, all_ref, partner_ref, send_sem, recv_sem):
    me = lax.axis_index("dp")
    t = lax.axis_index("tensor")

    barrier = pltpu.get_barrier_semaphore()

    def greet(step, carry):
        peer = lax.rem(me + step, n_dp)
        pl.semaphore_signal(
            barrier, inc=1, device_id=(peer, t), device_id_type=pl.DeviceIdType.MESH
        )
        return carry

    lax.fori_loop(1, n_dp, greet, 0)
    pl.semaphore_signal(
        barrier, inc=1, device_id=(me, 1 - t), device_id_type=pl.DeviceIdType.MESH
    )
    pl.semaphore_wait(barrier, n_dp)

    def to_peer(step):
        return pltpu.make_async_remote_copy(
            src_ref=slice_ref,
            dst_ref=all_ref.at[me],
            send_sem=send_sem.at[step],
            recv_sem=recv_sem.at[step],
            device_id=(lax.rem(me + step, n_dp), t),
            device_id_type=pl.DeviceIdType.MESH,
        )

    to_partner = pltpu.make_async_remote_copy(
        src_ref=bias_ref,
        dst_ref=partner_ref,
        send_sem=send_sem.at[0],
        recv_sem=recv_sem.at[0],
        device_id=(me, 1 - t),
        device_id_type=pl.DeviceIdType.MESH,
    )
    to_partner.start()

    def start(step, carry):
        to_peer(step).start()
        return carry

    def finish(step, carry):
        to_peer(step).wait()
        return carry

    lax.fori_loop(1, n_dp, start, 0)
    all_ref[me] = slice_ref[...]
    lax.fori_loop(1, n_dp, finish, 0)
    to_partner.wait()


def share_small(n_dp, slices, biases):
    vmem = pl.BlockSpec(memory_space=pltpu.VMEM)
    return pl.pallas_call(
        functools.partial(small_kernel, n_dp),
        in_specs=[vmem, vmem],
        out_specs=[vmem, vmem],
        out_shape=[
            jax.ShapeDtypeStruct((n_dp,) + slices.shape, F32),
            jax.ShapeDtypeStruct(biases.shape, F32),
        ],
        scratch_shapes=[
            pltpu.SemaphoreType.DMA((n_dp,)),
            pltpu.SemaphoreType.DMA((n_dp,)),
        ],
        compiler_params=pltpu.CompilerParams(collective_id=0, has_side_effects=True),
        name="share_small",
    )(slices, biases)


def by_rows(values):
    return with_layout_constraint(values, Layout((0, 1)))


def after(*values):
    return lax.optimization_barrier(values)


def swap(values):
    return lax.ppermute(values, "tensor", [(0, 1), (1, 0)])


def tree_gather(n_dp, t, values, split):
    me = lax.axis_index("dp")

    def joined(own, other, upper, axis):
        return jnp.where(
            upper, jnp.concatenate([other, own], axis=axis), jnp.concatenate([own, other], axis=axis)
        )

    blocks = values[None]
    steps = [1 << bit for bit in range(n_dp.bit_length() - 1)]
    for step in reversed(steps[1:]):
        other = lax.ppermute(blocks, "dp", [(i, i ^ step) for i in range(n_dp)])
        upper = (me // step) % 2 == 1
        blocks = joined(blocks[:, None], other[:, None], upper, 1).reshape((-1,) + values.shape)
    other = swap(blocks)
    blocks = jnp.concatenate(
        [
            joined(blocks[..., :split], other[..., :split], t == 1, 2),
            joined(blocks[..., split:], other[..., split:], t == 1, 2),
        ],
        axis=2,
    )
    other = lax.ppermute(blocks, "dp", [(i, i ^ 1) for i in range(n_dp)])
    full = joined(blocks[:, None], other[:, None], me % 2 == 1, 1)
    full = full.reshape(n_dp * values.shape[0], 2 * values.shape[1])
    return full


def dp_partners(n_dp, step):
    return [(i, i ^ step) for i in range(n_dp)]


def add_half(first, second, upper, exchange):
    mine = jnp.where(upper, second, first)
    arrived = exchange(jnp.where(upper, first, second))
    return (mine.astype(F32) + arrived.astype(F32)).astype(BF16)


def sum_on_chip(n_dp, piece, values):
    odd = lax.axis_index("dp") % 2 == 1
    blocks = values.reshape(n_dp // 2, 2, piece, values.shape[-1])
    return add_half(
        blocks[:, 0], blocks[:, 1], odd, lambda v: lax.ppermute(v, "dp", dp_partners(n_dp, 1))
    )


def sum_over_tensor(t, values):
    low, high = jnp.split(values, 2, axis=-1)
    return add_half(low, high, t == 1, swap)


def tree_sum(n_dp, piece, total, rows):
    me = lax.axis_index("dp")
    arrived_rows = lax.ppermute(rows, "dp", dp_partners(n_dp, 1))
    rows = rows + arrived_rows
    arrived_rows = swap(rows)
    rows = rows + arrived_rows
    step = 2
    while step < n_dp:
        blocks = total.reshape(-1, 2, piece, total.shape[-1])
        upper = (me // step) % 2 == 1
        sent, rows = after(jnp.where(upper, blocks[:, 0], blocks[:, 1]), rows)
        partners = dp_partners(n_dp, step)
        arrived, arrived_rows = after(
            lax.ppermute(sent, "dp", partners), lax.ppermute(rows, "dp", partners)
        )
        mine = jnp.where(upper, blocks[:, 1], blocks[:, 0])
        total = (mine.astype(F32) + arrived.astype(F32)).astype(BF16)
        rows = rows + arrived_rows
        step *= 2
    return total.reshape(piece, -1).astype(F32), rows


def per_device(
    tokens,
    grad_tokens,
    dealing,
    segment_ids,
    ln1_gain,
    ln1_bias,
    w_qkv,
    b_qv,
    w_out,
    b_out,
    ln2_gain,
    ln2_bias,
    w_up,
    b_up,
    w_down,
    b_down,
):
    n_dp = lax.axis_size("dp")
    t = lax.axis_index("tensor")
    rows, width = tokens.shape
    piece = ln1_gain.shape[0]
    half = b_qv.shape[1]
    hidden_half = b_up.shape[0]
    pairs = width // LANES

    def join(own, other, axis):
        return jnp.where(
            t == 0,
            jnp.concatenate([own, other], axis=axis),
            jnp.concatenate([other, own], axis=axis),
        )

    def reduced(values):
        return lax.psum_scatter(values, "dp", scatter_dimension=0, tiled=True)

    def mine_of(values, axis):
        size = values.shape[axis] // 2
        low, high = (
            lax.slice_in_dim(values, 0, size, axis=axis),
            lax.slice_in_dim(values, size, 2 * size, axis=axis),
        )
        return jnp.where(t == 0, low, high), jnp.where(t == 0, high, low)

    kv_local = (
        w_qkv[:, 1:]
        .reshape(piece, 2, pairs // 2, LANES)
        .transpose(0, 2, 1, 3)
        .reshape(piece, 2 * half)
    )
    wqkv = tree_gather(n_dp, t, jnp.concatenate([w_qkv[:, 0], kv_local], axis=1), half)
    wq, wkv = wqkv[:, :width], wqkv[:, width:]
    rest_local = jnp.concatenate([w_out.T, w_up, w_down.T], axis=1)
    other_rest = swap(rest_local)
    up_at, down_at = half, half + hidden_half
    rest_local = jnp.concatenate(
        [
            join(rest_local[:, :up_at], other_rest[:, :up_at], 1),
            join(rest_local[:, up_at:down_at], other_rest[:, up_at:down_at], 1),
            join(rest_local[:, down_at:], other_rest[:, down_at:], 1),
        ],
        axis=1,
    )
    rest = lax.all_gather(rest_local, "dp", axis=0, tiled=True)
    wout_t = rest[:, :width]
    wup = rest[:, width : width + 2 * hidden_half]
    wdown_t = rest[:, width + 2 * hidden_half :]

    small = jnp.stack([ln1_gain, ln1_bias, b_out, ln2_gain, ln2_bias, b_down])
    small = jnp.pad(small, ((0, 2), (0, LANES - piece)))
    biases = jnp.concatenate([b_qv.reshape(-1), b_up])
    bias_rows = -(-biases.shape[0] // (8 * LANES)) * 8
    biases = jnp.pad(biases, (0, bias_rows * LANES - biases.shape[0]))
    biases = biases.reshape(bias_rows, LANES)
    small_all, other_biases = share_small(n_dp, small, biases)
    row_order = dealing[0]
    picks = (row_order[:, None] == jnp.arange(rows, dtype=jnp.int32)[None, :]).astype(BF16)
    sent_rows = mm(picks, tokens).astype(BF16)
    dealt = lax.all_to_all(sent_rows, "dp", split_axis=0, concat_axis=0, tiled=True)
    grad_tokens, dealt = after(grad_tokens, dealt)
    sent_grads = mm(picks, grad_tokens).astype(BF16)
    grad_out = lax.all_to_all(sent_grads, "dp", split_axis=0, concat_axis=0, tiled=True)
    dealt_of_pair = by_rows(swap(dealt))
    joined = (segment_ids[:1] == segment_ids[-1:]).astype(jnp.int32)

    small_full = small_all[:, :6, :piece].transpose(1, 0, 2).reshape(6, width)
    flat, other_flat = biases.reshape(-1), other_biases.reshape(-1)
    bqv_full = join(flat[: 2 * half].reshape(2, half), other_flat[: 2 * half].reshape(2, half), 1)
    bup_full = join(
        flat[2 * half : 2 * half + hidden_half],
        other_flat[2 * half : 2 * half + hidden_half],
        0,
    )

    resid = by_rows(dealt.astype(F32))
    ln_one, normed_one, factor_one = normalize(resid, small_full[0], small_full[1])
    ln_one = ln_one.astype(BF16)
    kv_bias = jnp.stack(
        [jnp.zeros((pairs, LANES), F32), bqv_full[1].reshape(pairs, LANES)], axis=1
    ).reshape(-1)
    score_scale = HD**-0.5 * LOG2E
    shift = jnp.concatenate([bqv_full[0] * score_scale, kv_bias])
    scale = jnp.concatenate([jnp.full((width,), score_scale, F32), jnp.ones((2 * width,), F32)])
    qkv = (mm(ln_one, wqkv) * scale + shift).astype(BF16)
    own, own_lse = attention_own(qkv)
    dealt_of_pair, own = after(dealt_of_pair, own)
    ln_of_pair = normalize(dealt_of_pair.astype(F32), small_full[0], small_full[1])[0].astype(BF16)
    kv_of_pair = (mm(ln_of_pair, wkv) + kv_bias).astype(BF16)
    attended, lse = attention_pair(joined, qkv, kv_of_pair, own, own_lse)
    hidden = by_rows(resid + mm(attended, wout_t, 1, 1) + small_full[2])

    ln_two, normed_two, factor_two = normalize(hidden, small_full[3], small_full[4])
    ln_two = ln_two.astype(BF16)
    pre_act = mm(ln_two, wup) + bup_full
    square = pre_act * pre_act
    bend = jnp.tanh(pre_act * (GELU_ONE + GELU_THREE * square))
    gate = 0.5 + 0.5 * bend
    slope = gate + (0.5 * pre_act) * (1.0 - bend * bend) * (GELU_ONE + 3.0 * GELU_THREE * square)
    act, slope = after((pre_act * gate).astype(BF16), slope.astype(BF16))

    grad_down_t = mm(grad_out, act, 0, 0).astype(BF16)
    grad_pre = (mm(grad_out, wdown_t) * slope.astype(F32)).astype(BF16)
    bias_up_grad = jnp.sum(grad_pre, axis=0, dtype=F32)
    grad_up = mm(ln_two, grad_pre, 0, 0).astype(BF16)
    grad_down_t, grad_up, grad_pre = after(grad_down_t, grad_up, grad_pre)
    grad_ln_two = by_rows(mm(grad_pre, wup, 1, 1))
    gain_two_grad = jnp.sum(grad_ln_two * normed_two, axis=0)
    bias_two_grad = jnp.sum(grad_ln_two, axis=0)
    grad_hidden = grad_out.astype(F32) + norm_back(
        grad_ln_two, normed_two, factor_two, small_full[3]
    )
    grad_branch = grad_hidden.astype(BF16)
    grad_wout_t = mm(grad_branch, attended, 0, 0).astype(BF16)
    mlp_grads = jnp.concatenate([grad_down_t, grad_up, grad_wout_t], axis=1)
    mlp_grads, grad_branch, act = after(mlp_grads, grad_branch, act)
    mlp_sum = reduced(mlp_grads)
    grad_att = mm(grad_branch, wout_t).astype(BF16)
    output = by_rows((hidden + mm(act, wdown_t, 1, 1) + small_full[5]).astype(BF16))
    grad_att, output = after(grad_att, output)

    pair_dq, pair_dkv = attention_back_pair(
        joined, qkv, kv_of_pair, grad_att, attended, lse
    )
    for_pair = mm(pair_dkv, wkv, 1, 1).astype(BF16)
    for_pair = swap(for_pair)
    dq, dkv = attention_back_own(qkv, grad_att, attended, lse, pair_dq)
    grad_wq = mm(ln_one, dq, 0, 0).astype(BF16)
    grad_wkv = (mm(ln_one, dkv, 0, 0) + mm(ln_of_pair, pair_dkv, 0, 0)).astype(BF16)
    dq, dkv, grad_wq, grad_wkv = after(dq, dkv, grad_wq, grad_wkv)
    wq_sum = sum_on_chip(n_dp, piece, grad_wq)
    wkv_sum = sum_on_chip(n_dp, piece, grad_wkv)
    wqkv_sum = jnp.concatenate([sum_over_tensor(t, wq_sum), sum_over_tensor(t, wkv_sum)], axis=-1)
    grad_ln_one = by_rows(mm(dq, wq, 1, 1) + mm(dkv, wkv, 1, 1) + for_pair.astype(F32))
    grad_input = (
        grad_hidden + norm_back(grad_ln_one, normed_one, factor_one, small_full[0])
    ).astype(BF16)
    bias_q_grad = jnp.sum(dq, axis=0, dtype=F32)
    kv_sum = jnp.sum(dkv, axis=0, dtype=F32) + jnp.sum(pair_dkv, axis=0, dtype=F32)
    bias_v_grad = kv_sum.reshape(pairs, 2, LANES)[:, 1].reshape(-1)
    row_sums = jnp.concatenate(
        [
            jnp.stack(
                [
                    jnp.sum(grad_ln_one * normed_one, axis=0),
                    jnp.sum(grad_ln_one, axis=0),
                    jnp.sum(grad_hidden, axis=0),
                    gain_two_grad,
                    bias_two_grad,
                    jnp.sum(grad_out, axis=0, dtype=F32),
                    bias_q_grad,
                    bias_v_grad,
                ]
            ),
            bias_up_grad.reshape(-1, width),
        ]
    )
    qkv_part, row_sums = tree_sum(n_dp, piece, wqkv_sum, row_sums)
    small_part = lax.dynamic_slice_in_dim(
        row_sums[:6], lax.axis_index("dp") * piece, piece, 1
    )
    qv_part = mine_of(row_sums[6:8], 1)[0]
    bias_up_part = mine_of(row_sums[8:].reshape(-1), 0)[0]

    def paired(values, sizes):
        columns, start = [], 0
        for size in sizes:
            columns.append(mine_of(values[:, start : start + size], 1))
            start += size
        mine = jnp.concatenate([c[0] for c in columns], axis=1)
        other = jnp.concatenate([c[1] for c in columns], axis=1)
        other = swap(other)
        total = mine.astype(F32) + other.astype(F32)
        cuts = [sum(sizes[:i]) // 2 for i in range(1, len(sizes))]
        return jnp.split(total, cuts, axis=1)

    down_part, up_part, wout_part = paired(mlp_sum, (2 * hidden_half, 2 * hidden_half, width))
    down_part, wout_part = down_part.T, wout_part.T
    q_part, kv_part = qkv_part[:, :half], qkv_part[:, half:]
    kv_part = kv_part.reshape(piece, pairs // 2, 2, LANES).transpose(0, 2, 1, 3)
    qkv_part = jnp.concatenate(
        [q_part.reshape(piece, 1, half), kv_part.reshape(piece, 2, half)], axis=1
    )

    sent_out = lax.all_to_all(output, "dp", split_axis=0, concat_axis=0, tiled=True)
    sent_grad = lax.all_to_all(grad_input, "dp", split_axis=0, concat_axis=0, tiled=True)
    restored_out = mm(picks, sent_out, 0, 0).astype(BF16)
    restored_grad = mm(picks, sent_grad, 0, 0).astype(BF16)
    return (
        restored_out,
        restored_grad,
        small_part[0],
        small_part[1],
        qkv_part,
        qv_part,
        wout_part,
        small_part[2],
        small_part[3],
        small_part[4],
        up_part,
        bias_up_part,
        down_part,
        small_part[5],
    )


def solution(mesh):
    placed = (
        P(("dp", "tensor"), None),
        P(("dp", "tensor"), None),
        P(("dp", "tensor"), None),
        P("dp"),
        P("dp"),
        P("dp"),
        P("dp", None, "tensor"),
        P(None, "tensor"),
        P("tensor", "dp"),
        P("dp"),
        P("dp"),
        P("dp"),
        P("dp", "tensor"),
        P("tensor"),
        P("tensor", "dp"),
        P("dp"),
    )

    return jax.shard_map(
        per_device,
        mesh=mesh,
        in_specs=placed,
        out_specs=(
            P(("dp", "tensor"), None),
            P(("dp", "tensor"), None),
            P("dp"),
            P("dp"),
            P("dp", None, "tensor"),
            P(None, "tensor"),
            P("tensor", "dp"),
            P("dp"),
            P("dp"),
            P("dp"),
            P("dp", "tensor"),
            P("tensor"),
            P("tensor", "dp"),
            P("dp"),
        ),
        check_vma=False,
    )
```

```python
import functools

import jax
import jax.numpy as jnp
from jax import lax
from jax.experimental import pallas as pl
from jax.experimental.layout import Layout, with_layout_constraint
from jax.experimental.pallas import tpu as pltpu
from jax.sharding import PartitionSpec as P


DP, TP = "dp", "tensor"
HD = 64
LANES = 128
EPS = 1e-06
LN2 = 0.6931471805599453
LOG2E = 1.4426950408889634
GELU_ONE = 0.7978845608028654
GELU_THREE = 0.7978845608028654 * 0.044715
F32 = jnp.float32
BF16 = jnp.bfloat16


def normalize(values, gain_row, bias_row):
    centred = values - jnp.mean(values, axis=-1, keepdims=True)
    factor = lax.rsqrt(jnp.mean(centred * centred, axis=-1, keepdims=True) + EPS)
    normed = centred * factor
    return (normed * gain_row + bias_row, normed, factor)


def norm_back(grad_rows, normed, factor, gain_row):
    scaled = grad_rows * gain_row
    centred = scaled - jnp.mean(scaled, axis=-1, keepdims=True)
    return factor * (centred - normed * jnp.mean(scaled * normed, axis=-1, keepdims=True))


def mm(left, right, left_dim=1, right_dim=0):
    return lax.dot_general(
        left, right, (((left_dim,), (right_dim,)), ((), ())), preferred_element_type=F32
    )


def head_lanes(head):
    return (lax.broadcasted_iota(jnp.int32, (1, LANES), 1) // HD) == head


def attend_rows(q, keys, values):
    outs, lses = [], []
    one = jnp.ones((), BF16)
    for head in range(2):
        mine = head_lanes(head)
        scores = mm(jnp.where(mine, q, jnp.zeros_like(q)), keys, 1, 1)
        row_max = jnp.max(scores, axis=1, keepdims=True)
        weights = jnp.exp2(scores - row_max).astype(BF16)
        mixed = mm(weights, jnp.where(mine, values, one))
        total = jnp.sum(jnp.where(mine, 0.0, mixed), axis=1, keepdims=True) * (1.0 / HD)
        outs.append(mixed / total)
        lses.append(row_max + jnp.log2(total))
    first = head_lanes(0)
    return (jnp.where(first, outs[0], outs[1]), jnp.where(first, lses[0], lses[1]))


def own_forward(q_ref, kv_ref, mixed_ref, lse_ref, *, qblock):
    for block in range(q_ref.shape[0] // qblock):
        rows = pl.ds(block * qblock, qblock)
        mixed, lse = attend_rows(q_ref[rows, :], kv_ref[:, :LANES], kv_ref[:, LANES:])
        mixed_ref[rows, :] = mixed
        lse_ref[rows, :] = lse


def pair_forward(joined_ref, q_ref, kv_ref, own_ref, own_lse_ref, mixed_ref, lse_ref, *, qblock):
    joined = joined_ref[0] > 0

    @pl.when(joined)
    def _():
        for block in range(q_ref.shape[0] // qblock):
            rows = pl.ds(block * qblock, qblock)
            mixed, lse = attend_rows(q_ref[rows, :], kv_ref[:, :LANES], kv_ref[:, LANES:])
            own_lse = own_lse_ref[rows, :]
            top = jnp.maximum(own_lse, lse)
            own_share = jnp.exp2(own_lse - top)
            pair_share = jnp.exp2(lse - top)
            total = own_share + pair_share
            mixed_ref[rows, :] = (
                (own_ref[rows, :] * own_share + mixed * pair_share) / total
            ).astype(BF16)
            lse_ref[rows, :] = top + jnp.log2(total)

    @pl.when(jnp.logical_not(joined))
    def _():
        mixed_ref[...] = own_ref[...].astype(BF16)
        lse_ref[...] = own_lse_ref[...]


def split_three(values):
    high = values.astype(BF16)
    rest = values - high.astype(F32)
    middle = rest.astype(BF16)
    return high, middle, (rest - middle.astype(F32)).astype(BF16)


def attend_back(q_ref, grad_ref, mixed_ref, lse_ref, kv_ref, dkv_ref, dq_sum, kblock):
    lane = lax.broadcasted_iota(jnp.int32, (1, LANES), 1)
    q = q_ref[...]
    grad = grad_ref[...]
    products = grad.astype(F32) * mixed_ref[...].astype(F32)
    wide_q, wide_grad = [], []
    for head in range(2):
        mine = head_lanes(head)
        spare = (1 - head) * HD
        inner = jnp.sum(jnp.where(mine, products, 0.0), axis=1, keepdims=True)
        lse_parts = split_three(-lse_ref[:, head * HD : head * HD + 1])
        inner_parts = split_three(-inner)
        q_head = jnp.where(mine, q, jnp.zeros_like(q))
        grad_head = jnp.where(mine, grad, jnp.zeros_like(grad))
        for part in range(3):
            q_head = jnp.where(lane == spare + part, lse_parts[part], q_head)
            grad_head = jnp.where(lane == spare + part, inner_parts[part], grad_head)
        wide_q.append(q_head)
        wide_grad.append(grad_head)
    one = jnp.ones((), BF16)
    first = head_lanes(0)
    for block in range(kv_ref.shape[0] // kblock):
        rows = pl.ds(block * kblock, kblock)
        keys = kv_ref[rows, :LANES]
        values = kv_ref[rows, LANES:]
        key_grads, value_grads = [], []
        for head in range(2):
            mine = head_lanes(head)
            weights = jnp.exp2(mm(jnp.where(mine, keys, one), wide_q[head], 1, 1))
            grad_weights = mm(jnp.where(mine, values, one), wide_grad[head], 1, 1)
            grad_scores = (weights * grad_weights).astype(BF16)
            value_grads.append(mm(weights.astype(BF16), grad))
            key_grads.append(mm(grad_scores, q))
            dq_sum[head] += mm(keys, grad_scores, 0, 0)
        dkv_ref[rows, :LANES] = (jnp.where(first, key_grads[0], key_grads[1]) * LN2).astype(BF16)
        dkv_ref[rows, LANES:] = jnp.where(first, value_grads[0], value_grads[1]).astype(BF16)


def query_grad(dq_sum):
    return jnp.concatenate([dq_sum[0, :HD, :], dq_sum[1, HD:, :]], axis=0)


def pair_backward(
    joined_ref, q_ref, grad_ref, mixed_ref, lse_ref, kv_ref, dq_ref, dkv_ref, dq_sum, *, kblock
):
    joined = joined_ref[0] > 0
    dq_sum[...] = jnp.zeros_like(dq_sum)

    @pl.when(joined)
    def _():
        attend_back(q_ref, grad_ref, mixed_ref, lse_ref, kv_ref, dkv_ref, dq_sum, kblock)

    @pl.when(jnp.logical_not(joined))
    def _():
        dkv_ref[...] = jnp.zeros_like(dkv_ref)

    dq_ref[...] = query_grad(dq_sum)


def own_backward(
    q_ref, grad_ref, mixed_ref, lse_ref, kv_ref, pair_dq_ref, dq_ref, dkv_ref, dq_sum, *, kblock
):
    dq_sum[...] = jnp.zeros_like(dq_sum)
    attend_back(q_ref, grad_ref, mixed_ref, lse_ref, kv_ref, dkv_ref, dq_sum, kblock)
    total = query_grad(dq_sum) + pair_dq_ref[...]
    dq_ref[...] = (total.T * HD**-0.5).astype(BF16)


def params(**extra):
    return pltpu.CompilerParams(vmem_limit_bytes=56 << 20, **extra)


def cost(rows, keys, width, products):
    return pl.CostEstimate(
        flops=2 * rows * keys * width * products * 4,
        bytes_accessed=2 * width * (rows + 2 * keys),
        transcendentals=rows * keys * width // HD,
    )


def attention_own(qkv):
    rows = qkv.shape[0]
    width = qkv.shape[1] // 3
    pairs = width // LANES
    column = pl.BlockSpec((rows, LANES), lambda p: (0, p))
    own_kv = pl.BlockSpec((rows, 2 * LANES), lambda p: (0, pairs // 2 + p))
    shape = jax.ShapeDtypeStruct((rows, width), F32)
    return pl.pallas_call(
        functools.partial(own_forward, qblock=min(512, rows)),
        grid=(pairs,),
        in_specs=[column, own_kv],
        out_specs=[column, column],
        out_shape=[shape, shape],
        compiler_params=params(),
        cost_estimate=cost(rows, rows, width, 2),
        name="attend_own",
    )(qkv, qkv)


def attention_pair(joined, qkv, kv_of_pair, own, own_lse):
    rows, width = own.shape
    pairs = width // LANES
    column = pl.BlockSpec((rows, LANES), lambda p: (0, p))
    pair_kv = pl.BlockSpec((rows, 2 * LANES), lambda p: (0, p))
    return pl.pallas_call(
        functools.partial(pair_forward, qblock=min(512, rows)),
        grid=(pairs,),
        in_specs=[pl.BlockSpec(memory_space=pltpu.SMEM), column, pair_kv, column, column],
        out_specs=[column, column],
        out_shape=[
            jax.ShapeDtypeStruct((rows, width), BF16),
            jax.ShapeDtypeStruct((rows, width), F32),
        ],
        compiler_params=params(),
        cost_estimate=cost(rows, rows, width, 2),
        name="attend_pair",
    )(joined, qkv, kv_of_pair, own, own_lse)


def attention_back_pair(joined, qkv, kv_of_pair, grad, mixed, lse):
    rows, width = grad.shape
    pairs = width // LANES
    column = pl.BlockSpec((rows, LANES), lambda p: (0, p))
    pair_kv = pl.BlockSpec((rows, 2 * LANES), lambda p: (0, p))
    across = pl.BlockSpec((LANES, rows), lambda p: (p, 0))
    return pl.pallas_call(
        functools.partial(pair_backward, kblock=min(512, rows)),
        grid=(pairs,),
        in_specs=[pl.BlockSpec(memory_space=pltpu.SMEM)] + [column] * 4 + [pair_kv],
        out_specs=[across, pair_kv],
        out_shape=[
            jax.ShapeDtypeStruct((width, rows), F32),
            jax.ShapeDtypeStruct((rows, 2 * width), BF16),
        ],
        scratch_shapes=[pltpu.VMEM((2, LANES, rows), F32)],
        compiler_params=params(),
        cost_estimate=cost(rows, rows, width, 5),
        name="attend_back_pair",
    )(joined, qkv, grad, mixed, lse, kv_of_pair)


def attention_back_own(qkv, grad, mixed, lse, pair_dq):
    rows, width = grad.shape
    pairs = width // LANES
    column = pl.BlockSpec((rows, LANES), lambda p: (0, p))
    own_kv = pl.BlockSpec((rows, 2 * LANES), lambda p: (0, pairs // 2 + p))
    kv_out = pl.BlockSpec((rows, 2 * LANES), lambda p: (0, p))
    across = pl.BlockSpec((LANES, rows), lambda p: (p, 0))
    return pl.pallas_call(
        functools.partial(own_backward, kblock=min(512, rows)),
        grid=(pairs,),
        in_specs=[column] * 4 + [own_kv, across],
        out_specs=[column, kv_out],
        out_shape=[
            jax.ShapeDtypeStruct((rows, width), BF16),
            jax.ShapeDtypeStruct((rows, 2 * width), BF16),
        ],
        scratch_shapes=[pltpu.VMEM((2, LANES, rows), F32)],
        compiler_params=params(),
        cost_estimate=cost(rows, rows, width, 5),
        name="attend_back_own",
    )(qkv, grad, mixed, lse, qkv, pair_dq)


def small_kernel(n_dp, slice_ref, bias_ref, all_ref, partner_ref, send_sem, recv_sem):
    me = lax.axis_index(DP)
    t = lax.axis_index(TP)

    barrier = pltpu.get_barrier_semaphore()

    def greet(step, carry):
        peer = lax.rem(me + step, n_dp)
        pl.semaphore_signal(
            barrier, inc=1, device_id=(peer, t), device_id_type=pl.DeviceIdType.MESH
        )
        return carry

    lax.fori_loop(1, n_dp, greet, 0)
    pl.semaphore_signal(
        barrier, inc=1, device_id=(me, 1 - t), device_id_type=pl.DeviceIdType.MESH
    )
    pl.semaphore_wait(barrier, n_dp)

    def to_peer(step):
        return pltpu.make_async_remote_copy(
            src_ref=slice_ref,
            dst_ref=all_ref.at[me],
            send_sem=send_sem.at[step],
            recv_sem=recv_sem.at[step],
            device_id=(lax.rem(me + step, n_dp), t),
            device_id_type=pl.DeviceIdType.MESH,
        )

    to_partner = pltpu.make_async_remote_copy(
        src_ref=bias_ref,
        dst_ref=partner_ref,
        send_sem=send_sem.at[0],
        recv_sem=recv_sem.at[0],
        device_id=(me, 1 - t),
        device_id_type=pl.DeviceIdType.MESH,
    )
    to_partner.start()

    def start(step, carry):
        to_peer(step).start()
        return carry

    def finish(step, carry):
        to_peer(step).wait()
        return carry

    lax.fori_loop(1, n_dp, start, 0)
    all_ref[me] = slice_ref[...]
    lax.fori_loop(1, n_dp, finish, 0)
    to_partner.wait()


def share_small(n_dp, slices, biases):
    vmem = pl.BlockSpec(memory_space=pltpu.VMEM)
    return pl.pallas_call(
        functools.partial(small_kernel, n_dp),
        in_specs=[vmem, vmem],
        out_specs=[vmem, vmem],
        out_shape=[
            jax.ShapeDtypeStruct((n_dp,) + slices.shape, F32),
            jax.ShapeDtypeStruct(biases.shape, F32),
        ],
        scratch_shapes=[
            pltpu.SemaphoreType.DMA((n_dp,)),
            pltpu.SemaphoreType.DMA((n_dp,)),
        ],
        compiler_params=pltpu.CompilerParams(collective_id=0, has_side_effects=True),
        name="share_small",
    )(slices, biases)


def by_rows(values):
    return with_layout_constraint(values, Layout((0, 1)))


def after(*values):
    return lax.optimization_barrier(values)


def swap(values):
    return lax.ppermute(values, TP, [(0, 1), (1, 0)])


def tree_gather(n_dp, t, values, split):
    me = lax.axis_index(DP)

    def joined(own, other, upper, axis):
        return jnp.where(
            upper, jnp.concatenate([other, own], axis=axis), jnp.concatenate([own, other], axis=axis)
        )

    blocks = values[None]
    steps = [1 << bit for bit in range(n_dp.bit_length() - 1)]
    for step in reversed(steps[1:]):
        other = lax.ppermute(blocks, DP, [(i, i ^ step) for i in range(n_dp)])
        upper = (me // step) % 2 == 1
        blocks = joined(blocks[:, None], other[:, None], upper, 1).reshape((-1,) + values.shape)
    other = swap(blocks)
    blocks = jnp.concatenate(
        [
            joined(blocks[..., :split], other[..., :split], t == 1, 2),
            joined(blocks[..., split:], other[..., split:], t == 1, 2),
        ],
        axis=2,
    )
    other = lax.ppermute(blocks, DP, [(i, i ^ 1) for i in range(n_dp)])
    full = joined(blocks[:, None], other[:, None], me % 2 == 1, 1)
    full = full.reshape(n_dp * values.shape[0], 2 * values.shape[1])
    return full


def dp_partners(n_dp, step):
    return [(i, i ^ step) for i in range(n_dp)]


def add_half(first, second, upper, exchange):
    mine = jnp.where(upper, second, first)
    arrived = exchange(jnp.where(upper, first, second))
    return (mine.astype(F32) + arrived.astype(F32)).astype(BF16)


def sum_on_chip(n_dp, piece, values):
    odd = lax.axis_index(DP) % 2 == 1
    blocks = values.reshape(n_dp // 2, 2, piece, values.shape[-1])
    return add_half(
        blocks[:, 0], blocks[:, 1], odd, lambda v: lax.ppermute(v, DP, dp_partners(n_dp, 1))
    )


def sum_over_tensor(t, values):
    low, high = jnp.split(values, 2, axis=-1)
    return add_half(low, high, t == 1, swap)


def tree_sum(n_dp, piece, total, rows):
    me = lax.axis_index(DP)
    arrived_rows = lax.ppermute(rows, DP, dp_partners(n_dp, 1))
    rows = rows + arrived_rows
    arrived_rows = swap(rows)
    rows = rows + arrived_rows
    step = 2
    while step < n_dp:
        blocks = total.reshape(-1, 2, piece, total.shape[-1])
        upper = (me // step) % 2 == 1
        sent, rows = after(jnp.where(upper, blocks[:, 0], blocks[:, 1]), rows)
        partners = dp_partners(n_dp, step)
        arrived, arrived_rows = after(
            lax.ppermute(sent, DP, partners), lax.ppermute(rows, DP, partners)
        )
        mine = jnp.where(upper, blocks[:, 1], blocks[:, 0])
        total = (mine.astype(F32) + arrived.astype(F32)).astype(BF16)
        rows = rows + arrived_rows
        step *= 2
    return total.reshape(piece, -1).astype(F32), rows


def per_device(
    tokens,
    grad_tokens,
    dealing,
    segment_ids,
    ln1_gain,
    ln1_bias,
    w_qkv,
    b_qv,
    w_out,
    b_out,
    ln2_gain,
    ln2_bias,
    w_up,
    b_up,
    w_down,
    b_down,
):
    n_dp = lax.axis_size(DP)
    t = lax.axis_index(TP)
    rows, width = tokens.shape
    piece = ln1_gain.shape[0]
    half = b_qv.shape[1]
    hidden_half = b_up.shape[0]
    pairs = width // LANES

    def join(own, other, axis):
        return jnp.where(
            t == 0,
            jnp.concatenate([own, other], axis=axis),
            jnp.concatenate([other, own], axis=axis),
        )

    def reduced(values):
        return lax.psum_scatter(values, DP, scatter_dimension=0, tiled=True)

    def mine_of(values, axis):
        size = values.shape[axis] // 2
        low, high = (
            lax.slice_in_dim(values, 0, size, axis=axis),
            lax.slice_in_dim(values, size, 2 * size, axis=axis),
        )
        return jnp.where(t == 0, low, high), jnp.where(t == 0, high, low)

    kv_local = (
        w_qkv[:, 1:]
        .reshape(piece, 2, pairs // 2, LANES)
        .transpose(0, 2, 1, 3)
        .reshape(piece, 2 * half)
    )
    wqkv = tree_gather(n_dp, t, jnp.concatenate([w_qkv[:, 0], kv_local], axis=1), half)
    wq, wkv = wqkv[:, :width], wqkv[:, width:]
    rest_local = jnp.concatenate([w_out.T, w_up, w_down.T], axis=1)
    other_rest = swap(rest_local)
    up_at, down_at = half, half + hidden_half
    rest_local = jnp.concatenate(
        [
            join(rest_local[:, :up_at], other_rest[:, :up_at], 1),
            join(rest_local[:, up_at:down_at], other_rest[:, up_at:down_at], 1),
            join(rest_local[:, down_at:], other_rest[:, down_at:], 1),
        ],
        axis=1,
    )
    rest = lax.all_gather(rest_local, DP, axis=0, tiled=True)
    wout_t = rest[:, :width]
    wup = rest[:, width : width + 2 * hidden_half]
    wdown_t = rest[:, width + 2 * hidden_half :]

    small = jnp.stack([ln1_gain, ln1_bias, b_out, ln2_gain, ln2_bias, b_down])
    small = jnp.pad(small, ((0, 2), (0, LANES - piece)))
    biases = jnp.concatenate([b_qv.reshape(-1), b_up])
    bias_rows = -(-biases.shape[0] // (8 * LANES)) * 8
    biases = jnp.pad(biases, (0, bias_rows * LANES - biases.shape[0]))
    biases = biases.reshape(bias_rows, LANES)
    small_all, other_biases = share_small(n_dp, small, biases)
    row_order = dealing[0]
    picks = (row_order[:, None] == jnp.arange(rows, dtype=jnp.int32)[None, :]).astype(BF16)
    sent_rows = mm(picks, tokens).astype(BF16)
    dealt = lax.all_to_all(sent_rows, DP, split_axis=0, concat_axis=0, tiled=True)
    grad_tokens, dealt = after(grad_tokens, dealt)
    sent_grads = mm(picks, grad_tokens).astype(BF16)
    grad_out = lax.all_to_all(sent_grads, DP, split_axis=0, concat_axis=0, tiled=True)
    dealt_of_pair = by_rows(swap(dealt))
    joined = (segment_ids[:1] == segment_ids[-1:]).astype(jnp.int32)

    small_full = small_all[:, :6, :piece].transpose(1, 0, 2).reshape(6, width)
    flat, other_flat = biases.reshape(-1), other_biases.reshape(-1)
    bqv_full = join(flat[: 2 * half].reshape(2, half), other_flat[: 2 * half].reshape(2, half), 1)
    bup_full = join(
        flat[2 * half : 2 * half + hidden_half],
        other_flat[2 * half : 2 * half + hidden_half],
        0,
    )

    resid = by_rows(dealt.astype(F32))
    ln_one, normed_one, factor_one = normalize(resid, small_full[0], small_full[1])
    ln_one = ln_one.astype(BF16)
    kv_bias = jnp.stack(
        [jnp.zeros((pairs, LANES), F32), bqv_full[1].reshape(pairs, LANES)], axis=1
    ).reshape(-1)
    score_scale = HD**-0.5 * LOG2E
    shift = jnp.concatenate([bqv_full[0] * score_scale, kv_bias])
    scale = jnp.concatenate([jnp.full((width,), score_scale, F32), jnp.ones((2 * width,), F32)])
    qkv = (mm(ln_one, wqkv) * scale + shift).astype(BF16)
    own, own_lse = attention_own(qkv)
    dealt_of_pair, own = after(dealt_of_pair, own)
    ln_of_pair = normalize(dealt_of_pair.astype(F32), small_full[0], small_full[1])[0].astype(BF16)
    kv_of_pair = (mm(ln_of_pair, wkv) + kv_bias).astype(BF16)
    attended, lse = attention_pair(joined, qkv, kv_of_pair, own, own_lse)
    hidden = by_rows(resid + mm(attended, wout_t, 1, 1) + small_full[2])

    ln_two, normed_two, factor_two = normalize(hidden, small_full[3], small_full[4])
    ln_two = ln_two.astype(BF16)
    pre_act = mm(ln_two, wup) + bup_full
    square = pre_act * pre_act
    bend = jnp.tanh(pre_act * (GELU_ONE + GELU_THREE * square))
    gate = 0.5 + 0.5 * bend
    slope = gate + (0.5 * pre_act) * (1.0 - bend * bend) * (GELU_ONE + 3.0 * GELU_THREE * square)
    act, slope = after((pre_act * gate).astype(BF16), slope.astype(BF16))

    grad_down_t = mm(grad_out, act, 0, 0).astype(BF16)
    grad_pre = (mm(grad_out, wdown_t) * slope.astype(F32)).astype(BF16)
    bias_up_grad = jnp.sum(grad_pre, axis=0, dtype=F32)
    grad_up = mm(ln_two, grad_pre, 0, 0).astype(BF16)
    grad_down_t, grad_up, grad_pre = after(grad_down_t, grad_up, grad_pre)
    grad_ln_two = by_rows(mm(grad_pre, wup, 1, 1))
    gain_two_grad = jnp.sum(grad_ln_two * normed_two, axis=0)
    bias_two_grad = jnp.sum(grad_ln_two, axis=0)
    grad_hidden = grad_out.astype(F32) + norm_back(
        grad_ln_two, normed_two, factor_two, small_full[3]
    )
    grad_branch = grad_hidden.astype(BF16)
    grad_wout_t = mm(grad_branch, attended, 0, 0).astype(BF16)
    mlp_grads = jnp.concatenate([grad_down_t, grad_up, grad_wout_t], axis=1)
    mlp_grads, grad_branch, act = after(mlp_grads, grad_branch, act)
    mlp_sum = reduced(mlp_grads)
    grad_att = mm(grad_branch, wout_t).astype(BF16)
    output = by_rows((hidden + mm(act, wdown_t, 1, 1) + small_full[5]).astype(BF16))
    grad_att, output = after(grad_att, output)

    pair_dq, pair_dkv = attention_back_pair(
        joined, qkv, kv_of_pair, grad_att, attended, lse
    )
    for_pair = mm(pair_dkv, wkv, 1, 1).astype(BF16)
    for_pair = swap(for_pair)
    dq, dkv = attention_back_own(qkv, grad_att, attended, lse, pair_dq)
    grad_wq = mm(ln_one, dq, 0, 0).astype(BF16)
    grad_wkv = (mm(ln_one, dkv, 0, 0) + mm(ln_of_pair, pair_dkv, 0, 0)).astype(BF16)
    dq, dkv, grad_wq, grad_wkv = after(dq, dkv, grad_wq, grad_wkv)
    wq_sum = sum_on_chip(n_dp, piece, grad_wq)
    wkv_sum = sum_on_chip(n_dp, piece, grad_wkv)
    wqkv_sum = jnp.concatenate(
        [sum_over_tensor(t, wq_sum), sum_over_tensor(t, wkv_sum)], axis=-1
    )
    grad_ln_one = by_rows(mm(dq, wq, 1, 1) + mm(dkv, wkv, 1, 1) + for_pair.astype(F32))
    grad_input = (
        grad_hidden + norm_back(grad_ln_one, normed_one, factor_one, small_full[0])
    ).astype(BF16)
    bias_q_grad = jnp.sum(dq, axis=0, dtype=F32)
    kv_sum = jnp.sum(dkv, axis=0, dtype=F32) + jnp.sum(pair_dkv, axis=0, dtype=F32)
    bias_v_grad = kv_sum.reshape(pairs, 2, LANES)[:, 1].reshape(-1)
    row_sums = jnp.concatenate(
        [
            jnp.stack(
                [
                    jnp.sum(grad_ln_one * normed_one, axis=0),
                    jnp.sum(grad_ln_one, axis=0),
                    jnp.sum(grad_hidden, axis=0),
                    gain_two_grad,
                    bias_two_grad,
                    jnp.sum(grad_out, axis=0, dtype=F32),
                    bias_q_grad,
                    bias_v_grad,
                ]
            ),
            bias_up_grad.reshape(-1, width),
        ]
    )
    qkv_part, row_sums = tree_sum(n_dp, piece, wqkv_sum, row_sums)
    small_part = lax.dynamic_slice_in_dim(
        row_sums[:6], lax.axis_index(DP) * piece, piece, 1
    )
    qv_part = mine_of(row_sums[6:8], 1)[0]
    bias_up_part = mine_of(row_sums[8:].reshape(-1), 0)[0]

    def paired(values, sizes):
        columns, start = [], 0
        for size in sizes:
            columns.append(mine_of(values[:, start : start + size], 1))
            start += size
        mine = jnp.concatenate([c[0] for c in columns], axis=1)
        other = jnp.concatenate([c[1] for c in columns], axis=1)
        other = swap(other)
        total = mine.astype(F32) + other.astype(F32)
        cuts = [sum(sizes[:i]) // 2 for i in range(1, len(sizes))]
        return jnp.split(total, cuts, axis=1)

    down_part, up_part, wout_part = paired(mlp_sum, (2 * hidden_half, 2 * hidden_half, width))
    down_part, wout_part = down_part.T, wout_part.T
    q_part, kv_part = qkv_part[:, :half], qkv_part[:, half:]
    kv_part = kv_part.reshape(piece, pairs // 2, 2, LANES).transpose(0, 2, 1, 3)
    qkv_part = jnp.concatenate(
        [q_part.reshape(piece, 1, half), kv_part.reshape(piece, 2, half)], axis=1
    )

    sent_out = lax.all_to_all(output, DP, split_axis=0, concat_axis=0, tiled=True)
    sent_grad = lax.all_to_all(grad_input, DP, split_axis=0, concat_axis=0, tiled=True)
    restored_out = mm(picks, sent_out, 0, 0).astype(BF16)
    restored_grad = mm(picks, sent_grad, 0, 0).astype(BF16)
    return (
        restored_out,
        restored_grad,
        small_part[0],
        small_part[1],
        qkv_part,
        qv_part,
        wout_part,
        small_part[2],
        small_part[3],
        small_part[4],
        up_part,
        bias_up_part,
        down_part,
        small_part[5],
    )


def solution(mesh):
    both, dp, tp, by_both = P((DP, TP), None), P(DP), P(TP), P(DP, TP)
    placed = (both, both, both, dp, dp, dp, P(DP, None, TP), P(None, TP), P(TP, DP), dp, dp, dp)
    placed += (by_both, tp, P(TP, DP), dp)

    return jax.shard_map(
        per_device,
        mesh=mesh,
        in_specs=placed,
        out_specs=placed[:2] + placed[4:],
        check_vma=False,
    )
```

```python
import functools

import jax
import jax.numpy as jnp
from jax import lax
from jax.experimental import pallas as pl
from jax.experimental.layout import Layout, with_layout_constraint
from jax.experimental.pallas import tpu as pltpu
from jax.sharding import PartitionSpec as P


DP, TP = "dp", "tensor"
HD = 64
LANES = 128
EPS = 1e-06
LN2 = 0.6931471805599453
LOG2E = 1.4426950408889634
GELU_ONE = 0.7978845608028654
GELU_THREE = 0.7978845608028654 * 0.044715
F32 = jnp.float32
BF16 = jnp.bfloat16


def normalize(values, gain_row, bias_row):
    centred = values - jnp.mean(values, axis=-1, keepdims=True)
    factor = lax.rsqrt(jnp.mean(centred * centred, axis=-1, keepdims=True) + EPS)
    normed = centred * factor
    return (normed * gain_row + bias_row, normed, factor)


def norm_back(grad_rows, normed, factor, gain_row):
    scaled = grad_rows * gain_row
    centred = scaled - jnp.mean(scaled, axis=-1, keepdims=True)
    return factor * (centred - normed * jnp.mean(scaled * normed, axis=-1, keepdims=True))


def mm(left, right, left_dim=1, right_dim=0):
    return lax.dot_general(
        left, right, (((left_dim,), (right_dim,)), ((), ())), preferred_element_type=F32
    )


def head_lanes(head):
    return (lax.broadcasted_iota(jnp.int32, (1, LANES), 1) // HD) == head


def attend_rows(q, keys, values):
    outs, lses = [], []
    one = jnp.ones((), BF16)
    for head in range(2):
        mine = head_lanes(head)
        scores = mm(jnp.where(mine, q, jnp.zeros_like(q)), keys, 1, 1)
        row_max = jnp.max(scores, axis=1, keepdims=True)
        weights = jnp.exp2(scores - row_max).astype(BF16)
        mixed = mm(weights, jnp.where(mine, values, one))
        total = jnp.sum(jnp.where(mine, 0.0, mixed), axis=1, keepdims=True) * (1.0 / HD)
        outs.append(mixed / total)
        lses.append(row_max + jnp.log2(total))
    first = head_lanes(0)
    return (jnp.where(first, outs[0], outs[1]), jnp.where(first, lses[0], lses[1]))


def own_forward(q_ref, kv_ref, mixed_ref, lse_ref, *, qblock):
    for block in range(q_ref.shape[0] // qblock):
        rows = pl.ds(block * qblock, qblock)
        mixed, lse = attend_rows(q_ref[rows, :], kv_ref[:, :LANES], kv_ref[:, LANES:])
        mixed_ref[rows, :] = mixed
        lse_ref[rows, :] = lse


def pair_forward(joined_ref, q_ref, kv_ref, own_ref, own_lse_ref, mixed_ref, lse_ref, *, qblock):
    joined = joined_ref[0] > 0

    @pl.when(joined)
    def _():
        for block in range(q_ref.shape[0] // qblock):
            rows = pl.ds(block * qblock, qblock)
            mixed, lse = attend_rows(q_ref[rows, :], kv_ref[:, :LANES], kv_ref[:, LANES:])
            own_lse = own_lse_ref[rows, :]
            top = jnp.maximum(own_lse, lse)
            own_share = jnp.exp2(own_lse - top)
            pair_share = jnp.exp2(lse - top)
            total = own_share + pair_share
            mixed_ref[rows, :] = (
                (own_ref[rows, :] * own_share + mixed * pair_share) / total
            ).astype(BF16)
            lse_ref[rows, :] = top + jnp.log2(total)

    @pl.when(jnp.logical_not(joined))
    def _():
        mixed_ref[...] = own_ref[...].astype(BF16)
        lse_ref[...] = own_lse_ref[...]


def split_three(values):
    high = values.astype(BF16)
    rest = values - high.astype(F32)
    middle = rest.astype(BF16)
    return high, middle, (rest - middle.astype(F32)).astype(BF16)


def attend_back(q_ref, grad_ref, mixed_ref, lse_ref, kv_ref, dkv_ref, dq_sum, kblock):
    lane = lax.broadcasted_iota(jnp.int32, (1, LANES), 1)
    q = q_ref[...]
    grad = grad_ref[...]
    products = grad.astype(F32) * mixed_ref[...].astype(F32)
    wide_q, wide_grad = [], []
    for head in range(2):
        mine = head_lanes(head)
        spare = (1 - head) * HD
        inner = jnp.sum(jnp.where(mine, products, 0.0), axis=1, keepdims=True)
        lse_parts = split_three(-lse_ref[:, head * HD : head * HD + 1])
        inner_parts = split_three(-inner)
        q_head = jnp.where(mine, q, jnp.zeros_like(q))
        grad_head = jnp.where(mine, grad, jnp.zeros_like(grad))
        for part in range(3):
            q_head = jnp.where(lane == spare + part, lse_parts[part], q_head)
            grad_head = jnp.where(lane == spare + part, inner_parts[part], grad_head)
        wide_q.append(q_head)
        wide_grad.append(grad_head)
    one = jnp.ones((), BF16)
    first = head_lanes(0)
    for block in range(kv_ref.shape[0] // kblock):
        rows = pl.ds(block * kblock, kblock)
        keys = kv_ref[rows, :LANES]
        values = kv_ref[rows, LANES:]
        key_grads, value_grads = [], []
        for head in range(2):
            mine = head_lanes(head)
            weights = jnp.exp2(mm(jnp.where(mine, keys, one), wide_q[head], 1, 1))
            grad_weights = mm(jnp.where(mine, values, one), wide_grad[head], 1, 1)
            grad_scores = (weights * grad_weights).astype(BF16)
            value_grads.append(mm(weights.astype(BF16), grad))
            key_grads.append(mm(grad_scores, q))
            dq_sum[head] += mm(keys, grad_scores, 0, 0)
        dkv_ref[rows, :LANES] = (jnp.where(first, key_grads[0], key_grads[1]) * LN2).astype(BF16)
        dkv_ref[rows, LANES:] = jnp.where(first, value_grads[0], value_grads[1]).astype(BF16)


def query_grad(dq_sum):
    return jnp.concatenate([dq_sum[0, :HD, :], dq_sum[1, HD:, :]], axis=0)


def pair_backward(
    joined_ref, q_ref, grad_ref, mixed_ref, lse_ref, kv_ref, dq_ref, dkv_ref, dq_sum, *, kblock
):
    joined = joined_ref[0] > 0
    dq_sum[...] = jnp.zeros_like(dq_sum)

    @pl.when(joined)
    def _():
        attend_back(q_ref, grad_ref, mixed_ref, lse_ref, kv_ref, dkv_ref, dq_sum, kblock)

    @pl.when(jnp.logical_not(joined))
    def _():
        dkv_ref[...] = jnp.zeros_like(dkv_ref)

    dq_ref[...] = query_grad(dq_sum)


def own_backward(
    q_ref, grad_ref, mixed_ref, lse_ref, kv_ref, pair_dq_ref, dq_ref, dkv_ref, dq_sum, *, kblock
):
    dq_sum[...] = jnp.zeros_like(dq_sum)
    attend_back(q_ref, grad_ref, mixed_ref, lse_ref, kv_ref, dkv_ref, dq_sum, kblock)
    total = query_grad(dq_sum) + pair_dq_ref[...]
    dq_ref[...] = (total.T * HD**-0.5).astype(BF16)


def params(**extra):
    return pltpu.CompilerParams(vmem_limit_bytes=56 << 20, **extra)


def cost(rows, keys, width, products):
    return pl.CostEstimate(
        flops=2 * rows * keys * width * products * 4,
        bytes_accessed=2 * width * (rows + 2 * keys),
        transcendentals=rows * keys * width // HD,
    )


def attention_own(qkv):
    rows = qkv.shape[0]
    width = qkv.shape[1] // 3
    pairs = width // LANES
    column = pl.BlockSpec((rows, LANES), lambda p: (0, p))
    own_kv = pl.BlockSpec((rows, 2 * LANES), lambda p: (0, pairs // 2 + p))
    shape = jax.ShapeDtypeStruct((rows, width), F32)
    return pl.pallas_call(
        functools.partial(own_forward, qblock=min(512, rows)),
        grid=(pairs,),
        in_specs=[column, own_kv],
        out_specs=[column, column],
        out_shape=[shape, shape],
        compiler_params=params(),
        cost_estimate=cost(rows, rows, width, 2),
        name="attend_own",
    )(qkv, qkv)


def attention_pair(joined, qkv, kv_of_pair, own, own_lse):
    rows, width = own.shape
    pairs = width // LANES
    column = pl.BlockSpec((rows, LANES), lambda p: (0, p))
    pair_kv = pl.BlockSpec((rows, 2 * LANES), lambda p: (0, p))
    return pl.pallas_call(
        functools.partial(pair_forward, qblock=min(512, rows)),
        grid=(pairs,),
        in_specs=[pl.BlockSpec(memory_space=pltpu.SMEM), column, pair_kv, column, column],
        out_specs=[column, column],
        out_shape=[
            jax.ShapeDtypeStruct((rows, width), BF16),
            jax.ShapeDtypeStruct((rows, width), F32),
        ],
        compiler_params=params(),
        cost_estimate=cost(rows, rows, width, 2),
        name="attend_pair",
    )(joined, qkv, kv_of_pair, own, own_lse)


def attention_back_pair(joined, qkv, kv_of_pair, grad, mixed, lse):
    rows, width = grad.shape
    pairs = width // LANES
    column = pl.BlockSpec((rows, LANES), lambda p: (0, p))
    pair_kv = pl.BlockSpec((rows, 2 * LANES), lambda p: (0, p))
    across = pl.BlockSpec((LANES, rows), lambda p: (p, 0))
    return pl.pallas_call(
        functools.partial(pair_backward, kblock=min(512, rows)),
        grid=(pairs,),
        in_specs=[pl.BlockSpec(memory_space=pltpu.SMEM)] + [column] * 4 + [pair_kv],
        out_specs=[across, pair_kv],
        out_shape=[
            jax.ShapeDtypeStruct((width, rows), F32),
            jax.ShapeDtypeStruct((rows, 2 * width), BF16),
        ],
        scratch_shapes=[pltpu.VMEM((2, LANES, rows), F32)],
        compiler_params=params(),
        cost_estimate=cost(rows, rows, width, 5),
        name="attend_back_pair",
    )(joined, qkv, grad, mixed, lse, kv_of_pair)


def attention_back_own(qkv, grad, mixed, lse, pair_dq):
    rows, width = grad.shape
    pairs = width // LANES
    column = pl.BlockSpec((rows, LANES), lambda p: (0, p))
    own_kv = pl.BlockSpec((rows, 2 * LANES), lambda p: (0, pairs // 2 + p))
    kv_out = pl.BlockSpec((rows, 2 * LANES), lambda p: (0, p))
    across = pl.BlockSpec((LANES, rows), lambda p: (p, 0))
    return pl.pallas_call(
        functools.partial(own_backward, kblock=min(512, rows)),
        grid=(pairs,),
        in_specs=[column] * 4 + [own_kv, across],
        out_specs=[column, kv_out],
        out_shape=[
            jax.ShapeDtypeStruct((rows, width), BF16),
            jax.ShapeDtypeStruct((rows, 2 * width), BF16),
        ],
        scratch_shapes=[pltpu.VMEM((2, LANES, rows), F32)],
        compiler_params=params(),
        cost_estimate=cost(rows, rows, width, 5),
        name="attend_back_own",
    )(qkv, grad, mixed, lse, qkv, pair_dq)


def small_kernel(n_dp, slice_ref, bias_ref, all_ref, partner_ref, send_sem, recv_sem):
    me = lax.axis_index(DP)
    t = lax.axis_index(TP)

    barrier = pltpu.get_barrier_semaphore()

    def greet(step, carry):
        peer = lax.rem(me + step, n_dp)
        pl.semaphore_signal(
            barrier, inc=1, device_id=(peer, t), device_id_type=pl.DeviceIdType.MESH
        )
        return carry

    lax.fori_loop(1, n_dp, greet, 0)
    pl.semaphore_signal(
        barrier, inc=1, device_id=(me, 1 - t), device_id_type=pl.DeviceIdType.MESH
    )
    pl.semaphore_wait(barrier, n_dp)

    def to_peer(step):
        return pltpu.make_async_remote_copy(
            src_ref=slice_ref,
            dst_ref=all_ref.at[me],
            send_sem=send_sem.at[step],
            recv_sem=recv_sem.at[step],
            device_id=(lax.rem(me + step, n_dp), t),
            device_id_type=pl.DeviceIdType.MESH,
        )

    to_partner = pltpu.make_async_remote_copy(
        src_ref=bias_ref,
        dst_ref=partner_ref,
        send_sem=send_sem.at[0],
        recv_sem=recv_sem.at[0],
        device_id=(me, 1 - t),
        device_id_type=pl.DeviceIdType.MESH,
    )
    to_partner.start()

    def start(step, carry):
        to_peer(step).start()
        return carry

    def finish(step, carry):
        to_peer(step).wait()
        return carry

    lax.fori_loop(1, n_dp, start, 0)
    all_ref[me] = slice_ref[...]
    lax.fori_loop(1, n_dp, finish, 0)
    to_partner.wait()


def share_small(n_dp, slices, biases):
    vmem = pl.BlockSpec(memory_space=pltpu.VMEM)
    return pl.pallas_call(
        functools.partial(small_kernel, n_dp),
        in_specs=[vmem, vmem],
        out_specs=[vmem, vmem],
        out_shape=[
            jax.ShapeDtypeStruct((n_dp,) + slices.shape, F32),
            jax.ShapeDtypeStruct(biases.shape, F32),
        ],
        scratch_shapes=[
            pltpu.SemaphoreType.DMA((n_dp,)),
            pltpu.SemaphoreType.DMA((n_dp,)),
        ],
        compiler_params=pltpu.CompilerParams(collective_id=0, has_side_effects=True),
        name="share_small",
    )(slices, biases)


def by_rows(values):
    return with_layout_constraint(values, Layout((0, 1)))


def after(*values):
    return lax.optimization_barrier(values)


def swap(values):
    return lax.ppermute(values, TP, [(0, 1), (1, 0)])


def tree_gather(n_dp, t, values, split):
    me = lax.axis_index(DP)

    def joined(own, other, upper, axis):
        return jnp.where(
            upper, jnp.concatenate([other, own], axis=axis), jnp.concatenate([own, other], axis=axis)
        )

    blocks = values[None]
    steps = [1 << bit for bit in range(n_dp.bit_length() - 1)]
    for step in reversed(steps[1:]):
        other = lax.ppermute(blocks, DP, [(i, i ^ step) for i in range(n_dp)])
        upper = (me // step) % 2 == 1
        blocks = joined(blocks[:, None], other[:, None], upper, 1).reshape((-1,) + values.shape)
    other = swap(blocks)
    blocks = jnp.concatenate(
        [
            joined(blocks[..., :split], other[..., :split], t == 1, 2),
            joined(blocks[..., split:], other[..., split:], t == 1, 2),
        ],
        axis=2,
    )
    other = lax.ppermute(blocks, DP, [(i, i ^ 1) for i in range(n_dp)])
    full = joined(blocks[:, None], other[:, None], me % 2 == 1, 1)
    full = full.reshape(n_dp * values.shape[0], 2 * values.shape[1])
    return full


def dp_partners(n_dp, step):
    return [(i, i ^ step) for i in range(n_dp)]


def add_half(first, second, upper, exchange):
    mine = jnp.where(upper, second, first)
    arrived = exchange(jnp.where(upper, first, second))
    return (mine.astype(F32) + arrived.astype(F32)).astype(BF16)


def sum_on_chip(n_dp, piece, values):
    odd = lax.axis_index(DP) % 2 == 1
    blocks = values.reshape(n_dp // 2, 2, piece, values.shape[-1])
    return add_half(
        blocks[:, 0], blocks[:, 1], odd, lambda v: lax.ppermute(v, DP, dp_partners(n_dp, 1))
    )


def sum_over_tensor(t, values):
    low, high = jnp.split(values, 2, axis=-1)
    return add_half(low, high, t == 1, swap)


def tree_sum(n_dp, piece, total, rows):
    me = lax.axis_index(DP)
    arrived_rows = lax.ppermute(rows, DP, dp_partners(n_dp, 1))
    rows = rows + arrived_rows
    arrived_rows = swap(rows)
    rows = rows + arrived_rows
    step = 2
    while step < n_dp:
        blocks = total.reshape(-1, 2, piece, total.shape[-1])
        upper = (me // step) % 2 == 1
        sent, rows = after(jnp.where(upper, blocks[:, 0], blocks[:, 1]), rows)
        partners = dp_partners(n_dp, step)
        arrived, arrived_rows = after(
            lax.ppermute(sent, DP, partners), lax.ppermute(rows, DP, partners)
        )
        mine = jnp.where(upper, blocks[:, 1], blocks[:, 0])
        total = (mine.astype(F32) + arrived.astype(F32)).astype(BF16)
        rows = rows + arrived_rows
        step *= 2
    return total.reshape(piece, -1).astype(F32), rows


def per_device(
    tokens,
    grad_tokens,
    dealing,
    segment_ids,
    ln1_gain,
    ln1_bias,
    w_qkv,
    b_qv,
    w_out,
    b_out,
    ln2_gain,
    ln2_bias,
    w_up,
    b_up,
    w_down,
    b_down,
):
    n_dp = lax.axis_size(DP)
    t = lax.axis_index(TP)
    rows, width = tokens.shape
    piece = ln1_gain.shape[0]
    half = b_qv.shape[1]
    hidden_half = b_up.shape[0]
    pairs = width // LANES

    def join(own, other, axis):
        return jnp.where(
            t == 0,
            jnp.concatenate([own, other], axis=axis),
            jnp.concatenate([other, own], axis=axis),
        )

    def reduced(values):
        return lax.psum_scatter(values, DP, scatter_dimension=0, tiled=True)

    def mine_of(values, axis):
        size = values.shape[axis] // 2
        low, high = (
            lax.slice_in_dim(values, 0, size, axis=axis),
            lax.slice_in_dim(values, size, 2 * size, axis=axis),
        )
        return jnp.where(t == 0, low, high), jnp.where(t == 0, high, low)

    kv_local = (
        w_qkv[:, 1:]
        .reshape(piece, 2, pairs // 2, LANES)
        .transpose(0, 2, 1, 3)
        .reshape(piece, 2 * half)
    )
    wqkv = tree_gather(n_dp, t, jnp.concatenate([w_qkv[:, 0], kv_local], axis=1), half)
    wq, wkv = wqkv[:, :width], wqkv[:, width:]
    rest_local = jnp.concatenate([w_out.T, w_up, w_down.T], axis=1)
    other_rest = swap(rest_local)
    up_at, down_at = half, half + hidden_half
    rest_local = jnp.concatenate(
        [
            join(rest_local[:, :up_at], other_rest[:, :up_at], 1),
            join(rest_local[:, up_at:down_at], other_rest[:, up_at:down_at], 1),
            join(rest_local[:, down_at:], other_rest[:, down_at:], 1),
        ],
        axis=1,
    )
    rest = lax.all_gather(rest_local, DP, axis=0, tiled=True)
    wout_t = rest[:, :width]
    wup = rest[:, width : width + 2 * hidden_half]
    wdown_t = rest[:, width + 2 * hidden_half :]

    small = jnp.stack([ln1_gain, ln1_bias, b_out, ln2_gain, ln2_bias, b_down])
    small = jnp.pad(small, ((0, 2), (0, LANES - piece)))
    biases = jnp.concatenate([b_qv.reshape(-1), b_up])
    bias_rows = -(-biases.shape[0] // (8 * LANES)) * 8
    biases = jnp.pad(biases, (0, bias_rows * LANES - biases.shape[0]))
    biases = biases.reshape(bias_rows, LANES)
    small_all, other_biases = share_small(n_dp, small, biases)
    row_order = dealing[0]
    picks = (row_order[:, None] == jnp.arange(rows, dtype=jnp.int32)[None, :]).astype(BF16)
    sent_rows = mm(picks, tokens).astype(BF16)
    dealt = lax.all_to_all(sent_rows, DP, split_axis=0, concat_axis=0, tiled=True)
    sent_grads = mm(picks, grad_tokens).astype(BF16)
    grad_out = lax.all_to_all(sent_grads, DP, split_axis=0, concat_axis=0, tiled=True)
    dealt_of_pair = by_rows(swap(dealt))
    joined = (segment_ids[:1] == segment_ids[-1:]).astype(jnp.int32)

    small_full = small_all[:, :6, :piece].transpose(1, 0, 2).reshape(6, width)
    flat, other_flat = biases.reshape(-1), other_biases.reshape(-1)
    bqv_full = join(flat[: 2 * half].reshape(2, half), other_flat[: 2 * half].reshape(2, half), 1)
    bup_full = join(
        flat[2 * half : 2 * half + hidden_half],
        other_flat[2 * half : 2 * half + hidden_half],
        0,
    )

    resid = by_rows(dealt.astype(F32))
    ln_one, normed_one, factor_one = normalize(resid, small_full[0], small_full[1])
    ln_one = ln_one.astype(BF16)
    kv_bias = jnp.stack(
        [jnp.zeros((pairs, LANES), F32), bqv_full[1].reshape(pairs, LANES)], axis=1
    ).reshape(-1)
    score_scale = HD**-0.5 * LOG2E
    shift = jnp.concatenate([bqv_full[0] * score_scale, kv_bias])
    scale = jnp.concatenate([jnp.full((width,), score_scale, F32), jnp.ones((2 * width,), F32)])
    qkv = (mm(ln_one, wqkv) * scale + shift).astype(BF16)
    own, own_lse = attention_own(qkv)
    dealt_of_pair, own = after(dealt_of_pair, own)
    ln_of_pair = normalize(dealt_of_pair.astype(F32), small_full[0], small_full[1])[0].astype(BF16)
    kv_of_pair = (mm(ln_of_pair, wkv) + kv_bias).astype(BF16)
    attended, lse = attention_pair(joined, qkv, kv_of_pair, own, own_lse)
    hidden = by_rows(resid + mm(attended, wout_t, 1, 1) + small_full[2])

    ln_two, normed_two, factor_two = normalize(hidden, small_full[3], small_full[4])
    ln_two = ln_two.astype(BF16)
    pre_act = mm(ln_two, wup) + bup_full
    square = pre_act * pre_act
    gate = 0.5 + 0.5 * jnp.tanh(pre_act * (GELU_ONE + GELU_THREE * square))
    act = pre_act * gate
    slope = gate + (act - act * gate) * (2.0 * GELU_ONE + 6.0 * GELU_THREE * square)
    act, slope = after(act.astype(BF16), slope.astype(BF16))

    grad_down_t = mm(grad_out, act, 0, 0).astype(BF16)
    grad_pre = (mm(grad_out, wdown_t) * slope.astype(F32)).astype(BF16)
    bias_up_grad = jnp.sum(grad_pre, axis=0, dtype=F32)
    grad_up = mm(ln_two, grad_pre, 0, 0).astype(BF16)
    grad_down_t, grad_up, grad_pre = after(grad_down_t, grad_up, grad_pre)
    grad_ln_two = by_rows(mm(grad_pre, wup, 1, 1))
    gain_two_grad = jnp.sum(grad_ln_two * normed_two, axis=0)
    bias_two_grad = jnp.sum(grad_ln_two, axis=0)
    grad_hidden = grad_out.astype(F32) + norm_back(
        grad_ln_two, normed_two, factor_two, small_full[3]
    )
    grad_branch = grad_hidden.astype(BF16)
    grad_wout_t = mm(grad_branch, attended, 0, 0).astype(BF16)
    mlp_grads = jnp.concatenate([grad_down_t, grad_up, grad_wout_t], axis=1)
    mlp_grads, grad_branch, act = after(mlp_grads, grad_branch, act)
    mlp_sum = reduced(mlp_grads)
    grad_att = mm(grad_branch, wout_t).astype(BF16)
    output = by_rows((hidden + mm(act, wdown_t, 1, 1) + small_full[5]).astype(BF16))
    grad_att, output = after(grad_att, output)

    pair_dq, pair_dkv = attention_back_pair(
        joined, qkv, kv_of_pair, grad_att, attended, lse
    )
    for_pair = mm(pair_dkv, wkv, 1, 1).astype(BF16)
    for_pair = swap(for_pair)
    dq, dkv = attention_back_own(qkv, grad_att, attended, lse, pair_dq)
    grad_wq = mm(ln_one, dq, 0, 0).astype(BF16)
    grad_wkv = (mm(ln_one, dkv, 0, 0) + mm(ln_of_pair, pair_dkv, 0, 0)).astype(BF16)
    dq, dkv, grad_wq, grad_wkv = after(dq, dkv, grad_wq, grad_wkv)
    wq_sum = sum_on_chip(n_dp, piece, grad_wq)
    wkv_sum = sum_on_chip(n_dp, piece, grad_wkv)
    wqkv_sum = jnp.concatenate(
        [sum_over_tensor(t, wq_sum), sum_over_tensor(t, wkv_sum)], axis=-1
    )
    grad_ln_one = by_rows(mm(dq, wq, 1, 1) + mm(dkv, wkv, 1, 1) + for_pair.astype(F32))
    grad_input = (
        grad_hidden + norm_back(grad_ln_one, normed_one, factor_one, small_full[0])
    ).astype(BF16)
    bias_q_grad = jnp.sum(dq, axis=0, dtype=F32)
    kv_sum = jnp.sum(dkv, axis=0, dtype=F32) + jnp.sum(pair_dkv, axis=0, dtype=F32)
    bias_v_grad = kv_sum.reshape(pairs, 2, LANES)[:, 1].reshape(-1)
    row_sums = jnp.concatenate(
        [
            jnp.stack(
                [
                    jnp.sum(grad_ln_one * normed_one, axis=0),
                    jnp.sum(grad_ln_one, axis=0),
                    jnp.sum(grad_hidden, axis=0),
                    gain_two_grad,
                    bias_two_grad,
                    jnp.sum(grad_out, axis=0, dtype=F32),
                    bias_q_grad,
                    bias_v_grad,
                ]
            ),
            bias_up_grad.reshape(-1, width),
        ]
    )
    qkv_part, row_sums = tree_sum(n_dp, piece, wqkv_sum, row_sums)
    small_part = lax.dynamic_slice_in_dim(
        row_sums[:6], lax.axis_index(DP) * piece, piece, 1
    )
    qv_part = mine_of(row_sums[6:8], 1)[0]
    bias_up_part = mine_of(row_sums[8:].reshape(-1), 0)[0]

    def paired(values, sizes):
        columns, start = [], 0
        for size in sizes:
            columns.append(mine_of(values[:, start : start + size], 1))
            start += size
        mine = jnp.concatenate([c[0] for c in columns], axis=1)
        other = jnp.concatenate([c[1] for c in columns], axis=1)
        other = swap(other)
        total = mine.astype(F32) + other.astype(F32)
        cuts = [sum(sizes[:i]) // 2 for i in range(1, len(sizes))]
        return jnp.split(total, cuts, axis=1)

    down_part, up_part, wout_part = paired(mlp_sum, (2 * hidden_half, 2 * hidden_half, width))
    down_part, wout_part = down_part.T, wout_part.T
    q_part, kv_part = qkv_part[:, :half], qkv_part[:, half:]
    kv_part = kv_part.reshape(piece, pairs // 2, 2, LANES).transpose(0, 2, 1, 3)
    qkv_part = jnp.concatenate(
        [q_part.reshape(piece, 1, half), kv_part.reshape(piece, 2, half)], axis=1
    )

    sent_out = lax.all_to_all(output, DP, split_axis=0, concat_axis=0, tiled=True)
    sent_grad = lax.all_to_all(grad_input, DP, split_axis=0, concat_axis=0, tiled=True)
    restored_out = mm(picks, sent_out, 0, 0).astype(BF16)
    restored_grad = mm(picks, sent_grad, 0, 0).astype(BF16)
    return (
        restored_out,
        restored_grad,
        small_part[0],
        small_part[1],
        qkv_part,
        qv_part,
        wout_part,
        small_part[2],
        small_part[3],
        small_part[4],
        up_part,
        bias_up_part,
        down_part,
        small_part[5],
    )


def solution(mesh):
    both, dp, tp, by_both = P((DP, TP), None), P(DP), P(TP), P(DP, TP)
    placed = (both, both, both, dp, dp, dp, P(DP, None, TP), P(None, TP), P(TP, DP), dp, dp, dp)
    placed += (by_both, tp, P(TP, DP), dp)

    return jax.shard_map(
        per_device,
        mesh=mesh,
        in_specs=placed,
        out_specs=placed[:2] + placed[4:],
        check_vma=False,
    )
```
